8 devices in a mesh: dp: 1 (over z), cp: 2 (over y), tp: 4 (over x, core).
Axes of the slice: x: 2, y: 2, z: 1, core: 2. Of those that a mesh axis runs over, the one named last changes fastest.
Arguments:
- x_tok: bfloat16 [3072, 1536], P(('dp', 'cp', 'tp'))
- w_q: bfloat16 [1536, 48, 32], P(None, 'tp')
- w_k: bfloat16 [1536, 8, 32], P(None, 'tp')
- w_v: bfloat16 [1536, 8, 32], P(None, 'tp')
- w_o: bfloat16 [48, 32, 1536], P('tp')
- expert_ids: int32 [3072, 2], P(('dp', 'cp', 'tp'))
- gate_wts: float32 [3072, 2], P(('dp', 'cp', 'tp'))
- w_gate: bfloat16 [16, 1536, 2048], P(('cp', 'tp'))
- w_up: bfloat16 [16, 1536, 2048], P(('cp', 'tp'))
- w_down: bfloat16 [16, 2048, 1536], P(('cp', 'tp'))
Outputs:
- output: bfloat16 [3072, 1536], P(('dp', 'cp', 'tp'))
All inputs are finite; a program needn't handle non-finite values.
Results may differ from the reference program's by a relative error of at most 0.0104868.
Values are sent between devices in bfloat16 or wider.
A program may use at most 1 GiB of HBM per device.

```python
import math
import jax
import jax.numpy as jnp
from jax import lax

TOK_DEV = 384
CP = 2
TP = 4
HID = 1536
FFN = 4096
HEADS = 48
KV_HEADS = 8
HEAD = 32
EXPERTS = 8
TOP = 2

SEQ = TOK_DEV * CP * TP
BLOCKS = CP * TP
PAIRS = CP * TP // 2
LOCAL = EXPERTS // PAIRS
HALF_FFN = FFN // 2
GROUP = HEADS // KV_HEADS


def token_positions():
    half_len = SEQ // CP
    chunk_len = half_len // 2
    row_ids = jnp.arange(SEQ)
    cp_rank = row_ids // half_len
    in_half = row_ids % half_len
    return jnp.where(in_half < chunk_len, cp_rank * chunk_len + in_half, (2 * CP - 1 - cp_rank) * chunk_len + in_half - chunk_len)


def draw_routing(route_key):
    perm_key, label_key = jax.random.split(route_key)
    tok_order = jax.vmap(lambda one_key: jax.random.permutation(one_key, TOK_DEV))(jax.random.split(perm_key, BLOCKS))
    relabel = jax.vmap(lambda one_key: jax.random.permutation(one_key, EXPERTS))(jax.random.split(label_key, BLOCKS))
    raw_ids = (tok_order[:, :, None] + jnp.arange(TOP)[None, None, :]) % EXPERTS
    picked = jax.vmap(lambda label_map, raw_set: label_map[raw_set])(relabel, raw_ids)
    return picked.reshape(SEQ, TOP).astype(jnp.int32)


def setup_inputs(seed: int = 0, part: int = 0) -> dict:
    part_key = jax.random.fold_in(jax.random.key(seed), part)
    key_x, key_route, key_gate = jax.random.split(part_key, 3)
    weight_keys = jax.random.split(jax.random.key(seed + 1), 7)
    score_gain = math.sqrt(max(math.log(SEQ / 8.0), 1.0))
    in_scale = 1.0 / math.sqrt(HID)
    x_tok = jax.random.normal(key_x, (SEQ, HID), jnp.float32).astype(jnp.bfloat16)
    w_q = (jax.random.normal(weight_keys[0], (HID, HEADS, HEAD), jnp.float32) * (score_gain * in_scale)).astype(jnp.bfloat16)
    w_k = (jax.random.normal(weight_keys[1], (HID, KV_HEADS, HEAD), jnp.float32) * in_scale).astype(jnp.bfloat16)
    w_v = (jax.random.normal(weight_keys[2], (HID, KV_HEADS, HEAD), jnp.float32) * in_scale).astype(jnp.bfloat16)
    w_o = (jax.random.normal(weight_keys[3], (HEADS, HEAD, HID), jnp.float32) * (2.0 / math.sqrt(HEADS * HEAD))).astype(jnp.bfloat16)
    w_gate = (jax.random.normal(weight_keys[4], (2 * EXPERTS, HID, HALF_FFN), jnp.float32) * in_scale).astype(jnp.bfloat16)
    w_up = (jax.random.normal(weight_keys[5], (2 * EXPERTS, HID, HALF_FFN), jnp.float32) * in_scale).astype(jnp.bfloat16)
    w_down = (jax.random.normal(weight_keys[6], (2 * EXPERTS, HALF_FFN, HID), jnp.float32) * (2.0 / math.sqrt(FFN))).astype(jnp.bfloat16)
    gate_raw = jax.random.uniform(key_gate, (SEQ, TOP), jnp.float32, 1.0, 3.0)
    gate_wts = gate_raw / jnp.sum(gate_raw, axis=1, keepdims=True)
    expert_ids = draw_routing(key_route)
    return {"x_tok": x_tok, "w_q": w_q, "w_k": w_k, "w_v": w_v, "w_o": w_o, "expert_ids": expert_ids, "gate_wts": gate_wts, "w_gate": w_gate, "w_up": w_up, "w_down": w_down}


def reference(x_tok, w_q, w_k, w_v, w_o, expert_ids, gate_wts, w_gate, w_up, w_down):
    q_all = jnp.dot(x_tok, w_q.reshape(HID, HEADS * HEAD), preferred_element_type=jnp.float32).astype(jnp.bfloat16)
    k_all = jnp.dot(x_tok, w_k.reshape(HID, KV_HEADS * HEAD), preferred_element_type=jnp.float32).astype(jnp.bfloat16)
    v_all = jnp.dot(x_tok, w_v.reshape(HID, KV_HEADS * HEAD), preferred_element_type=jnp.float32).astype(jnp.bfloat16)
    q_blocks = q_all.reshape(BLOCKS, TOK_DEV, KV_HEADS, GROUP, HEAD)
    positions = token_positions()
    pos_blocks = positions.reshape(BLOCKS, TOK_DEV)
    keys_f = k_all.reshape(SEQ, KV_HEADS, HEAD).astype(jnp.float32)
    vals_f = v_all.reshape(SEQ, KV_HEADS, HEAD).astype(jnp.float32)
    score_scale = HEAD ** -0.5

    def attend(blk_item):
        q_blk, q_pos = blk_item
        scores = jnp.einsum("qgrd,kgd->grqk", q_blk.astype(jnp.float32), keys_f) * score_scale
        allowed = q_pos[:, None] >= positions[None, :]
        scores = jnp.where(allowed[None, None], scores, -jnp.inf)
        row_peak = jnp.max(scores, axis=-1, keepdims=True)
        prob_vals = jnp.exp(scores - row_peak)
        row_sum = jnp.sum(prob_vals, axis=-1)
        mixed_vals = jnp.einsum("grqk,kgd->qgrd", prob_vals.astype(jnp.bfloat16).astype(jnp.float32), vals_f)
        return (mixed_vals / jnp.moveaxis(row_sum, -1, 0)[..., None]).astype(jnp.bfloat16)

    attn_out = lax.map(attend, (q_blocks, pos_blocks)).reshape(SEQ, HEADS * HEAD)
    h_tok = (x_tok.astype(jnp.float32) + jnp.dot(attn_out, w_o.reshape(HEADS * HEAD, HID), preferred_element_type=jnp.float32)).astype(jnp.bfloat16)

    full_gate = w_gate.reshape(PAIRS, 2, LOCAL, HID, HALF_FFN).transpose(0, 2, 3, 1, 4).reshape(EXPERTS, HID, FFN)
    full_up = w_up.reshape(PAIRS, 2, LOCAL, HID, HALF_FFN).transpose(0, 2, 3, 1, 4).reshape(EXPERTS, HID, FFN)
    full_down = w_down.reshape(PAIRS, 2, LOCAL, HALF_FFN, HID).transpose(0, 2, 1, 3, 4).reshape(EXPERTS, FFN, HID)
    flat_ids = expert_ids.reshape(-1)
    sort_order = jnp.argsort(flat_ids, stable=True)
    per_expert = SEQ * TOP // EXPERTS
    tok_rows = (sort_order // TOP).reshape(EXPERTS, per_expert)

    def run_expert(expert_item):
        rows_e, gate_e, up_e, down_e = expert_item
        tokens = h_tok[rows_e]
        gate_pre = jnp.dot(tokens, gate_e, preferred_element_type=jnp.float32)
        up_pre = jnp.dot(tokens, up_e, preferred_element_type=jnp.float32)
        hidden = (jax.nn.silu(gate_pre) * up_pre).astype(jnp.bfloat16)
        return jnp.dot(hidden, down_e, preferred_element_type=jnp.float32).astype(jnp.bfloat16)

    z_sorted = lax.map(run_expert, (tok_rows, full_gate, full_up, full_down)).reshape(SEQ * TOP, HID)
    back_order = jnp.argsort(sort_order)
    z_choice = z_sorted[back_order].reshape(SEQ, TOP, HID)
    y_acc = h_tok.astype(jnp.float32)
    for choice in range(TOP):
        y_acc = y_acc + gate_wts[:, choice:choice + 1] * z_choice[:, choice].astype(jnp.float32)
    return y_acc.astype(jnp.bfloat16)
```

```python
import functools
import math

import jax
import jax.numpy as jnp
from jax import lax
from jax.experimental import pallas as pl
from jax.experimental.pallas import tpu as pltpu
from jax.sharding import PartitionSpec as P

MESH = pl.DeviceIdType.MESH
F32 = jnp.float32
BF16 = jnp.bfloat16

NT = (((1,), (1,)), ((), ()))
QT = 128
KC = 256


def dot(a, b):
    return jnp.dot(a, b, preferred_element_type=F32)


def dot_nt(a, b):
    return lax.dot_general(a, b, NT, preferred_element_type=F32)


def remote(src, dst, send, recv, **dev):
    return pltpu.make_async_remote_copy(src_ref=src, dst_ref=dst, send_sem=send, recv_sem=recv, device_id=dev, device_id_type=MESH)


def attn_kernel(x, wq_h, wk_h, wv_h, wo_h, wg, wu, wd,
                h_out, wg_r, wu_r, wd_r,
                xh, wq, wkv, wo, kvown, kvrecv, kaug, vt, qaug, osend, orecv, m_s, l_s, acc_s,
                loc_sem, xf_s, xf_r, xp_s, xp_r, xw_s, xw_r, kv_s, kv_r, wo_s, wo_r, ew_s, ew_r, o_s, o_r):
    c = lax.axis_index("cp")
    t = lax.axis_index("tp")
    s = lax.rem(t, 2)
    part = t + 1 - 2 * s
    far = lax.rem(t + 2, 4)
    farp = lax.rem(part + 2, 4)
    cn = 1 - c
    tok = xh.shape[1]
    nr = tok // QT
    chunk = 2 * tok
    hid = x.shape[1]
    heads = wq_h.shape[0] // 32
    npair = heads // 2
    scale = 32 ** -0.5 * math.log2(math.e)

    bar = pltpu.get_barrier_semaphore()
    pl.semaphore_signal(bar, inc=1, device_id={"tp": part}, device_id_type=MESH)
    pl.semaphore_signal(bar, inc=1, device_id={"tp": far}, device_id_type=MESH)
    pl.semaphore_signal(bar, inc=1, device_id={"tp": farp}, device_id_type=MESH)
    pl.semaphore_signal(bar, inc=1, device_id={"cp": cn}, device_id_type=MESH)

    locs = [
        pltpu.make_async_copy(x, xh.at[t], loc_sem.at[0]),
        pltpu.make_async_copy(wq_h, wq, loc_sem.at[1]),
        pltpu.make_async_copy(wk_h, wkv.at[pl.ds(0, 64)], loc_sem.at[2]),
        pltpu.make_async_copy(wv_h, wkv.at[pl.ds(64, 64)], loc_sem.at[3]),
        pltpu.make_async_copy(wo_h, wo.at[t], loc_sem.at[4]),
    ]
    for cp_ in locs:
        cp_.start()
    pl.semaphore_wait(bar, 4)

    xfar = [remote(x.at[pl.ds(k * QT, QT)], xh.at[t, pl.ds(k * QT, QT)], xf_s.at[k], xf_r.at[k], tp=far) for k in range(nr)]
    xpart = remote(x, xh.at[t], xp_s, xp_r, tp=part)
    xfwd = [remote(xh.at[far, pl.ds(k * QT, QT)], xh.at[far, pl.ds(k * QT, QT)], xw_s.at[k], xw_r.at[k], tp=part) for k in range(nr)]
    for k in range(nr):
        xfar[k].start()
    xpart.start()

    qaug[:, :, 96:128, :] = jnp.zeros((qaug.shape[0], npair, 32, 2 * QT), BF16)

    def project(b):
        xb = xh[b]
        qt = dot_nt(wq[...], xb).astype(BF16)
        qs = qt.astype(F32) * scale
        h1 = qs.astype(BF16)
        r1 = qs - h1.astype(F32)
        h2 = r1.astype(BF16)
        h3 = (r1 - h2.astype(F32)).astype(BF16)
        for r in range(nr):
            for hd in range(heads):
                for k, part_v in enumerate((h1, h2, h3)):
                    qaug[b * nr + r, hd // 2, k * 32:(k + 1) * 32, (hd % 2) * QT:(hd % 2 + 1) * QT] = part_v[hd * 32:(hd + 1) * 32, r * QT:(r + 1) * QT]
        kvown[b] = dot_nt(wkv[...], xb).astype(BF16)

    def kvcopy(b):
        return remote(kvown.at[b], kvrecv.at[b], kv_s.at[b], kv_r.at[b], cp=cn)

    for cp_ in locs[:4]:
        cp_.wait()
    project(t)
    kvcopy(t).start()
    xpart.wait_recv()
    project(part)
    kvcopy(part).start()
    for k in range(nr):
        xfar[k].wait_recv()
        xfwd[k].start()
    project(far)
    kvcopy(far).start()
    for k in range(nr):
        xfwd[k].wait_recv()
    project(farp)
    kvcopy(farp).start()
    for k in range(nr):
        xfar[k].wait_send()
        xfwd[k].wait_send()
    xpart.wait_send()

    locs[4].wait()
    wofar = remote(wo_h, wo.at[t], wo_s.at[0], wo_r.at[0], tp=far)
    wopart = remote(wo_h, wo.at[t], wo_s.at[1], wo_r.at[1], tp=part)
    wofwd = remote(wo.at[far], wo.at[far], wo_s.at[2], wo_r.at[2], tp=part)
    wofar.start()
    wopart.start()

    zero_pad = jnp.zeros((32, tok), BF16)

    def place(b, src, cc):
        second = b // 2
        ck = cc * (1 - second) + (3 - cc) * second
        pos = pl.multiple_of(ck * chunk + lax.rem(b, 2) * tok, QT)
        kv = src[b]
        for g in range(2):
            kt = kv[g * 32:(g + 1) * 32]
            kaug[g, pl.ds(pos, tok), :] = jnp.concatenate([kt, kt, kt, zero_pad], axis=0).T
        vt[:, pl.ds(pos, tok)] = kv[64:128]

    def place_own(b, carry):
        place(b, kvown, c)
        return carry

    def place_recv(b, carry):
        kvcopy(b).wait_recv()
        place(b, kvrecv, cn)
        return carry

    lax.fori_loop(0, 4, place_own, 0)
    lax.fori_loop(0, 4, place_recv, 0)

    def ocopy(i, b, r):
        return remote(osend.at[i], orecv.at[pl.ds(r * QT, QT), pl.ds(t * tok, tok)], o_s.at[i], o_r.at[t, r], tp=b)

    def tile_of(ii):
        kk = ii // nr
        r = lax.rem(ii, nr)
        xb = lax.rem(t // 2 + 1 - kk // 2, 2)
        sb = lax.rem(s + lax.rem((kk + 1) // 2, 2), 2)
        return 2 * xb + sb, r

    def wcopy(ii):
        out = []
        for w, wr in ((wg, wg_r), (wu, wu_r)):
            n = w.shape[1] // (4 * nr)
            sl = pl.ds(pl.multiple_of(ii * n, n), n)
            k = 0 if w is wg else 1
            out.append(remote(w.at[1 - s, sl], wr.at[sl], ew_s.at[k], ew_r.at[k], tp=part))
        return out

    def wdcopy(ii):
        n = wd.shape[1] // 8
        sl = pl.ds(pl.multiple_of(ii * n, n), n)
        return remote(wd.at[1 - s, sl], wd_r.at[sl], ew_s.at[2], ew_r.at[2], tp=part)

    def tile(ii, carry):
        for cp_ in wcopy(ii):
            cp_.start()

        @pl.when(ii < 8)
        def _():
            wdcopy(ii).start()

        @pl.when(ii == 2 * nr)
        def _():
            wofar.wait_recv()
            wofwd.start()

        b, r = tile_of(ii)
        i = b * nr + r
        second = b // 2
        ck = c * (1 - second) + (3 - c) * second
        qpos = ck * chunk + lax.rem(b, 2) * tok + r * QT
        nfull = qpos // KC
        m_s[...] = jnp.full(m_s.shape, -jnp.inf, F32)
        l_s[...] = jnp.zeros(l_s.shape, F32)
        acc_s[...] = jnp.zeros(acc_s.shape, F32)

        def step(j, masked):
            k0 = pl.multiple_of(j * KC, KC)
            if masked:
                key_i = lax.broadcasted_iota(jnp.int32, (KC, 2 * QT), 0) + k0
                q_i = lax.rem(lax.broadcasted_iota(jnp.int32, (KC, 2 * QT), 1), QT) + qpos
                allowed = key_i <= q_i
            for p in range(npair):
                g = p // (npair // 2)
                sc = dot(kaug[g, pl.ds(k0, KC), :], qaug[i, p])
                if masked:
                    sc = jnp.where(allowed, sc, -jnp.inf)
                s8 = sc.reshape(KC // 8, 8, 2 * QT)
                mx = jnp.max(jnp.max(s8, axis=0), axis=0, keepdims=True)
                m_old = m_s[p]
                m_new = jnp.maximum(m_old, mx)
                alpha = jnp.exp2(m_old - m_new)
                pr = jnp.exp2(sc - m_new)
                l_s[p] = l_s[p] * alpha + jnp.sum(pr.reshape(KC // 8, 8, 2 * QT), axis=0)
                pv = dot(vt[g * 32:(g + 1) * 32, pl.ds(k0, KC)], pr.astype(BF16))
                acc_s[p] = acc_s[p] * alpha + pv
                m_s[p] = m_new

        def body(j, cc):
            step(j, False)
            return cc

        lax.fori_loop(0, nfull, body, 0)
        step(nfull, True)

        pieces = []
        for p in range(npair):
            o = acc_s[p] / jnp.sum(l_s[p], axis=0, keepdims=True)
            pieces += [o[:, :QT], o[:, QT:]]
        tile_o = jnp.concatenate(pieces, axis=0).T.astype(BF16)

        @pl.when(ii < 3 * nr)
        def _():
            osend[i] = tile_o
            ocopy(i, b, r).start()

        @pl.when(ii >= 3 * nr)
        def _():
            orecv[pl.ds(pl.multiple_of(r * QT, QT), QT), pl.ds(pl.multiple_of(t * tok, QT), tok)] = tile_o
        return carry

    lax.fori_loop(0, 4 * nr, tile, 0)

    def odone(ii, carry):
        b, r = tile_of(ii)
        ocopy(b * nr + r, b, r).wait_send()
        remote(osend.at[0], orecv.at[pl.ds(pl.multiple_of(r * QT, QT), QT), pl.ds(pl.multiple_of(b * tok, QT), tok)], o_s.at[0], o_r.at[b, r], tp=b).wait_recv()
        return carry

    lax.fori_loop(0, 3 * nr, odone, 0)
    wofar.wait_send()
    wopart.wait()
    wofwd.wait()

    nt = hid // 4

    def proj_out(n, carry):
        sl = pl.ds(pl.multiple_of(n * nt, QT), nt)
        ow = dot(orecv[...], wo[:, :, sl].reshape(hid, nt))
        h_out[:, sl] = (xh[t, :, sl].astype(F32) + ow).astype(BF16)
        return carry

    lax.fori_loop(0, 4, proj_out, 0)

    def kvdone(b, carry):
        kvcopy(b).wait_send()
        return carry

    lax.fori_loop(0, 4, kvdone, 0)
    for k, (w, wr) in enumerate(((wg, wg_r), (wu, wu_r), (wd, wd_r))):
        remote(w.at[1 - s], wr, ew_s.at[k], ew_r.at[k], tp=part).wait()


def moe_kernel(h, ids, gates, wg, wu, wd, wg_r, wu_r, wd_r,
               y_out,
               g_v, u_v, d_v, send, recv, zsend, zret, zacc,
               w_sem, s_s, s_r, z_s, z_r):
    c = lax.axis_index("cp")
    t = lax.axis_index("tp")
    s = lax.rem(t, 2)
    xx = t // 2
    tok, hid = h.shape
    cap = recv.shape[1]
    nf = g_v.shape[0]
    fw = g_v.shape[2]
    half = nf // 2

    def peer(r):
        return {"cp": lax.rem(c + (r // 2) % 2, 2), "tp": 2 * lax.rem(xx + r // 4, 2) + lax.rem(s + r % 2, 2)}

    def peer_dyn(r):
        return {"cp": lax.rem(c + lax.rem(r // 2, 2), 2), "tp": 2 * lax.rem(xx + r // 4, 2) + lax.rem(s + lax.rem(r, 2), 2)}

    bar = pltpu.get_barrier_semaphore()
    for r in range(1, 8):
        pl.semaphore_signal(bar, inc=1, device_id=peer(r), device_id_type=MESH)

    def wload(f, own):
        if own:
            sl = pl.ds(pl.multiple_of(f * fw, fw), fw)
            srcs = (wg.at[s, :, sl], wu.at[s, :, sl], wd.at[s, sl])
        else:
            sl = pl.ds(pl.multiple_of((f - half) * fw, fw), fw)
            srcs = (wg_r.at[:, sl], wu_r.at[:, sl], wd_r.at[sl])
        return [pltpu.make_async_copy(src, dst.at[f], w_sem.at[k, f]) for k, (src, dst) in enumerate(zip(srcs, (g_v, u_v, d_v)))]

    for f in range(nf):
        for cp_ in wload(f, f < half):
            cp_.start()

    ids_v = ids[...]
    rel = lax.rem(ids_v // 2 + xx, 2) * 4 + lax.rem(ids_v // 4 + c, 2) * 2 + lax.rem(ids_v + s, 2)
    ex_i = lax.broadcasted_iota(jnp.int32, (8, tok), 0)
    oh0 = (rel[0:1] == ex_i).astype(F32)
    oh1 = (rel[1:2] == ex_i).astype(F32)
    before = (lax.broadcasted_iota(jnp.int32, (tok, tok), 0) < lax.broadcasted_iota(jnp.int32, (tok, tok), 1)).astype(F32).astype(BF16)
    cum = dot(jnp.concatenate([oh0, oh1], axis=0).astype(BF16), before)
    base = ex_i.astype(F32) * cap
    tot0 = jnp.sum(oh0, axis=1, keepdims=True)
    slot0 = jnp.sum(oh0 * (base + cum[0:8]), axis=0, keepdims=True)
    slot1 = jnp.sum(oh1 * (base + tot0 + cum[8:16]), axis=0, keepdims=True)

    cap_i = lax.broadcasted_iota(jnp.int32, (cap, tok), 0).astype(F32)

    def block(r):
        want = cap_i + float(r * cap)
        sel = ((slot0 == want) | (slot1 == want)).astype(F32).astype(BF16)
        return dot(sel, h[...]).astype(BF16)

    def scopy(r):
        return remote(send.at[r], recv.at[r], s_s.at[r], s_r.at[r], **peer_dyn(r))

    def zcopy(r):
        return remote(zsend.at[r], zret.at[r], z_s.at[r], z_r.at[r], **peer_dyn(r))

    pl.semaphore_wait(bar, 7)
    for r in (4, 2, 5, 3, 1, 6, 7):
        send[r] = block(r)
        scopy(r).start()
    recv[0] = block(0)

    def group(gi, carry):
        g = lax.rem(gi, 2) * 2 + gi // 2
        @pl.when(gi > 0)
        def _():
            scopy(2 * g).wait_recv()
        scopy(2 * g + 1).wait_recv()
        xg = recv[pl.ds(2 * g, 2)].reshape(2 * cap, hid)
        zacc[...] = jnp.zeros(zacc.shape, F32)

        def fstep(f, cc):
            @pl.when(jnp.logical_and(gi == 0, f < half))
            def _():
                for cp_ in wload(f, True):
                    cp_.wait()

            @pl.when(jnp.logical_and(gi == 0, f >= half))
            def _():
                for cp_ in wload(f, False):
                    cp_.wait()

            gp = dot(xg, g_v[f])
            up = dot(xg, u_v[f])
            a = (jax.nn.silu(gp) * up).astype(BF16)
            zacc[...] += dot(a, d_v[f])
            return cc

        lax.fori_loop(0, nf, fstep, 0)
        z = zacc[...].astype(BF16)

        @pl.when(gi > 0)
        def _():
            zsend[2 * g] = z[:cap]
            zcopy(2 * g).start()

        @pl.when(gi == 0)
        def _():
            zret[0] = z[:cap]

        zsend[2 * g + 1] = z[cap:]
        zcopy(2 * g + 1).start()
        return carry

    lax.fori_loop(0, 4, group, 0)

    cols = jnp.concatenate([slot0, slot1, gates[...], jnp.zeros((4, tok), F32)], axis=0).T
    for r in range(1, 8):
        scopy(r).wait_send()
        zcopy(r).wait()
    slot_i = lax.broadcasted_iota(jnp.int32, (tok, 8 * cap), 1).astype(F32)
    z_all = zret[...].reshape(8 * cap, hid)
    y = h[...].astype(F32)
    for k in range(2):
        sel = (cols[:, k:k + 1] == slot_i).astype(F32).astype(BF16)
        y = y + cols[:, 2 + k:3 + k] * dot(sel, z_all)
    y_out[...] = y.astype(BF16)


def solution(mesh):
    row_spec = P(("dp", "cp", "tp"), None)
    head_spec = P(None, "tp", None)
    expert_spec = P(("cp", "tp"), None, None)
    any_spec = pl.BlockSpec(memory_space=pl.ANY)
    vm = pl.BlockSpec(memory_space=pltpu.VMEM)
    DMA = pltpu.SemaphoreType.DMA

    def device_step(x, w_q, w_k, w_v, w_o, ids, gates, w_gate, w_up, w_down):
        tok, hid = x.shape
        nr = tok // QT
        hd = w_q.shape[1] * w_q.shape[2]
        kd = w_k.shape[1] * w_k.shape[2]
        wq_t = w_q.transpose(1, 2, 0).reshape(hd, hid)
        wk_t = w_k.transpose(1, 2, 0).reshape(kd, hid)
        wv_t = w_v.transpose(1, 2, 0).reshape(kd, hid)
        wo = w_o.reshape(hd, hid)
        seq = 8 * tok
        npair = w_q.shape[1] // 2
        f = w_gate.shape[2]

        h, wg_r, wu_r, wd_r = pl.pallas_call(
            attn_kernel,
            out_shape=[
                jax.ShapeDtypeStruct((tok, hid), BF16),
                jax.ShapeDtypeStruct((hid, f), BF16),
                jax.ShapeDtypeStruct((hid, f), BF16),
                jax.ShapeDtypeStruct((f, hid), BF16),
            ],
            in_specs=[any_spec] * 8,
            out_specs=[vm, any_spec, any_spec, any_spec],
            scratch_shapes=[
                pltpu.VMEM((4, tok, hid), BF16),
                pltpu.VMEM((hd, hid), BF16),
                pltpu.VMEM((2 * kd, hid), BF16),
                pltpu.VMEM((4, hd, hid), BF16),
                pltpu.VMEM((4, 2 * kd, tok), BF16),
                pltpu.VMEM((4, 2 * kd, tok), BF16),
                pltpu.VMEM((2, seq, 128), BF16),
                pltpu.VMEM((kd, seq), BF16),
                pltpu.VMEM((4 * nr, npair, 128, 2 * QT), BF16),
                pltpu.VMEM((4 * nr, QT, hd), BF16),
                pltpu.VMEM((tok, 4 * hd), BF16),
                pltpu.VMEM((npair, 1, 2 * QT), F32),
                pltpu.VMEM((npair, 8, 2 * QT), F32),
                pltpu.VMEM((npair, 32, 2 * QT), F32),
                DMA((5,)), DMA((nr,)), DMA((nr,)), DMA, DMA, DMA((nr,)), DMA((nr,)),
                DMA((4,)), DMA((4,)), DMA((3,)), DMA((3,)), DMA((3,)), DMA((3,)),
                DMA((4 * nr,)), DMA((4, nr)),
            ],
            compiler_params=pltpu.CompilerParams(collective_id=0, has_side_effects=True, vmem_limit_bytes=60 * 1024 * 1024),
            name="attn",
        )(x, wq_t, wk_t, wv_t, wo, w_gate, w_up, w_down)

        cap = tok * 2 // 8
        fw = f // 4
        return pl.pallas_call(
            moe_kernel,
            out_shape=jax.ShapeDtypeStruct((tok, hid), BF16),
            in_specs=[vm, vm, vm] + [any_spec] * 6,
            out_specs=vm,
            scratch_shapes=[
                pltpu.VMEM((8, hid, fw), BF16),
                pltpu.VMEM((8, hid, fw), BF16),
                pltpu.VMEM((8, fw, hid), BF16),
                pltpu.VMEM((8, cap, hid), BF16),
                pltpu.VMEM((8, cap, hid), BF16),
                pltpu.VMEM((8, cap, hid), BF16),
                pltpu.VMEM((8, cap, hid), BF16),
                pltpu.VMEM((2 * cap, hid), F32),
                DMA((3, 8)), DMA((8,)), DMA((8,)), DMA((8,)), DMA((8,)),
            ],
            compiler_params=pltpu.CompilerParams(collective_id=1, has_side_effects=True, vmem_limit_bytes=63 * 1024 * 1024),
            name="moe",
        )(h, ids.T, gates.T, w_gate, w_up, w_down, wg_r, wu_r, wd_r)

    return jax.shard_map(device_step, mesh=mesh, in_specs=(row_spec, head_spec, head_spec, head_spec, P("tp", None, None), row_spec, row_spec, expert_spec, expert_spec, expert_spec), out_specs=row_spec, check_vma=False)
```

```python
import functools
import math

import jax
import jax.numpy as jnp
from jax import lax
from jax.experimental import pallas as pl
from jax.experimental.pallas import tpu as pltpu
from jax.sharding import PartitionSpec as P

MESH = pl.DeviceIdType.MESH
F32 = jnp.float32
BF16 = jnp.bfloat16

NT = (((1,), (1,)), ((), ()))
QT = 128
KC = 256


def dot(a, b):
    return jnp.dot(a, b, preferred_element_type=F32)


def dot_nt(a, b):
    return lax.dot_general(a, b, NT, preferred_element_type=F32)


def remote(src, dst, send, recv, **dev):
    return pltpu.make_async_remote_copy(src_ref=src, dst_ref=dst, send_sem=send, recv_sem=recv, device_id=dev, device_id_type=MESH)


def attn_kernel(x, wq_h, wk_h, wv_h, wo_h, wg, wu, wd,
                h_out, wg_r, wu_r, wd_r,
                xh, wq, wkv, wo, kvown, kvrecv, kaug, vt, qaug, osend, orecv, m_s, l_s, acc_s, s_s, mx_s,
                loc_sem, xf_s, xf_r, xp_s, xp_r, xw_s, xw_r, kv_s, kv_r, wo_s, wo_r, ew_s, ew_r, o_s, o_r):
    c = lax.axis_index("cp")
    t = lax.axis_index("tp")
    s = lax.rem(t, 2)
    part = t + 1 - 2 * s
    far = lax.rem(t + 2, 4)
    farp = lax.rem(part + 2, 4)
    cn = 1 - c
    tok = xh.shape[1]
    nr = tok // QT
    chunk = 2 * tok
    hid = x.shape[1]
    heads = wq_h.shape[0] // 32
    npair = heads // 2
    scale = 32 ** -0.5 * math.log2(math.e)

    bar = pltpu.get_barrier_semaphore()
    pl.semaphore_signal(bar, inc=1, device_id={"tp": part}, device_id_type=MESH)
    pl.semaphore_signal(bar, inc=1, device_id={"tp": far}, device_id_type=MESH)
    pl.semaphore_signal(bar, inc=1, device_id={"tp": farp}, device_id_type=MESH)
    pl.semaphore_signal(bar, inc=1, device_id={"cp": cn}, device_id_type=MESH)

    locs = [
        pltpu.make_async_copy(x, xh.at[t], loc_sem.at[0]),
        pltpu.make_async_copy(wq_h, wq, loc_sem.at[1]),
        pltpu.make_async_copy(wk_h, wkv.at[pl.ds(0, 64)], loc_sem.at[2]),
        pltpu.make_async_copy(wv_h, wkv.at[pl.ds(64, 64)], loc_sem.at[3]),
        pltpu.make_async_copy(wo_h, wo.at[t], loc_sem.at[4]),
    ]
    for cp_ in locs:
        cp_.start()
    pl.semaphore_wait(bar, 4)

    xfar = [remote(x.at[pl.ds(k * QT, QT)], xh.at[t, pl.ds(k * QT, QT)], xf_s.at[k], xf_r.at[k], tp=far) for k in range(nr)]
    xpart = remote(x, xh.at[t], xp_s, xp_r, tp=part)
    xfwd = [remote(xh.at[far, pl.ds(k * QT, QT)], xh.at[far, pl.ds(k * QT, QT)], xw_s.at[k], xw_r.at[k], tp=part) for k in range(nr)]
    for k in range(nr):
        xfar[k].start()
    xpart.start()

    qaug[:, :, 96:128, :] = jnp.zeros((qaug.shape[0], npair, 32, 2 * QT), BF16)

    def project(b):
        xb = xh[b]
        qt = dot_nt(wq[...], xb).astype(BF16)
        qs = qt.astype(F32) * scale
        h1 = qs.astype(BF16)
        r1 = qs - h1.astype(F32)
        h2 = r1.astype(BF16)
        h3 = (r1 - h2.astype(F32)).astype(BF16)
        for r in range(nr):
            for hd in range(heads):
                for k, part_v in enumerate((h1, h2, h3)):
                    qaug[b * nr + r, hd // 2, k * 32:(k + 1) * 32, (hd % 2) * QT:(hd % 2 + 1) * QT] = part_v[hd * 32:(hd + 1) * 32, r * QT:(r + 1) * QT]
        kvown[b] = dot_nt(wkv[...], xb).astype(BF16)

    def kvcopy(b):
        return remote(kvown.at[b], kvrecv.at[b], kv_s.at[b], kv_r.at[b], cp=cn)

    for cp_ in locs[:4]:
        cp_.wait()
    project(t)
    kvcopy(t).start()
    xpart.wait_recv()
    project(part)
    kvcopy(part).start()
    for k in range(nr):
        xfar[k].wait_recv()
        xfwd[k].start()
    project(far)
    kvcopy(far).start()
    for k in range(nr):
        xfwd[k].wait_recv()
    project(farp)
    kvcopy(farp).start()
    for k in range(nr):
        xfar[k].wait_send()
        xfwd[k].wait_send()
    xpart.wait_send()

    locs[4].wait()
    wofar = remote(wo_h, wo.at[t], wo_s.at[0], wo_r.at[0], tp=far)
    wopart = remote(wo_h, wo.at[t], wo_s.at[1], wo_r.at[1], tp=part)
    wofwd = remote(wo.at[far], wo.at[far], wo_s.at[2], wo_r.at[2], tp=part)
    wofar.start()
    wopart.start()

    zero_pad = jnp.zeros((32, tok), BF16)

    def place(b, src, cc):
        second = b // 2
        ck = cc * (1 - second) + (3 - cc) * second
        pos = pl.multiple_of(ck * chunk + lax.rem(b, 2) * tok, QT)
        kv = src[b]
        for g in range(2):
            kt = kv[g * 32:(g + 1) * 32]
            kaug[g, pl.ds(pos, tok), :] = jnp.concatenate([kt, kt, kt, zero_pad], axis=0).T
        vt[:, pl.ds(pos, tok)] = kv[64:128]

    def place_own(b, carry):
        place(b, kvown, c)
        return carry

    def place_recv(b, carry):
        kvcopy(b).wait_recv()
        place(b, kvrecv, cn)
        return carry

    lax.fori_loop(0, 4, place_own, 0)
    lax.fori_loop(0, 4, place_recv, 0)

    def ocopy(i, b, r):
        return remote(osend.at[i], orecv.at[pl.ds(r * QT, QT), pl.ds(t * tok, tok)], o_s.at[i], o_r.at[t, r], tp=b)

    def tile_of(ii):
        kk = ii // nr
        r = lax.rem(ii, nr)
        xb = lax.rem(t // 2 + 1 - kk // 2, 2)
        sb = lax.rem(s + lax.rem((kk + 1) // 2, 2), 2)
        return 2 * xb + sb, r

    def wcopy(ii):
        out = []
        for w, wr in ((wg, wg_r), (wu, wu_r)):
            n = w.shape[1] // (4 * nr)
            sl = pl.ds(pl.multiple_of(ii * n, n), n)
            k = 0 if w is wg else 1
            out.append(remote(w.at[1 - s, sl], wr.at[sl], ew_s.at[k], ew_r.at[k], tp=part))
        return out

    def wdcopy(ii):
        n = wd.shape[1] // 8
        sl = pl.ds(pl.multiple_of(ii * n, n), n)
        return remote(wd.at[1 - s, sl], wd_r.at[sl], ew_s.at[2], ew_r.at[2], tp=part)

    def fold_max(v):
        return jnp.max(v.reshape(KC // 8, 8, 2 * QT), axis=0)

    def score(p, i, j):
        return dot(kaug[p // (npair // 2), pl.ds(pl.multiple_of(j * KC, KC), KC), :], qaug[i, p])

    b0, r0 = tile_of(0)
    for p in range(npair):
        s_first = score(p, b0 * nr + r0, 0)
        s_s[p] = s_first
        mx_s[p] = fold_max(s_first)

    def tile(ii, carry):
        for cp_ in wcopy(ii):
            cp_.start()

        @pl.when(ii < 8)
        def _():
            wdcopy(ii).start()

        @pl.when(ii == 2 * nr)
        def _():
            wofar.wait_recv()
            wofwd.start()

        b, r = tile_of(ii)
        i = b * nr + r
        second = b // 2
        ck = c * (1 - second) + (3 - c) * second
        qpos = ck * chunk + lax.rem(b, 2) * tok + r * QT
        nfull = qpos // KC
        m_s[...] = jnp.full(m_s.shape, -jnp.inf, F32)
        l_s[...] = jnp.zeros(l_s.shape, F32)
        acc_s[...] = jnp.zeros(acc_s.shape, F32)

        def step(j, i_next, j_next, masked):
            k0 = pl.multiple_of(j * KC, KC)
            if masked:
                key_i = lax.broadcasted_iota(jnp.int32, (KC, 2 * QT), 0) + k0
                q_i = lax.rem(lax.broadcasted_iota(jnp.int32, (KC, 2 * QT), 1), QT) + qpos
                allowed = key_i <= q_i
            for p in range(npair):
                g = p // (npair // 2)
                s_next = score(p, i_next, j_next)
                sc = s_s[p]
                if masked:
                    sc = jnp.where(allowed, sc, -jnp.inf)
                    mx = fold_max(sc)
                else:
                    mx = mx_s[p]
                m_old = m_s[p]
                m_new = jnp.maximum(m_old, jnp.max(mx, axis=0, keepdims=True))
                alpha = jnp.exp2(m_old - m_new)
                pr = jnp.exp2(sc - m_new)
                l_s[p] = l_s[p] * alpha + jnp.sum(pr.reshape(KC // 8, 8, 2 * QT), axis=0)
                pv = dot(vt[g * 32:(g + 1) * 32, pl.ds(k0, KC)], pr.astype(BF16))
                acc_s[p] = acc_s[p] * alpha + pv
                m_s[p] = m_new
                s_s[p] = s_next
                mx_s[p] = fold_max(s_next)

        def body(j, cc):
            step(j, i, j + 1, False)
            return cc

        lax.fori_loop(0, nfull, body, 0)
        bn, rn = tile_of(jnp.minimum(ii + 1, 4 * nr - 1))
        step(nfull, bn * nr + rn, 0, True)

        pieces = []
        for p in range(npair):
            o = acc_s[p] / jnp.sum(l_s[p], axis=0, keepdims=True)
            pieces += [o[:, :QT], o[:, QT:]]
        tile_o = jnp.concatenate(pieces, axis=0).T.astype(BF16)

        @pl.when(ii < 3 * nr)
        def _():
            osend[i] = tile_o
            ocopy(i, b, r).start()

        @pl.when(ii >= 3 * nr)
        def _():
            orecv[pl.ds(pl.multiple_of(r * QT, QT), QT), pl.ds(pl.multiple_of(t * tok, QT), tok)] = tile_o
        return carry

    lax.fori_loop(0, 4 * nr, tile, 0)

    def odone(ii, carry):
        b, r = tile_of(ii)
        ocopy(b * nr + r, b, r).wait_send()
        remote(osend.at[0], orecv.at[pl.ds(pl.multiple_of(r * QT, QT), QT), pl.ds(pl.multiple_of(b * tok, QT), tok)], o_s.at[0], o_r.at[b, r], tp=b).wait_recv()
        return carry

    lax.fori_loop(0, 3 * nr, odone, 0)
    wofar.wait_send()
    wopart.wait()
    wofwd.wait()

    nt = hid // 4

    def proj_out(n, carry):
        sl = pl.ds(pl.multiple_of(n * nt, QT), nt)
        ow = dot(orecv[...], wo[:, :, sl].reshape(hid, nt))
        h_out[:, sl] = (xh[t, :, sl].astype(F32) + ow).astype(BF16)
        return carry

    lax.fori_loop(0, 4, proj_out, 0)

    def kvdone(b, carry):
        kvcopy(b).wait_send()
        return carry

    lax.fori_loop(0, 4, kvdone, 0)
    for k, (w, wr) in enumerate(((wg, wg_r), (wu, wu_r), (wd, wd_r))):
        remote(w.at[1 - s], wr, ew_s.at[k], ew_r.at[k], tp=part).wait()


def moe_kernel(h, ids, gates, wg, wu, wd, wg_r, wu_r, wd_r,
               y_out,
               g_v, u_v, d_v, send, recv, zsend, zret, zacc,
               w_sem, s_s, s_r, z_s, z_r):
    c = lax.axis_index("cp")
    t = lax.axis_index("tp")
    s = lax.rem(t, 2)
    xx = t // 2
    tok, hid = h.shape
    cap = recv.shape[1]
    nf = g_v.shape[0]
    fw = g_v.shape[2]
    half = nf // 2

    def peer(r):
        return {"cp": lax.rem(c + (r // 2) % 2, 2), "tp": 2 * lax.rem(xx + r // 4, 2) + lax.rem(s + r % 2, 2)}

    def peer_dyn(r):
        return {"cp": lax.rem(c + lax.rem(r // 2, 2), 2), "tp": 2 * lax.rem(xx + r // 4, 2) + lax.rem(s + lax.rem(r, 2), 2)}

    bar = pltpu.get_barrier_semaphore()
    for r in range(1, 8):
        pl.semaphore_signal(bar, inc=1, device_id=peer(r), device_id_type=MESH)

    def wload(f, own):
        if own:
            sl = pl.ds(pl.multiple_of(f * fw, fw), fw)
            srcs = (wg.at[s, :, sl], wu.at[s, :, sl], wd.at[s, sl])
        else:
            sl = pl.ds(pl.multiple_of((f - half) * fw, fw), fw)
            srcs = (wg_r.at[:, sl], wu_r.at[:, sl], wd_r.at[sl])
        return [pltpu.make_async_copy(src, dst.at[f], w_sem.at[k, f]) for k, (src, dst) in enumerate(zip(srcs, (g_v, u_v, d_v)))]

    for f in range(nf):
        for cp_ in wload(f, f < half):
            cp_.start()

    ids_v = ids[...]
    rel = lax.rem(ids_v // 2 + xx, 2) * 4 + lax.rem(ids_v // 4 + c, 2) * 2 + lax.rem(ids_v + s, 2)
    ex_i = lax.broadcasted_iota(jnp.int32, (8, tok), 0)
    oh0 = (rel[0:1] == ex_i).astype(F32)
    oh1 = (rel[1:2] == ex_i).astype(F32)
    before = (lax.broadcasted_iota(jnp.int32, (tok, tok), 0) < lax.broadcasted_iota(jnp.int32, (tok, tok), 1)).astype(F32).astype(BF16)
    cum = dot(jnp.concatenate([oh0, oh1], axis=0).astype(BF16), before)
    base = ex_i.astype(F32) * cap
    tot0 = jnp.sum(oh0, axis=1, keepdims=True)
    slot0 = jnp.sum(oh0 * (base + cum[0:8]), axis=0, keepdims=True)
    slot1 = jnp.sum(oh1 * (base + tot0 + cum[8:16]), axis=0, keepdims=True)

    cap_i = lax.broadcasted_iota(jnp.int32, (cap, tok), 0).astype(F32)

    def block(r):
        want = cap_i + float(r * cap)
        sel = ((slot0 == want) | (slot1 == want)).astype(F32).astype(BF16)
        return dot(sel, h[...]).astype(BF16)

    def scopy(r):
        return remote(send.at[r], recv.at[r], s_s.at[r], s_r.at[r], **peer_dyn(r))

    def zcopy(r):
        return remote(zsend.at[r], zret.at[r], z_s.at[r], z_r.at[r], **peer_dyn(r))

    pl.semaphore_wait(bar, 7)
    for r in (4, 2, 5, 3, 1, 6, 7):
        send[r] = block(r)
        scopy(r).start()
    recv[0] = block(0)

    def group(gi, carry):
        g = lax.rem(gi, 2) * 2 + gi // 2
        @pl.when(gi > 0)
        def _():
            scopy(2 * g).wait_recv()
        scopy(2 * g + 1).wait_recv()
        xg = recv[pl.ds(2 * g, 2)].reshape(2 * cap, hid)
        zacc[...] = jnp.zeros(zacc.shape, F32)

        def fstep(f, cc):
            @pl.when(jnp.logical_and(gi == 0, f < half))
            def _():
                for cp_ in wload(f, True):
                    cp_.wait()

            @pl.when(jnp.logical_and(gi == 0, f >= half))
            def _():
                for cp_ in wload(f, False):
                    cp_.wait()

            gp = dot(xg, g_v[f])
            up = dot(xg, u_v[f])
            a = (jax.nn.silu(gp) * up).astype(BF16)
            zacc[...] += dot(a, d_v[f])
            return cc

        lax.fori_loop(0, nf, fstep, 0)
        z = zacc[...].astype(BF16)

        @pl.when(gi > 0)
        def _():
            zsend[2 * g] = z[:cap]
            zcopy(2 * g).start()

        @pl.when(gi == 0)
        def _():
            zret[0] = z[:cap]

        zsend[2 * g + 1] = z[cap:]
        zcopy(2 * g + 1).start()
        return carry

    lax.fori_loop(0, 4, group, 0)

    cols = jnp.concatenate([slot0, slot1, gates[...], jnp.zeros((4, tok), F32)], axis=0).T
    for r in range(1, 8):
        scopy(r).wait_send()
        zcopy(r).wait()
    slot_i = lax.broadcasted_iota(jnp.int32, (tok, 8 * cap), 1).astype(F32)
    z_all = zret[...].reshape(8 * cap, hid)
    y = h[...].astype(F32)
    for k in range(2):
        sel = (cols[:, k:k + 1] == slot_i).astype(F32).astype(BF16)
        y = y + cols[:, 2 + k:3 + k] * dot(sel, z_all)
    y_out[...] = y.astype(BF16)


def solution(mesh):
    row_spec = P(("dp", "cp", "tp"), None)
    head_spec = P(None, "tp", None)
    expert_spec = P(("cp", "tp"), None, None)
    any_spec = pl.BlockSpec(memory_space=pl.ANY)
    vm = pl.BlockSpec(memory_space=pltpu.VMEM)
    DMA = pltpu.SemaphoreType.DMA

    def device_step(x, w_q, w_k, w_v, w_o, ids, gates, w_gate, w_up, w_down):
        tok, hid = x.shape
        nr = tok // QT
        hd = w_q.shape[1] * w_q.shape[2]
        kd = w_k.shape[1] * w_k.shape[2]
        wq_t = w_q.transpose(1, 2, 0).reshape(hd, hid)
        wk_t = w_k.transpose(1, 2, 0).reshape(kd, hid)
        wv_t = w_v.transpose(1, 2, 0).reshape(kd, hid)
        wo = w_o.reshape(hd, hid)
        seq = 8 * tok
        npair = w_q.shape[1] // 2
        f = w_gate.shape[2]

        h, wg_r, wu_r, wd_r = pl.pallas_call(
            attn_kernel,
            out_shape=[
                jax.ShapeDtypeStruct((tok, hid), BF16),
                jax.ShapeDtypeStruct((hid, f), BF16),
                jax.ShapeDtypeStruct((hid, f), BF16),
                jax.ShapeDtypeStruct((f, hid), BF16),
            ],
            in_specs=[any_spec] * 8,
            out_specs=[vm, any_spec, any_spec, any_spec],
            scratch_shapes=[
                pltpu.VMEM((4, tok, hid), BF16),
                pltpu.VMEM((hd, hid), BF16),
                pltpu.VMEM((2 * kd, hid), BF16),
                pltpu.VMEM((4, hd, hid), BF16),
                pltpu.VMEM((4, 2 * kd, tok), BF16),
                pltpu.VMEM((4, 2 * kd, tok), BF16),
                pltpu.VMEM((2, seq, 128), BF16),
                pltpu.VMEM((kd, seq), BF16),
                pltpu.VMEM((4 * nr, npair, 128, 2 * QT), BF16),
                pltpu.VMEM((4 * nr, QT, hd), BF16),
                pltpu.VMEM((tok, 4 * hd), BF16),
                pltpu.VMEM((npair, 1, 2 * QT), F32),
                pltpu.VMEM((npair, 8, 2 * QT), F32),
                pltpu.VMEM((npair, 32, 2 * QT), F32),
                pltpu.VMEM((npair, KC, 2 * QT), F32),
                pltpu.VMEM((npair, 8, 2 * QT), F32),
                DMA((5,)), DMA((nr,)), DMA((nr,)), DMA, DMA, DMA((nr,)), DMA((nr,)),
                DMA((4,)), DMA((4,)), DMA((3,)), DMA((3,)), DMA((3,)), DMA((3,)),
                DMA((4 * nr,)), DMA((4, nr)),
            ],
            compiler_params=pltpu.CompilerParams(collective_id=0, has_side_effects=True, vmem_limit_bytes=60 * 1024 * 1024),
            name="attn",
        )(x, wq_t, wk_t, wv_t, wo, w_gate, w_up, w_down)

        cap = tok * 2 // 8
        fw = f // 4
        return pl.pallas_call(
            moe_kernel,
            out_shape=jax.ShapeDtypeStruct((tok, hid), BF16),
            in_specs=[vm, vm, vm] + [any_spec] * 6,
            out_specs=vm,
            scratch_shapes=[
                pltpu.VMEM((8, hid, fw), BF16),
                pltpu.VMEM((8, hid, fw), BF16),
                pltpu.VMEM((8, fw, hid), BF16),
                pltpu.VMEM((8, cap, hid), BF16),
                pltpu.VMEM((8, cap, hid), BF16),
                pltpu.VMEM((8, cap, hid), BF16),
                pltpu.VMEM((8, cap, hid), BF16),
                pltpu.VMEM((2 * cap, hid), F32),
                DMA((3, 8)), DMA((8,)), DMA((8,)), DMA((8,)), DMA((8,)),
            ],
            compiler_params=pltpu.CompilerParams(collective_id=1, has_side_effects=True, vmem_limit_bytes=63 * 1024 * 1024),
            name="moe",
        )(h, ids.T, gates.T, w_gate, w_up, w_down, wg_r, wu_r, wd_r)

    return jax.shard_map(device_step, mesh=mesh, in_specs=(row_spec, head_spec, head_spec, head_spec, P("tp", None, None), row_spec, row_spec, expert_spec, expert_spec, expert_spec), out_specs=row_spec, check_vma=False)
```

```python
import functools
import math

import jax
import jax.numpy as jnp
from jax import lax
from jax.experimental import pallas as pl
from jax.experimental.pallas import tpu as pltpu
from jax.sharding import PartitionSpec as P

MESH = pl.DeviceIdType.MESH
F32 = jnp.float32
BF16 = jnp.bfloat16

NT = (((1,), (1,)), ((), ()))
QT = 128
KC = 256


def dot(a, b):
    return jnp.dot(a, b, preferred_element_type=F32)


def dot_nt(a, b):
    return lax.dot_general(a, b, NT, preferred_element_type=F32)


def remote(src, dst, send, recv, **dev):
    return pltpu.make_async_remote_copy(src_ref=src, dst_ref=dst, send_sem=send, recv_sem=recv, device_id=dev, device_id_type=MESH)


def attn_kernel(x, wq_h, wk_h, wv_h, wo_h, wg, wu, wd,
                h_out, wg_r, wu_r, wd_r,
                xh, wq, wkv, wo, kvown, kvrecv, kaug, vt, qaug, osend, orecv, m_s, l_s, acc_s, s_s, mx_s,
                loc_sem, xf_s, xf_r, xp_s, xp_r, xw_s, xw_r, kv_s, kv_r, wo_s, wo_r, ew_s, ew_r, o_s, o_r):
    c = lax.axis_index("cp")
    t = lax.axis_index("tp")
    s = lax.rem(t, 2)
    xx = t // 2
    part = t + 1 - 2 * s
    far = lax.rem(t + 2, 4)
    farp = lax.rem(part + 2, 4)
    cn = 1 - c
    tok, hid = x.shape
    nr = tok // QT
    nt = 2 * nr
    nk = 2 * tok // KC
    heads = wq_h.shape[0] // 32
    npair = heads // 2
    scale = 32 ** -0.5 * math.log2(math.e)

    lc = c + xx * (3 - 2 * c)
    rc = 3 - lc
    ln = cn + xx * (3 - 2 * cn)
    rn = 3 - ln
    pp = lax.rem(xx + c, 2)
    qq = 1 - pp

    bar = pltpu.get_barrier_semaphore()
    pl.semaphore_signal(bar, inc=1, device_id={"tp": part}, device_id_type=MESH)
    pl.semaphore_signal(bar, inc=1, device_id={"tp": far}, device_id_type=MESH)
    pl.semaphore_signal(bar, inc=1, device_id={"tp": farp}, device_id_type=MESH)
    pl.semaphore_signal(bar, inc=1, device_id={"cp": cn}, device_id_type=MESH)

    own_rows = pl.ds(pl.multiple_of(s * tok, QT), tok)
    locs = [
        pltpu.make_async_copy(x, xh.at[0, own_rows], loc_sem.at[0]),
        pltpu.make_async_copy(wq_h, wq, loc_sem.at[1]),
        pltpu.make_async_copy(wk_h, wkv.at[pl.ds(0, 64)], loc_sem.at[2]),
        pltpu.make_async_copy(wv_h, wkv.at[pl.ds(64, 64)], loc_sem.at[3]),
        pltpu.make_async_copy(wo_h, wo.at[t], loc_sem.at[4]),
    ]
    for cp_ in locs:
        cp_.start()
    pl.semaphore_wait(bar, 4)

    def piece(k, who):
        return pl.ds(pl.multiple_of((2 * k + who) * QT, QT), QT)

    def xfar(k):
        return remote(xh.at[0, piece(k, s)], xh.at[1, piece(k, s)], xf_s.at[k], xf_r.at[k], tp=far)

    def xfwd(k):
        return remote(xh.at[1, piece(k, s)], xh.at[1, piece(k, s)], xw_s.at[k], xw_r.at[k], tp=part)

    def xfwd_in(k):
        return remote(xh.at[1, piece(k, s)], xh.at[1, piece(k, 1 - s)], xw_s.at[k], xw_r.at[k], tp=part)

    hw = wo.shape[1] // 4

    def wo_rows(cc, n):
        return pl.ds(pl.multiple_of((2 * cc + n) * hw, hw), hw)

    def wofar(n):
        return remote(wo_h.at[wo_rows(c, n)], wo.at[t, wo_rows(c, n)], wo_s.at[n], wo_r.at[n], tp=far)

    def woy(n):
        return remote(wo.at[far, wo_rows(c, n)], wo.at[far, wo_rows(c, n)], wo_s.at[2 + n], wo_r.at[2 + n], cp=cn)

    def wofwd(n):
        return remote(wo.at[far, wo_rows(c, n)], wo.at[far, wo_rows(c, n)], wo_s.at[4 + n], wo_r.at[4 + n], tp=part)

    def wofwdy(n):
        return remote(wo.at[far, wo_rows(cn, n)], wo.at[far, wo_rows(cn, n)], wo_s.at[6 + n], wo_r.at[6 + n], tp=part)

    xpart = remote(x, xh.at[0, own_rows], xp_s, xp_r, tp=part)
    xpart.start()
    locs[0].wait()

    @pl.when(s == 0)
    def _():
        xfar(0).start()
        xfar(1).start()

    qaug[:, :, 96:128, :] = jnp.zeros((qaug.shape[0], npair, 32, 2 * QT), BF16)
    kaug[:, :, 96:128] = jnp.zeros((2, kaug.shape[1], 32), BF16)
    m_s[...] = jnp.full(m_s.shape, -jnp.inf, F32)
    l_s[...] = jnp.zeros(l_s.shape, F32)
    acc_s[...] = jnp.zeros(acc_s.shape, F32)

    zero_pad = jnp.zeros((32, KC), BF16)

    def place(kv, ck, k):
        pos = pl.multiple_of((ck * nk + k) * KC, KC)
        for g in range(2):
            kt = kv[g * 32:(g + 1) * 32]
            kaug[g, pl.ds(pos, KC), :] = jnp.concatenate([kt, kt, kt, zero_pad], axis=0).T
        vt[:, pl.ds(pos, KC)] = kv[64:128]

    def kvcopy(side, k):
        return remote(kvown.at[side, k], kvrecv.at[side, k], kv_s.at[side, k], kv_r.at[side, k], cp=cn)

    def project(side, k):
        xb = xh[side, pl.ds(pl.multiple_of(k * KC, KC), KC), :]
        kv = dot_nt(wkv[...], xb).astype(BF16)
        kvown[side, k] = kv
        kvcopy(side, k).start()
        place(kv, lc + side * (rc - lc), k)
        qt = dot_nt(wq[...], xb).astype(BF16)
        qs = qt.astype(F32) * scale
        h1 = qs.astype(BF16)
        r1 = qs - h1.astype(F32)
        h2 = r1.astype(BF16)
        h3 = (r1 - h2.astype(F32)).astype(BF16)
        for r in range(2):
            for hd in range(heads):
                for n, part_v in enumerate((h1, h2, h3)):
                    qaug[side * nt + 2 * k + r, hd // 2, n * 32:(n + 1) * 32, (hd % 2) * QT:(hd % 2 + 1) * QT] = part_v[hd * 32:(hd + 1) * 32, r * QT:(r + 1) * QT]

    for cp_ in locs[1:4]:
        cp_.wait()
    xpart.wait_recv()

    @pl.when(s == 1)
    def _():
        xfar(0).start()
        xfar(1).start()

    xfar(2).start()
    for n in range(2):
        wofar(n).start()

    def project_own(k, carry):
        project(0, k)
        return carry

    lax.fori_loop(0, nk, project_own, 0)

    wopart = remote(wo_h, wo.at[t], wo_s.at[8], wo_r.at[8], tp=part)
    wopart.start()

    e0 = 2 * nt + 3 * nt * pp
    e1 = e0 + 14 + 2 * qq
    e2 = e1 + 16 + 6 * qq
    njob = 78
    w0 = 8
    w1 = 60

    def pick(*pairs):
        out = pairs[-1][1]
        for cond, val in reversed(pairs[:-1]):
            out = jnp.where(cond, val, out)
        return out

    def job(i):
        k1 = pick((i < 2, 0), (i < 6, 1), (None, 2))
        v1 = i - k1 * (k1 + 1)
        v2 = i - 2 * nt
        k = pick((i < e1, 0), (i < e2, 1), (None, 2))
        u = i - pick((i < e1, e0), (i < e2, e1), (None, e2))
        nc2 = qq * 2 * k
        ua = jnp.where(u < 6, u, u - nc2)
        ub = u - 12 - nc2
        uc = ub - 2 * (k + 1)
        in1 = i < 2 * nt
        in2 = i < e0
        in_c2 = jnp.logical_and(u >= 6, u < 6 + nc2)
        in_a = u < 12 + nc2
        in_b = ub < 2 * (k + 1)
        first = xx == 0
        slot_a = jnp.where(first, nt + 2 * k + ua // 6, lax.rem(jnp.maximum(ua, 0), 6))
        ch_a = jnp.where(first, jnp.where(lax.rem(jnp.maximum(ua, 0), 6) < 3, lc, ln) * nk + lax.rem(jnp.maximum(ua, 0), 3), jnp.where(ua < 6, rc, rn) * nk + k)
        ubp = jnp.maximum(ub, 0)
        ucp = jnp.maximum(uc, 0)
        v2p = jnp.maximum(v2, 0)
        slot = pick((in1, 2 * k1 + lax.rem(jnp.maximum(v1, 0), 2)), (in2, v2p // 3), (in_c2, nt + u - 6), (in_a, slot_a), (in_b, nt + 2 * k + lax.rem(ubp, 2)), (None, nt + 2 * k + lax.rem(ucp, 2)))
        ch = pick((in1, lc * nk + v1 // 2), (in2, ln * nk + lax.rem(v2p, 3)), (in_c2, rn * nk + k), (in_a, ch_a), (in_b, rc * nk + ubp // 2), (None, rn * nk + ucp // 2))
        one, zero = jnp.int32(1), jnp.int32(0)
        masked = pick((in1, jnp.where(v1 // 2 == k1, one, zero)), (in2, zero), (in_a, zero), (in_b, jnp.where(ubp // 2 == k, one, zero)), (None, zero))
        last = jnp.where(k == 2, one, zero)
        fin = pick((in1, masked * (1 - xx) * qq), (in2, jnp.where(lax.rem(v2p, 3) == 2, 1 - xx, zero)), (in_c2, last), (in_a, last * xx * jnp.where(ua >= 6, one, zero)), (in_b, masked * pp), (None, last * jnp.where(ucp // 2 == 2, one, zero)))
        return slot, ch, masked, fin

    def fold_max(v):
        return jnp.max(v.reshape(KC // 8, 8, 2 * QT), axis=0)

    def score(p, slot, ch):
        return dot(kaug[p // (npair // 2), pl.ds(pl.multiple_of(ch * KC, KC), KC), :], qaug[slot, p])

    for p in range(npair):
        s_first = score(p, 0, lc * nk)
        s_s[p] = s_first
        mx_s[p] = fold_max(s_first)

    def wcopy(k, ii, n):
        w, wr = ((wg, wg_r), (wu, wu_r), (wd, wd_r))[k]
        sl = pl.ds(pl.multiple_of(ii * n, n), n)
        return remote(w.at[1 - s, sl], wr.at[sl], ew_s.at[k], ew_r.at[k], tp=part)

    def ocopy(slot, b, r):
        return remote(osend.at[slot], orecv.at[pl.ds(pl.multiple_of(r * QT, QT), QT), pl.ds(pl.multiple_of(t * tok, QT), tok)], o_s.at[slot], o_r.at[t, r], tp=b)

    def where_of(slot):
        u = lax.rem(slot, nt)
        chip = lax.rem(xx + slot // nt, 2)
        return 2 * chip + u // nr, lax.rem(u, nr)

    def step(i, carry):
        (slot, ch, masked, fin), following = carry
        slot_n, ch_n = following[:2]
        k_ev = pick((i < e1 - 1, 0), (i < e2 - 1, 1), (None, 2))
        e_ev = pick((i < e1 - 1, e0), (i < e2 - 1, e1), (None, e2))

        @pl.when(i == 2 * nt - 1)
        def _():
            def take(k, cc):
                kvcopy(0, k).wait_recv()
                place(kvrecv[0, k], ln, k)
                return cc
            lax.fori_loop(0, nk, take, 0)

        @pl.when(i == e_ev - 1)
        def _():
            xfar(k_ev).wait_recv()
            xfwd(k_ev).start()
            xfwd_in(k_ev).wait_recv()
            project(1, k_ev)

        @pl.when(i == w1)
        def _():
            locs[4].wait()
            for n in range(2):
                wofar(n).wait_recv()
                woy(n).start()
                wofwd(n).start()

        k_r = pick((i < e1, 0), (i < e2, 1), (None, 2))
        e_r = pick((i < e1, e0), (i < e2, e1), (None, e2))

        @pl.when(i == e_r + 5)
        def _():
            kvcopy(1, k_r).wait_recv()
            place(kvrecv[1, k_r], rn, k_r)

        wi = i - w0

        @pl.when(jnp.logical_and(wi >= 0, wi < 64))
        def _():
            wcopy(2, wi, wd.shape[1] // 64).start()

            @pl.when(lax.rem(wi, 2) == 0)
            def _():
                wcopy(0, wi // 2, wg.shape[1] // 32).start()

            @pl.when(lax.rem(wi, 2) == 1)
            def _():
                wcopy(1, wi // 2, wu.shape[1] // 32).start()

        @pl.when(masked == 1)
        def _():
            qpos = ((lc + (slot // nt) * (rc - lc)) * nt + lax.rem(slot, nt)) * QT
            key_i = lax.broadcasted_iota(jnp.int32, (KC, 2 * QT), 0) + ch * KC
            q_i = lax.rem(lax.broadcasted_iota(jnp.int32, (KC, 2 * QT), 1), QT) + qpos
            allowed = key_i <= q_i
            for p in range(npair):
                sc = jnp.where(allowed, s_s[p], -jnp.inf)
                s_s[p] = sc
                mx_s[p] = fold_max(sc)

        after = job(jnp.minimum(i + 2, njob - 1))
        k0 = pl.multiple_of(ch * KC, KC)
        for p in range(npair):
            g = p // (npair // 2)
            s_next = score(p, slot_n, ch_n)
            sc = s_s[p]
            m_old = m_s[slot, p]
            m_new = jnp.maximum(m_old, jnp.max(mx_s[p], axis=0, keepdims=True))
            alpha = jnp.exp2(m_old - m_new)
            pr = jnp.exp2(sc - m_new)
            l_s[slot, p] = l_s[slot, p] * alpha + jnp.sum(pr.reshape(KC // 8, 8, 2 * QT), axis=0)
            pv = dot(vt[g * 32:(g + 1) * 32, pl.ds(k0, KC)], pr.astype(BF16))
            acc_s[slot, p] = acc_s[slot, p] * alpha + pv
            m_s[slot, p] = m_new
            s_s[p] = s_next
            mx_s[p] = fold_max(s_next)

        @pl.when(fin == 1)
        def _():
            pieces = []
            for p in range(npair):
                o = acc_s[slot, p] / jnp.sum(l_s[slot, p], axis=0, keepdims=True)
                pieces += [o[:, :QT], o[:, QT:]]
            tile_o = jnp.concatenate(pieces, axis=0).T.astype(BF16)
            b, r = where_of(slot)

            @pl.when(b != t)
            def _():
                osend[slot] = tile_o
                ocopy(slot, b, r).start()

            @pl.when(b == t)
            def _():
                orecv[pl.ds(pl.multiple_of(r * QT, QT), QT), pl.ds(pl.multiple_of(t * tok, QT), tok)] = tile_o
        return following, after

    lax.fori_loop(0, njob, step, (job(jnp.int32(0)), job(jnp.int32(1))))

    for n in range(2):
        woy(n).wait_recv()
        wofwdy(n).start()

    def odone(slot, carry):
        b, r = where_of(slot)

        @pl.when(b != t)
        def _():
            ocopy(slot, b, r).wait_send()
            remote(osend.at[0], orecv.at[pl.ds(pl.multiple_of(r * QT, QT), QT), pl.ds(pl.multiple_of(b * tok, QT), tok)], o_s.at[0], o_r.at[b, r], tp=b).wait_recv()
        return carry

    lax.fori_loop(0, 2 * nt, odone, 0)
    wopart.wait()
    for n in range(2):
        wofar(n).wait_send()
        woy(n).wait_send()
        wofwd(n).wait()
        wofwdy(n).wait()

    nw = hid // 4

    def proj_out(n, carry):
        sl = pl.ds(pl.multiple_of(n * nw, QT), nw)
        ow = dot(orecv[...], wo[:, :, sl].reshape(hid, nw))
        h_out[:, sl] = (xh[0, own_rows, sl].astype(F32) + ow).astype(BF16)
        return carry

    lax.fori_loop(0, 4, proj_out, 0)

    def drain(k, carry):
        kvcopy(0, k).wait_send()
        kvcopy(1, k).wait_send()
        xfar(k).wait_send()
        xfwd(k).wait_send()
        return carry

    lax.fori_loop(0, nk, drain, 0)
    xpart.wait_send()
    for k, (w, wr) in enumerate(((wg, wg_r), (wu, wu_r), (wd, wd_r))):
        remote(w.at[1 - s], wr, ew_s.at[k], ew_r.at[k], tp=part).wait()


def moe_kernel(h, ids, gates, wg, wu, wd, wg_r, wu_r, wd_r,
               y_out,
               g_v, u_v, d_v, send, recv, zsend, zret, zacc,
               w_sem, s_s, s_r, z_s, z_r):
    c = lax.axis_index("cp")
    t = lax.axis_index("tp")
    s = lax.rem(t, 2)
    xx = t // 2
    tok, hid = h.shape
    cap = recv.shape[1]
    nf = g_v.shape[0]
    fw = g_v.shape[2]
    half = nf // 2

    def peer(r):
        return {"cp": lax.rem(c + (r // 2) % 2, 2), "tp": 2 * lax.rem(xx + r // 4, 2) + lax.rem(s + r % 2, 2)}

    def peer_dyn(r):
        return {"cp": lax.rem(c + lax.rem(r // 2, 2), 2), "tp": 2 * lax.rem(xx + r // 4, 2) + lax.rem(s + lax.rem(r, 2), 2)}

    bar = pltpu.get_barrier_semaphore()
    for r in range(1, 8):
        pl.semaphore_signal(bar, inc=1, device_id=peer(r), device_id_type=MESH)

    def wload(f, own):
        if own:
            sl = pl.ds(pl.multiple_of(f * fw, fw), fw)
            srcs = (wg.at[s, :, sl], wu.at[s, :, sl], wd.at[s, sl])
        else:
            sl = pl.ds(pl.multiple_of((f - half) * fw, fw), fw)
            srcs = (wg_r.at[:, sl], wu_r.at[:, sl], wd_r.at[sl])
        return [pltpu.make_async_copy(src, dst.at[f], w_sem.at[k, f]) for k, (src, dst) in enumerate(zip(srcs, (g_v, u_v, d_v)))]

    for f in range(nf):
        for cp_ in wload(f, f < half):
            cp_.start()

    ids_v = ids[...]
    rel = lax.rem(ids_v // 2 + xx, 2) * 4 + lax.rem(ids_v // 4 + c, 2) * 2 + lax.rem(ids_v + s, 2)
    ex_i = lax.broadcasted_iota(jnp.int32, (8, tok), 0)
    oh0 = (rel[0:1] == ex_i).astype(F32)
    oh1 = (rel[1:2] == ex_i).astype(F32)
    before = (lax.broadcasted_iota(jnp.int32, (tok, tok), 0) < lax.broadcasted_iota(jnp.int32, (tok, tok), 1)).astype(F32).astype(BF16)
    cum = dot(jnp.concatenate([oh0, oh1], axis=0).astype(BF16), before)
    base = ex_i.astype(F32) * cap
    tot0 = jnp.sum(oh0, axis=1, keepdims=True)
    slot0 = jnp.sum(oh0 * (base + cum[0:8]), axis=0, keepdims=True)
    slot1 = jnp.sum(oh1 * (base + tot0 + cum[8:16]), axis=0, keepdims=True)

    cap_i = lax.broadcasted_iota(jnp.int32, (cap, tok), 0).astype(F32)

    def block(r):
        want = cap_i + float(r * cap)
        sel = ((slot0 == want) | (slot1 == want)).astype(F32).astype(BF16)
        return dot(sel, h[...]).astype(BF16)

    def scopy(r):
        return remote(send.at[r], recv.at[r], s_s.at[r], s_r.at[r], **peer_dyn(r))

    def zcopy(r):
        return remote(zsend.at[r], zret.at[r], z_s.at[r], z_r.at[r], **peer_dyn(r))

    pl.semaphore_wait(bar, 7)
    for r in (4, 2, 5, 3, 1, 6, 7):
        send[r] = block(r)
        scopy(r).start()
    recv[0] = block(0)

    def group(gi, carry):
        g = lax.rem(gi, 2) * 2 + gi // 2
        @pl.when(gi > 0)
        def _():
            scopy(2 * g).wait_recv()
        scopy(2 * g + 1).wait_recv()
        xg = recv[pl.ds(2 * g, 2)].reshape(2 * cap, hid)
        zacc[...] = jnp.zeros(zacc.shape, F32)

        def fstep(f, cc):
            @pl.when(jnp.logical_and(gi == 0, f < half))
            def _():
                for cp_ in wload(f, True):
                    cp_.wait()

            @pl.when(jnp.logical_and(gi == 0, f >= half))
            def _():
                for cp_ in wload(f, False):
                    cp_.wait()

            gp = dot(xg, g_v[f])
            up = dot(xg, u_v[f])
            a = (jax.nn.silu(gp) * up).astype(BF16)
            zacc[...] += dot(a, d_v[f])
            return cc

        lax.fori_loop(0, nf, fstep, 0)
        z = zacc[...].astype(BF16)

        @pl.when(gi > 0)
        def _():
            zsend[2 * g] = z[:cap]
            zcopy(2 * g).start()

        @pl.when(gi == 0)
        def _():
            zret[0] = z[:cap]

        zsend[2 * g + 1] = z[cap:]
        zcopy(2 * g + 1).start()
        return carry

    lax.fori_loop(0, 4, group, 0)

    cols = jnp.concatenate([slot0, slot1, gates[...], jnp.zeros((4, tok), F32)], axis=0).T
    for r in range(1, 8):
        scopy(r).wait_send()
        zcopy(r).wait()
    slot_i = lax.broadcasted_iota(jnp.int32, (tok, 8 * cap), 1).astype(F32)
    z_all = zret[...].reshape(8 * cap, hid)
    y = h[...].astype(F32)
    for k in range(2):
        sel = (cols[:, k:k + 1] == slot_i).astype(F32).astype(BF16)
        y = y + cols[:, 2 + k:3 + k] * dot(sel, z_all)
    y_out[...] = y.astype(BF16)


def solution(mesh):
    row_spec = P(("dp", "cp", "tp"), None)
    head_spec = P(None, "tp", None)
    expert_spec = P(("cp", "tp"), None, None)
    any_spec = pl.BlockSpec(memory_space=pl.ANY)
    vm = pl.BlockSpec(memory_space=pltpu.VMEM)
    DMA = pltpu.SemaphoreType.DMA

    def device_step(x, w_q, w_k, w_v, w_o, ids, gates, w_gate, w_up, w_down):
        tok, hid = x.shape
        nr = tok // QT
        hd = w_q.shape[1] * w_q.shape[2]
        kd = w_k.shape[1] * w_k.shape[2]
        wq_t = w_q.transpose(1, 2, 0).reshape(hd, hid)
        wk_t = w_k.transpose(1, 2, 0).reshape(kd, hid)
        wv_t = w_v.transpose(1, 2, 0).reshape(kd, hid)
        wo = w_o.reshape(hd, hid)
        seq = 8 * tok
        nk = 2 * tok // KC
        npair = w_q.shape[1] // 2
        f = w_gate.shape[2]

        h, wg_r, wu_r, wd_r = pl.pallas_call(
            attn_kernel,
            out_shape=[
                jax.ShapeDtypeStruct((tok, hid), BF16),
                jax.ShapeDtypeStruct((hid, f), BF16),
                jax.ShapeDtypeStruct((hid, f), BF16),
                jax.ShapeDtypeStruct((f, hid), BF16),
            ],
            in_specs=[any_spec] * 8,
            out_specs=[vm, any_spec, any_spec, any_spec],
            scratch_shapes=[
                pltpu.VMEM((2, 2 * tok, hid), BF16),
                pltpu.VMEM((hd, hid), BF16),
                pltpu.VMEM((2 * kd, hid), BF16),
                pltpu.VMEM((4, hd, hid), BF16),
                pltpu.VMEM((2, nk, 2 * kd, KC), BF16),
                pltpu.VMEM((2, nk, 2 * kd, KC), BF16),
                pltpu.VMEM((2, seq, 128), BF16),
                pltpu.VMEM((kd, seq), BF16),
                pltpu.VMEM((4 * nr, npair, 128, 2 * QT), BF16),
                pltpu.VMEM((4 * nr, QT, hd), BF16),
                pltpu.VMEM((tok, 4 * hd), BF16),
                pltpu.VMEM((4 * nr, npair, 1, 2 * QT), F32),
                pltpu.VMEM((4 * nr, npair, 8, 2 * QT), F32),
                pltpu.VMEM((4 * nr, npair, 32, 2 * QT), F32),
                pltpu.VMEM((npair, KC, 2 * QT), F32),
                pltpu.VMEM((npair, 8, 2 * QT), F32),
                DMA((5,)), DMA((nk,)), DMA((nk,)), DMA, DMA, DMA((nk,)), DMA((nk,)),
                DMA((2, nk)), DMA((2, nk)), DMA((9,)), DMA((9,)), DMA((3,)), DMA((3,)),
                DMA((4 * nr,)), DMA((4, nr)),
            ],
            compiler_params=pltpu.CompilerParams(collective_id=0, has_side_effects=True, vmem_limit_bytes=60 * 1024 * 1024),
            name="attn",
        )(x, wq_t, wk_t, wv_t, wo, w_gate, w_up, w_down)

        cap = tok * 2 // 8
        fw = f // 4
        return pl.pallas_call(
            moe_kernel,
            out_shape=jax.ShapeDtypeStruct((tok, hid), BF16),
            in_specs=[vm, vm, vm] + [any_spec] * 6,
            out_specs=vm,
            scratch_shapes=[
                pltpu.VMEM((8, hid, fw), BF16),
                pltpu.VMEM((8, hid, fw), BF16),
                pltpu.VMEM((8, fw, hid), BF16),
                pltpu.VMEM((8, cap, hid), BF16),
                pltpu.VMEM((8, cap, hid), BF16),
                pltpu.VMEM((8, cap, hid), BF16),
                pltpu.VMEM((8, cap, hid), BF16),
                pltpu.VMEM((2 * cap, hid), F32),
                DMA((3, 8)), DMA((8,)), DMA((8,)), DMA((8,)), DMA((8,)),
            ],
            compiler_params=pltpu.CompilerParams(collective_id=1, has_side_effects=True, vmem_limit_bytes=63 * 1024 * 1024),
            name="moe",
        )(h, ids.T, gates.T, w_gate, w_up, w_down, wg_r, wu_r, wd_r)

    return jax.shard_map(device_step, mesh=mesh, in_specs=(row_spec, head_spec, head_spec, head_spec, P("tp", None, None), row_spec, row_spec, expert_spec, expert_spec, expert_spec), out_specs=row_spec, check_vma=False)
```

```python
import functools
import math

import jax
import jax.numpy as jnp
from jax import lax
from jax.experimental import pallas as pl
from jax.experimental.pallas import tpu as pltpu
from jax.sharding import PartitionSpec as P

MESH = pl.DeviceIdType.MESH
F32 = jnp.float32
BF16 = jnp.bfloat16

NT = (((1,), (1,)), ((), ()))
QT = 128
KC = 256


def dot(a, b):
    return jnp.dot(a, b, preferred_element_type=F32)


def dot_nt(a, b):
    return lax.dot_general(a, b, NT, preferred_element_type=F32)


def remote(src, dst, send, recv, **dev):
    return pltpu.make_async_remote_copy(src_ref=src, dst_ref=dst, send_sem=send, recv_sem=recv, device_id=dev, device_id_type=MESH)


def attn_kernel(x, wq_h, wk_h, wv_h, wo_h, wg, wu, wd,
                h_out, wg_r, wu_r, wd_r,
                xh, wq, wkv, wo, kvown, kvrecv, kaug, vt, qaug, osend, orecv, m_s, l_s, acc_s, s_s, mx_s, bias, eye,
                loc_sem, xf_s, xf_r, xp_s, xp_r, xw_s, xw_r, kv_s, kv_r, wo_s, wo_r, ew_s, ew_r, o_s, o_r):
    c = lax.axis_index("cp")
    t = lax.axis_index("tp")
    s = lax.rem(t, 2)
    xx = t // 2
    part = t + 1 - 2 * s
    far = lax.rem(t + 2, 4)
    farp = lax.rem(part + 2, 4)
    cn = 1 - c
    tok, hid = x.shape
    nr = tok // QT
    nt = 2 * nr
    nk = 2 * tok // KC
    heads = wq_h.shape[0] // 32
    npair = heads // 2
    scale = 32 ** -0.5 * math.log2(math.e)

    lc = c + xx * (3 - 2 * c)
    rc = 3 - lc
    ln = cn + xx * (3 - 2 * cn)
    rn = 3 - ln
    pp = lax.rem(xx + c, 2)
    qq = 1 - pp

    bar = pltpu.get_barrier_semaphore()
    pl.semaphore_signal(bar, inc=1, device_id={"tp": part}, device_id_type=MESH)
    pl.semaphore_signal(bar, inc=1, device_id={"tp": far}, device_id_type=MESH)
    pl.semaphore_signal(bar, inc=1, device_id={"tp": farp}, device_id_type=MESH)
    pl.semaphore_signal(bar, inc=1, device_id={"cp": cn}, device_id_type=MESH)

    own_rows = pl.ds(pl.multiple_of(s * tok, QT), tok)
    locs = [
        pltpu.make_async_copy(x, xh.at[0, own_rows], loc_sem.at[0]),
        pltpu.make_async_copy(wq_h, wq, loc_sem.at[1]),
        pltpu.make_async_copy(wk_h, wkv.at[pl.ds(0, 64)], loc_sem.at[2]),
        pltpu.make_async_copy(wv_h, wkv.at[pl.ds(64, 64)], loc_sem.at[3]),
        pltpu.make_async_copy(wo_h, wo.at[t], loc_sem.at[4]),
    ]
    for cp_ in locs:
        cp_.start()
    pl.semaphore_wait(bar, 4)

    def piece(k, who):
        return pl.ds(pl.multiple_of((2 * k + who) * QT, QT), QT)

    def xfar(k):
        return remote(xh.at[0, piece(k, s)], xh.at[1, piece(k, s)], xf_s.at[k], xf_r.at[k], tp=far)

    def xfwd(k):
        return remote(xh.at[1, piece(k, s)], xh.at[1, piece(k, s)], xw_s.at[k], xw_r.at[k], tp=part)

    def xfwd_in(k):
        return remote(xh.at[1, piece(k, s)], xh.at[1, piece(k, 1 - s)], xw_s.at[k], xw_r.at[k], tp=part)

    hw = wo.shape[1] // 4

    def wo_rows(cc, n):
        return pl.ds(pl.multiple_of((2 * cc + n) * hw, hw), hw)

    def wofar(n):
        return remote(wo_h.at[wo_rows(c, n)], wo.at[t, wo_rows(c, n)], wo_s.at[n], wo_r.at[n], tp=far)

    def woy(n):
        return remote(wo.at[far, wo_rows(c, n)], wo.at[far, wo_rows(c, n)], wo_s.at[2 + n], wo_r.at[2 + n], cp=cn)

    def wofwd(n):
        return remote(wo.at[far, wo_rows(c, n)], wo.at[far, wo_rows(c, n)], wo_s.at[4 + n], wo_r.at[4 + n], tp=part)

    def wofwdy(n):
        return remote(wo.at[far, wo_rows(cn, n)], wo.at[far, wo_rows(cn, n)], wo_s.at[6 + n], wo_r.at[6 + n], tp=part)

    xpart = remote(x, xh.at[0, own_rows], xp_s, xp_r, tp=part)
    xpart.start()
    locs[0].wait()

    @pl.when(s == 0)
    def _():
        xfar(0).start()
        xfar(1).start()

    qaug[:, :, 96:128, :] = jnp.zeros((qaug.shape[0], npair, 32, 2 * QT), BF16)
    kaug[:, :, 96:128] = jnp.zeros((2, kaug.shape[1], 32), BF16)
    m_s[...] = jnp.full(m_s.shape, -jnp.inf, F32)
    l_s[...] = jnp.zeros(l_s.shape, F32)
    acc_s[...] = jnp.zeros(acc_s.shape, F32)

    zero_pad = jnp.zeros((32, KC), BF16)

    key_i = lax.broadcasted_iota(jnp.int32, (KC, QT), 0)
    q_i = lax.broadcasted_iota(jnp.int32, (KC, QT), 1)
    bias[0] = jnp.zeros((KC, QT), BF16)
    for n in range(2):
        bias[1 + n] = jnp.where(key_i > q_i + n * QT, -3.38e38, 0.0).astype(BF16)
    eye[...] = (lax.broadcasted_iota(jnp.int32, (QT, 2 * QT), 0) == lax.rem(lax.broadcasted_iota(jnp.int32, (QT, 2 * QT), 1), QT)).astype(F32).astype(BF16)

    def place(kv, ck, k):
        pos = pl.multiple_of((ck * nk + k) * KC, KC)
        for g in range(2):
            kt = kv[g * 32:(g + 1) * 32]
            kaug[g, pl.ds(pos, KC), :] = jnp.concatenate([kt, kt, kt, zero_pad], axis=0).T
        vt[:, pl.ds(pos, KC)] = kv[64:128]

    def kvcopy(side, k):
        return remote(kvown.at[side, k], kvrecv.at[side, k], kv_s.at[side, k], kv_r.at[side, k], cp=cn)

    def project(side, k):
        xb = xh[side, pl.ds(pl.multiple_of(k * KC, KC), KC), :]
        kv = dot_nt(wkv[...], xb).astype(BF16)
        kvown[side, k] = kv
        kvcopy(side, k).start()
        place(kv, lc + side * (rc - lc), k)
        qt = dot_nt(wq[...], xb).astype(BF16)
        qs = qt.astype(F32) * scale
        h1 = qs.astype(BF16)
        r1 = qs - h1.astype(F32)
        h2 = r1.astype(BF16)
        h3 = (r1 - h2.astype(F32)).astype(BF16)
        for r in range(2):
            for hd in range(heads):
                for n, part_v in enumerate((h1, h2, h3)):
                    qaug[side * nt + 2 * k + r, hd // 2, n * 32:(n + 1) * 32, (hd % 2) * QT:(hd % 2 + 1) * QT] = part_v[hd * 32:(hd + 1) * 32, r * QT:(r + 1) * QT]

    for cp_ in locs[1:4]:
        cp_.wait()
    xpart.wait_recv()

    @pl.when(s == 1)
    def _():
        xfar(0).start()
        xfar(1).start()

    xfar(2).start()
    for n in range(2):
        wofar(n).start()

    def project_own(k, carry):
        project(0, k)
        return carry

    lax.fori_loop(0, nk, project_own, 0)

    wopart = remote(wo_h, wo.at[t], wo_s.at[8], wo_r.at[8], tp=part)
    wopart.start()

    e0 = 2 * nt + 3 * nt * pp
    e1 = e0 + 14 + 2 * qq
    e2 = e1 + 16 + 6 * qq
    njob = 78
    w0 = 8
    w1 = 52
    g_ev = (11, 24, 38)

    def pick(*pairs):
        out = pairs[-1][1]
        for cond, val in reversed(pairs[:-1]):
            out = jnp.where(cond, val, out)
        return out

    def job(i):
        k1 = pick((i < 2, 0), (i < 6, 1), (None, 2))
        v1 = i - k1 * (k1 + 1)
        v2 = i - 2 * nt
        k = pick((i < e1, 0), (i < e2, 1), (None, 2))
        u = i - pick((i < e1, e0), (i < e2, e1), (None, e2))
        nc2 = qq * 2 * k
        ua = jnp.where(u < 6, u, u - nc2)
        ub = u - 12 - nc2
        uc = ub - 2 * (k + 1)
        in1 = i < 2 * nt
        in2 = i < e0
        in_c2 = jnp.logical_and(u >= 6, u < 6 + nc2)
        in_a = u < 12 + nc2
        in_b = ub < 2 * (k + 1)
        first = xx == 0
        slot_a = jnp.where(first, nt + 2 * k + ua // 6, lax.rem(jnp.maximum(ua, 0), 6))
        ch_a = jnp.where(first, jnp.where(lax.rem(jnp.maximum(ua, 0), 6) < 3, lc, ln) * nk + lax.rem(jnp.maximum(ua, 0), 3), jnp.where(ua < 6, rc, rn) * nk + k)
        ubp = jnp.maximum(ub, 0)
        ucp = jnp.maximum(uc, 0)
        v2p = jnp.maximum(v2, 0)
        slot = pick((in1, 2 * k1 + lax.rem(jnp.maximum(v1, 0), 2)), (in2, v2p // 3), (in_c2, nt + u - 6), (in_a, slot_a), (in_b, nt + 2 * k + lax.rem(ubp, 2)), (None, nt + 2 * k + lax.rem(ucp, 2)))
        ch = pick((in1, lc * nk + v1 // 2), (in2, ln * nk + lax.rem(v2p, 3)), (in_c2, rn * nk + k), (in_a, ch_a), (in_b, rc * nk + ubp // 2), (None, rn * nk + ucp // 2))
        one, zero = jnp.int32(1), jnp.int32(0)
        masked = pick((in1, jnp.where(v1 // 2 == k1, one, zero)), (in2, zero), (in_a, zero), (in_b, jnp.where(ubp // 2 == k, one, zero)), (None, zero))
        last = jnp.where(k == 2, one, zero)
        fin = pick((in1, masked * (1 - xx) * qq), (in2, jnp.where(lax.rem(v2p, 3) == 2, 1 - xx, zero)), (in_c2, last), (in_a, last * xx * jnp.where(ua >= 6, one, zero)), (in_b, masked * pp), (None, last * jnp.where(ucp // 2 == 2, one, zero)))
        return slot, ch, masked * (1 + lax.rem(slot, 2)), fin

    def fold_max(v):
        return jnp.max(v.reshape(KC // 8, 8, 2 * QT), axis=0)

    def score(p, slot, ch, sel):
        keys = jnp.concatenate([kaug[p // (npair // 2), pl.ds(pl.multiple_of(ch * KC, KC), KC), :], bias[sel]], axis=1)
        return dot(keys, jnp.concatenate([qaug[slot, p], eye[...]], axis=0))

    for p in range(npair):
        s_first = score(p, 0, lc * nk, 1)
        s_s[p] = s_first
        mx_s[p] = fold_max(s_first)

    def wcopy(k, ii, n):
        w, wr = ((wg, wg_r), (wu, wu_r), (wd, wd_r))[k]
        sl = pl.ds(pl.multiple_of(ii * n, n), n)
        return remote(w.at[1 - s, sl], wr.at[sl], ew_s.at[k], ew_r.at[k], tp=part)

    def ocopy(slot, b, r):
        return remote(osend.at[slot], orecv.at[pl.ds(pl.multiple_of(r * QT, QT), QT), pl.ds(pl.multiple_of(t * tok, QT), tok)], o_s.at[slot], o_r.at[t, r], tp=b)

    def where_of(slot):
        u = lax.rem(slot, nt)
        chip = lax.rem(xx + slot // nt, 2)
        return 2 * chip + u // nr, lax.rem(u, nr)

    def attend(cur, nxt):
        slot, ch = cur[:2]
        k0 = pl.multiple_of(ch * KC, KC)
        for p in range(npair):
            g = p // (npair // 2)
            s_next = score(p, *nxt[:3])
            sc = s_s[p]
            m_old = m_s[slot, p]
            m_new = jnp.maximum(m_old, jnp.max(mx_s[p], axis=0, keepdims=True))
            alpha = jnp.exp2(m_old - m_new)
            pr = jnp.exp2(sc - m_new)
            l_s[slot, p] = l_s[slot, p] * alpha + jnp.sum(pr.reshape(KC // 8, 8, 2 * QT), axis=0)
            pv = dot(vt[g * 32:(g + 1) * 32, pl.ds(k0, KC)], pr.astype(BF16))
            acc_s[slot, p] = acc_s[slot, p] * alpha + pv
            m_s[slot, p] = m_new
            s_s[p] = s_next
            mx_s[p] = fold_max(s_next)

    def finish(slot):
        pieces = []
        for p in range(npair):
            o = acc_s[slot, p] / jnp.sum(l_s[slot, p], axis=0, keepdims=True)
            pieces += [o[:, :QT], o[:, QT:]]
        osend[slot] = jnp.concatenate(pieces, axis=0).T.astype(BF16)
        b, r = where_of(slot)

        @pl.when(b != t)
        def _():
            ocopy(slot, b, r).start()

        @pl.when(b == t)
        def _():
            orecv[pl.ds(pl.multiple_of(r * QT, QT), QT), pl.ds(pl.multiple_of(t * tok, QT), tok)] = osend[slot]

    g_step = [g // 2 for g in g_ev]
    r_step = [(e + 5) // 2 for e in (e0, e1, e2)]

    def any_of(m, steps):
        out = m == steps[0]
        for v in steps[1:]:
            out = jnp.logical_or(out, m == v)
        return out

    def step(m, carry):
        first, second = carry
        i = 2 * m

        @pl.when(any_of(m, g_step + r_step + [w1 // 2]))
        def _():
            @pl.when(m == nt - 1)
            def _():
                def take(k, cc):
                    kvcopy(0, k).wait_recv()
                    place(kvrecv[0, k], ln, k)
                    return cc
                lax.fori_loop(0, nk, take, 0)

            @pl.when(any_of(m, g_step))
            def _():
                k_ev = jnp.where(m <= g_step[0], 0, jnp.where(m <= g_step[1], 1, 2))
                xfar(k_ev).wait_recv()
                xfwd(k_ev).start()
                xfwd_in(k_ev).wait_recv()
                project(1, k_ev)

            @pl.when(m == w1 // 2)
            def _():
                locs[4].wait()
                for n in range(2):
                    wofar(n).wait_recv()
                    woy(n).start()
                    wofwd(n).start()

            @pl.when(any_of(m, r_step))
            def _():
                k_r = jnp.where(m <= r_step[0], 0, jnp.where(m <= r_step[1], 1, 2))
                kvcopy(1, k_r).wait_recv()
                place(kvrecv[1, k_r], rn, k_r)

        wi = m - w0 // 2

        @pl.when(jnp.logical_and(wi >= 0, wi < 32))
        def _():
            wcopy(0, wi, wg.shape[1] // 32).start()
            wcopy(1, wi, wu.shape[1] // 32).start()
            wcopy(2, wi, wd.shape[1] // 32).start()

        third = job(jnp.minimum(i + 2, njob - 1))
        fourth = job(jnp.minimum(i + 3, njob - 1))
        attend(first, second)
        attend(second, third)

        def done(n, cc):
            finish(first[0] + n * (second[0] - first[0]))
            return cc

        lax.fori_loop(1 - first[3], 1 + second[3], done, 0)
        return third, fourth

    lax.fori_loop(0, njob // 2, step, (job(jnp.int32(0)), job(jnp.int32(1))))

    for n in range(2):
        woy(n).wait_recv()
        wofwdy(n).start()

    def odone(slot, carry):
        b, r = where_of(slot)

        @pl.when(b != t)
        def _():
            ocopy(slot, b, r).wait_send()
            remote(osend.at[0], orecv.at[pl.ds(pl.multiple_of(r * QT, QT), QT), pl.ds(pl.multiple_of(b * tok, QT), tok)], o_s.at[0], o_r.at[b, r], tp=b).wait_recv()
        return carry

    lax.fori_loop(0, 2 * nt, odone, 0)
    wopart.wait()
    for n in range(2):
        wofar(n).wait_send()
        woy(n).wait_send()
        wofwd(n).wait()
        wofwdy(n).wait()

    nw = hid // 4

    def proj_out(n, carry):
        sl = pl.ds(pl.multiple_of(n * nw, QT), nw)
        ow = dot(orecv[...], wo[:, :, sl].reshape(hid, nw))
        h_out[:, sl] = (xh[0, own_rows, sl].astype(F32) + ow).astype(BF16)
        return carry

    lax.fori_loop(0, 4, proj_out, 0)

    def drain(k, carry):
        kvcopy(0, k).wait_send()
        kvcopy(1, k).wait_send()
        xfar(k).wait_send()
        xfwd(k).wait_send()
        return carry

    lax.fori_loop(0, nk, drain, 0)
    xpart.wait_send()
    for k, (w, wr) in enumerate(((wg, wg_r), (wu, wu_r), (wd, wd_r))):
        remote(w.at[1 - s], wr, ew_s.at[k], ew_r.at[k], tp=part).wait()


def moe_kernel(h, ids, gates, wg, wu, wd, wg_r, wu_r, wd_r,
               y_out,
               g_v, u_v, d_v, send, recv, zsend, zret, zacc,
               w_sem, s_s, s_r, z_s, z_r):
    c = lax.axis_index("cp")
    t = lax.axis_index("tp")
    s = lax.rem(t, 2)
    xx = t // 2
    tok, hid = h.shape
    cap = recv.shape[1]
    nf = g_v.shape[0]
    fw = g_v.shape[2]
    half = nf // 2

    def peer(r):
        return {"cp": lax.rem(c + (r // 2) % 2, 2), "tp": 2 * lax.rem(xx + r // 4, 2) + lax.rem(s + r % 2, 2)}

    def peer_dyn(r):
        return {"cp": lax.rem(c + lax.rem(r // 2, 2), 2), "tp": 2 * lax.rem(xx + r // 4, 2) + lax.rem(s + lax.rem(r, 2), 2)}

    bar = pltpu.get_barrier_semaphore()
    for r in range(1, 8):
        pl.semaphore_signal(bar, inc=1, device_id=peer(r), device_id_type=MESH)

    def wload(f, own):
        if own:
            sl = pl.ds(pl.multiple_of(f * fw, fw), fw)
            srcs = (wg.at[s, :, sl], wu.at[s, :, sl], wd.at[s, sl])
        else:
            sl = pl.ds(pl.multiple_of((f - half) * fw, fw), fw)
            srcs = (wg_r.at[:, sl], wu_r.at[:, sl], wd_r.at[sl])
        return [pltpu.make_async_copy(src, dst.at[f], w_sem.at[k, f]) for k, (src, dst) in enumerate(zip(srcs, (g_v, u_v, d_v)))]

    for f in range(nf):
        for cp_ in wload(f, f < half):
            cp_.start()

    ids_v = ids[...]
    rel = lax.rem(ids_v // 2 + xx, 2) * 4 + lax.rem(ids_v // 4 + c, 2) * 2 + lax.rem(ids_v + s, 2)
    ex_i = lax.broadcasted_iota(jnp.int32, (8, tok), 0)
    oh0 = (rel[0:1] == ex_i).astype(F32)
    oh1 = (rel[1:2] == ex_i).astype(F32)
    before = (lax.broadcasted_iota(jnp.int32, (tok, tok), 0) < lax.broadcasted_iota(jnp.int32, (tok, tok), 1)).astype(F32).astype(BF16)
    cum = dot(jnp.concatenate([oh0, oh1], axis=0).astype(BF16), before)
    base = ex_i.astype(F32) * cap
    tot0 = jnp.sum(oh0, axis=1, keepdims=True)
    slot0 = jnp.sum(oh0 * (base + cum[0:8]), axis=0, keepdims=True)
    slot1 = jnp.sum(oh1 * (base + tot0 + cum[8:16]), axis=0, keepdims=True)

    cap_i = lax.broadcasted_iota(jnp.int32, (cap, tok), 0).astype(F32)

    def block(r):
        want = cap_i + float(r * cap)
        sel = ((slot0 == want) | (slot1 == want)).astype(F32).astype(BF16)
        return dot(sel, h[...]).astype(BF16)

    def scopy(r):
        return remote(send.at[r], recv.at[r], s_s.at[r], s_r.at[r], **peer_dyn(r))

    def zcopy(r):
        return remote(zsend.at[r], zret.at[r], z_s.at[r], z_r.at[r], **peer_dyn(r))

    pl.semaphore_wait(bar, 7)
    for r in (4, 2, 5, 3, 1, 6, 7):
        send[r] = block(r)
        scopy(r).start()
    recv[0] = block(0)

    def group(gi, carry):
        g = lax.rem(gi, 2) * 2 + gi // 2
        @pl.when(gi > 0)
        def _():
            scopy(2 * g).wait_recv()
        scopy(2 * g + 1).wait_recv()
        xg = recv[pl.ds(2 * g, 2)].reshape(2 * cap, hid)
        zacc[...] = jnp.zeros(zacc.shape, F32)

        def fstep(f, cc):
            @pl.when(jnp.logical_and(gi == 0, f < half))
            def _():
                for cp_ in wload(f, True):
                    cp_.wait()

            @pl.when(jnp.logical_and(gi == 0, f >= half))
            def _():
                for cp_ in wload(f, False):
                    cp_.wait()

            gp = dot(xg, g_v[f])
            up = dot(xg, u_v[f])
            a = (jax.nn.silu(gp) * up).astype(BF16)
            zacc[...] += dot(a, d_v[f])
            return cc

        lax.fori_loop(0, nf, fstep, 0)
        z = zacc[...].astype(BF16)

        @pl.when(gi > 0)
        def _():
            zsend[2 * g] = z[:cap]
            zcopy(2 * g).start()

        @pl.when(gi == 0)
        def _():
            zret[0] = z[:cap]

        zsend[2 * g + 1] = z[cap:]
        zcopy(2 * g + 1).start()
        return carry

    lax.fori_loop(0, 4, group, 0)

    cols = jnp.concatenate([slot0, slot1, gates[...], jnp.zeros((4, tok), F32)], axis=0).T
    for r in range(1, 8):
        scopy(r).wait_send()
        zcopy(r).wait()
    slot_i = lax.broadcasted_iota(jnp.int32, (tok, 8 * cap), 1).astype(F32)
    z_all = zret[...].reshape(8 * cap, hid)
    y = h[...].astype(F32)
    for k in range(2):
        sel = (cols[:, k:k + 1] == slot_i).astype(F32).astype(BF16)
        y = y + cols[:, 2 + k:3 + k] * dot(sel, z_all)
    y_out[...] = y.astype(BF16)


def solution(mesh):
    row_spec = P(("dp", "cp", "tp"), None)
    head_spec = P(None, "tp", None)
    expert_spec = P(("cp", "tp"), None, None)
    any_spec = pl.BlockSpec(memory_space=pl.ANY)
    vm = pl.BlockSpec(memory_space=pltpu.VMEM)
    DMA = pltpu.SemaphoreType.DMA

    def device_step(x, w_q, w_k, w_v, w_o, ids, gates, w_gate, w_up, w_down):
        tok, hid = x.shape
        nr = tok // QT
        hd = w_q.shape[1] * w_q.shape[2]
        kd = w_k.shape[1] * w_k.shape[2]
        wq_t = w_q.transpose(1, 2, 0).reshape(hd, hid)
        wk_t = w_k.transpose(1, 2, 0).reshape(kd, hid)
        wv_t = w_v.transpose(1, 2, 0).reshape(kd, hid)
        wo = w_o.reshape(hd, hid)
        seq = 8 * tok
        nk = 2 * tok // KC
        npair = w_q.shape[1] // 2
        f = w_gate.shape[2]

        h, wg_r, wu_r, wd_r = pl.pallas_call(
            attn_kernel,
            out_shape=[
                jax.ShapeDtypeStruct((tok, hid), BF16),
                jax.ShapeDtypeStruct((hid, f), BF16),
                jax.ShapeDtypeStruct((hid, f), BF16),
                jax.ShapeDtypeStruct((f, hid), BF16),
            ],
            in_specs=[any_spec] * 8,
            out_specs=[vm, any_spec, any_spec, any_spec],
            scratch_shapes=[
                pltpu.VMEM((2, 2 * tok, hid), BF16),
                pltpu.VMEM((hd, hid), BF16),
                pltpu.VMEM((2 * kd, hid), BF16),
                pltpu.VMEM((4, hd, hid), BF16),
                pltpu.VMEM((2, nk, 2 * kd, KC), BF16),
                pltpu.VMEM((2, nk, 2 * kd, KC), BF16),
                pltpu.VMEM((2, seq, 128), BF16),
                pltpu.VMEM((kd, seq), BF16),
                pltpu.VMEM((4 * nr, npair, 128, 2 * QT), BF16),
                pltpu.VMEM((4 * nr, QT, hd), BF16),
                pltpu.VMEM((tok, 4 * hd), BF16),
                pltpu.VMEM((4 * nr, npair, 1, 2 * QT), F32),
                pltpu.VMEM((4 * nr, npair, 8, 2 * QT), F32),
                pltpu.VMEM((4 * nr, npair, 32, 2 * QT), F32),
                pltpu.VMEM((npair, KC, 2 * QT), F32),
                pltpu.VMEM((npair, 8, 2 * QT), F32),
                pltpu.VMEM((3, KC, QT), BF16),
                pltpu.VMEM((QT, 2 * QT), BF16),
                DMA((5,)), DMA((nk,)), DMA((nk,)), DMA, DMA, DMA((nk,)), DMA((nk,)),
                DMA((2, nk)), DMA((2, nk)), DMA((9,)), DMA((9,)), DMA((3,)), DMA((3,)),
                DMA((4 * nr,)), DMA((4, nr)),
            ],
            compiler_params=pltpu.CompilerParams(collective_id=0, has_side_effects=True, vmem_limit_bytes=60 * 1024 * 1024),
            name="attn",
        )(x, wq_t, wk_t, wv_t, wo, w_gate, w_up, w_down)

        cap = tok * 2 // 8
        fw = f // 4
        return pl.pallas_call(
            moe_kernel,
            out_shape=jax.ShapeDtypeStruct((tok, hid), BF16),
            in_specs=[vm, vm, vm] + [any_spec] * 6,
            out_specs=vm,
            scratch_shapes=[
                pltpu.VMEM((8, hid, fw), BF16),
                pltpu.VMEM((8, hid, fw), BF16),
                pltpu.VMEM((8, fw, hid), BF16),
                pltpu.VMEM((8, cap, hid), BF16),
                pltpu.VMEM((8, cap, hid), BF16),
                pltpu.VMEM((8, cap, hid), BF16),
                pltpu.VMEM((8, cap, hid), BF16),
                pltpu.VMEM((2 * cap, hid), F32),
                DMA((3, 8)), DMA((8,)), DMA((8,)), DMA((8,)), DMA((8,)),
            ],
            compiler_params=pltpu.CompilerParams(collective_id=1, has_side_effects=True, vmem_limit_bytes=63 * 1024 * 1024),
            name="moe",
        )(h, ids.T, gates.T, w_gate, w_up, w_down, wg_r, wu_r, wd_r)

    return jax.shard_map(device_step, mesh=mesh, in_specs=(row_spec, head_spec, head_spec, head_spec, P("tp", None, None), row_spec, row_spec, expert_spec, expert_spec, expert_spec), out_specs=row_spec, check_vma=False)
```

```python
import functools
import math

import jax
import jax.numpy as jnp
from jax import lax
from jax.experimental import pallas as pl
from jax.experimental.pallas import tpu as pltpu
from jax.sharding import PartitionSpec as P

MESH = pl.DeviceIdType.MESH
F32 = jnp.float32
BF16 = jnp.bfloat16

NT = (((1,), (1,)), ((), ()))
QT = 128
KC = 256
QW = QT + QT


def dot(a, b):
    return jnp.dot(a, b, preferred_element_type=F32)


def dot_nt(a, b):
    return lax.dot_general(a, b, NT, preferred_element_type=F32)


def remote(src, dst, send, recv, **dev):
    return pltpu.make_async_remote_copy(src_ref=src, dst_ref=dst, send_sem=send, recv_sem=recv, device_id=dev, device_id_type=MESH)


def attn_kernel(x, wq_h, wk_h, wv_h, wo_h, wg, wu, wd,
                h_out, wg_r, wu_r, wd_r,
                xh, wq, wkv, wo, kvown, kvrecv, kaug, vt, qaug, osend, orecv, m_s, l_s, acc_s, s_s, mx_s, bias, eye,
                loc_sem, xf_s, xf_r, xp_s, xp_r, xw_s, xw_r, kv_s, kv_r, wo_s, wo_r, ew_s, ew_r, o_s, o_r):
    c = lax.axis_index("cp")
    t = lax.axis_index("tp")
    s = lax.rem(t, 2)
    xx = t // 2
    part = t + 1 - 2 * s
    far = lax.rem(t + 2, 4)
    farp = lax.rem(part + 2, 4)
    cn = 1 - c
    tok, hid = x.shape
    nr = tok // QT
    nt = 2 * nr
    nk = 2 * tok // KC
    heads = wq_h.shape[0] // 32
    npair = heads // 2
    scale = 32 ** -0.5 * math.log2(math.e)

    lc = c + xx * (3 - 2 * c)
    rc = 3 - lc
    ln = cn + xx * (3 - 2 * cn)
    rn = 3 - ln
    pp = lax.rem(xx + c, 2)
    qq = 1 - pp

    bar = pltpu.get_barrier_semaphore()
    for dev in ({"tp": part}, {"tp": far}, {"tp": farp}, {"cp": cn}):
        pl.semaphore_signal(bar, device_id=dev, device_id_type=MESH)

    own_rows = pl.ds(pl.multiple_of(s * tok, QT), tok)
    locs = [
        pltpu.make_async_copy(x, xh.at[0, own_rows], loc_sem.at[0]),
        pltpu.make_async_copy(wq_h, wq, loc_sem.at[1]),
        pltpu.make_async_copy(wk_h, wkv.at[pl.ds(0, 64)], loc_sem.at[2]),
        pltpu.make_async_copy(wv_h, wkv.at[pl.ds(64, 64)], loc_sem.at[3]),
        pltpu.make_async_copy(wo_h, wo.at[t], loc_sem.at[4]),
    ]
    for cp_ in locs:
        cp_.start()
    pl.semaphore_wait(bar, 4)

    def piece(k, who):
        return pl.ds(pl.multiple_of((2 * k + who) * QT, QT), QT)

    def xfar(k):
        return remote(xh.at[0, piece(k, s)], xh.at[1, piece(k, s)], xf_s.at[k], xf_r.at[k], tp=far)

    def xfwd(k):
        return remote(xh.at[1, piece(k, s)], xh.at[1, piece(k, s)], xw_s.at[k], xw_r.at[k], tp=part)

    def xfwd_in(k):
        return remote(xh.at[1, piece(k, s)], xh.at[1, piece(k, 1 - s)], xw_s.at[k], xw_r.at[k], tp=part)

    hw = wo.shape[1] // 4

    def wo_rows(cc, n):
        return pl.ds(pl.multiple_of((2 * cc + n) * hw, hw), hw)

    def wofar(n):
        return remote(wo_h.at[wo_rows(c, n)], wo.at[t, wo_rows(c, n)], wo_s.at[n], wo_r.at[n], tp=far)

    def woy(n):
        return remote(wo.at[far, wo_rows(c, n)], wo.at[far, wo_rows(c, n)], wo_s.at[2 + n], wo_r.at[2 + n], cp=cn)

    def wofwd(n):
        return remote(wo.at[far, wo_rows(c, n)], wo.at[far, wo_rows(c, n)], wo_s.at[4 + n], wo_r.at[4 + n], tp=part)

    def wofwdy(n):
        return remote(wo.at[far, wo_rows(cn, n)], wo.at[far, wo_rows(cn, n)], wo_s.at[6 + n], wo_r.at[6 + n], tp=part)

    xpart = remote(x, xh.at[0, own_rows], xp_s, xp_r, tp=part)
    xpart.start()
    locs[0].wait()

    @pl.when(s == 0)
    def _():
        xfar(0).start()
        xfar(1).start()

    qaug[:, :, 96:128, :] = jnp.zeros((qaug.shape[0], npair, 32, QW), BF16)
    kaug[:, :, 96:128] = jnp.zeros((2, kaug.shape[1], 32), BF16)
    m_s[...] = jnp.full(m_s.shape, -jnp.inf, F32)
    l_s[...] = jnp.zeros(l_s.shape, F32)
    acc_s[...] = jnp.zeros(acc_s.shape, F32)

    zero_pad = jnp.zeros((32, KC), BF16)

    key_i = lax.broadcasted_iota(jnp.int32, (KC, QT), 0)
    q_i = lax.broadcasted_iota(jnp.int32, (KC, QT), 1)
    bias[0] = jnp.zeros((KC, QT), BF16)
    for n in range(2):
        bias[1 + n] = jnp.where(key_i > q_i + n * QT, -3.38e38, 0.0).astype(BF16)
    eye[...] = (lax.broadcasted_iota(jnp.int32, (QT, QW), 0) == lax.rem(lax.broadcasted_iota(jnp.int32, (QT, QW), 1), QT)).astype(F32).astype(BF16)

    def place(kv, ck, k):
        pos = pl.multiple_of((ck * nk + k) * KC, KC)
        for g in range(2):
            kt = kv[g * 32:(g + 1) * 32]
            kaug[g, pl.ds(pos, KC), :] = jnp.concatenate([kt, kt, kt, zero_pad], axis=0).T
        vt[:, pl.ds(pos, KC)] = kv[64:128]

    def kvcopy(side, k):
        return remote(kvown.at[side, k], kvrecv.at[side, k], kv_s.at[side, k], kv_r.at[side, k], cp=cn)

    def project(side, k):
        xb = xh[side, pl.ds(pl.multiple_of(k * KC, KC), KC), :]
        kv = dot_nt(wkv[...], xb).astype(BF16)
        kvown[side, k] = kv
        kvcopy(side, k).start()
        place(kv, lc + side * (rc - lc), k)
        qt = dot_nt(wq[...], xb).astype(BF16)
        qs = qt.astype(F32) * scale
        h1 = qs.astype(BF16)
        r1 = qs - h1.astype(F32)
        h2 = r1.astype(BF16)
        h3 = (r1 - h2.astype(F32)).astype(BF16)
        for r in range(2):
            for hd in range(heads):
                for n, part_v in enumerate((h1, h2, h3)):
                    qaug[side * nt + 2 * k + r, hd // 2, n * 32:(n + 1) * 32, (hd % 2) * QT:(hd % 2 + 1) * QT] = part_v[hd * 32:(hd + 1) * 32, r * QT:(r + 1) * QT]

    for cp_ in locs[1:4]:
        cp_.wait()
    xpart.wait_recv()

    @pl.when(s == 1)
    def _():
        xfar(0).start()
        xfar(1).start()

    xfar(2).start()
    for n in range(2):
        wofar(n).start()

    def project_own(k, carry):
        project(0, k)
        return carry

    lax.fori_loop(0, nk, project_own, 0)

    wopart = remote(wo_h, wo.at[t], wo_s.at[8], wo_r.at[8], tp=part)
    wopart.start()

    e0 = 2 * nt + 3 * nt * pp
    e1 = e0 + 14 + 2 * qq
    e2 = e1 + 16 + 6 * qq
    njob = 78
    w0 = 8
    w1 = 52
    g_ev = (11, 24, 38)

    def pick(*pairs):
        out = pairs[-1][1]
        for cond, val in reversed(pairs[:-1]):
            out = jnp.where(cond, val, out)
        return out

    def job(i):
        k1 = pick((i < 2, 0), (i < 6, 1), (None, 2))
        v1 = i - k1 * (k1 + 1)
        v2 = i - 2 * nt
        k = pick((i < e1, 0), (i < e2, 1), (None, 2))
        u = i - pick((i < e1, e0), (i < e2, e1), (None, e2))
        nc2 = qq * 2 * k
        ua = jnp.where(u < 6, u, u - nc2)
        ub = u - 12 - nc2
        uc = ub - 2 * (k + 1)
        in1 = i < 2 * nt
        in2 = i < e0
        in_c2 = jnp.logical_and(u >= 6, u < 6 + nc2)
        in_a = u < 12 + nc2
        in_b = ub < 2 * (k + 1)
        first = xx == 0
        slot_a = jnp.where(first, nt + 2 * k + ua // 6, lax.rem(jnp.maximum(ua, 0), 6))
        ch_a = jnp.where(first, jnp.where(lax.rem(jnp.maximum(ua, 0), 6) < 3, lc, ln) * nk + lax.rem(jnp.maximum(ua, 0), 3), jnp.where(ua < 6, rc, rn) * nk + k)
        ubp = jnp.maximum(ub, 0)
        ucp = jnp.maximum(uc, 0)
        v2p = jnp.maximum(v2, 0)
        slot = pick((in1, 2 * k1 + lax.rem(jnp.maximum(v1, 0), 2)), (in2, v2p // 3), (in_c2, nt + u - 6), (in_a, slot_a), (in_b, nt + 2 * k + lax.rem(ubp, 2)), (None, nt + 2 * k + lax.rem(ucp, 2)))
        ch = pick((in1, lc * nk + v1 // 2), (in2, ln * nk + lax.rem(v2p, 3)), (in_c2, rn * nk + k), (in_a, ch_a), (in_b, rc * nk + ubp // 2), (None, rn * nk + ucp // 2))
        one, zero = jnp.int32(1), jnp.int32(0)
        masked = pick((in1, jnp.where(v1 // 2 == k1, one, zero)), (in2, zero), (in_a, zero), (in_b, jnp.where(ubp // 2 == k, one, zero)), (None, zero))
        last = jnp.where(k == 2, one, zero)
        fin = pick((in1, masked * (1 - xx) * qq), (in2, jnp.where(lax.rem(v2p, 3) == 2, 1 - xx, zero)), (in_c2, last), (in_a, last * xx * jnp.where(ua >= 6, one, zero)), (in_b, masked * pp), (None, last * jnp.where(ucp // 2 == 2, one, zero)))
        return slot, ch, masked * (1 + lax.rem(slot, 2)), fin

    def fold_max(v):
        return jnp.max(v.reshape(KC // 8, 8, QW), axis=0)

    def score(p, slot, ch, sel):
        keys = jnp.concatenate([kaug[p // (npair // 2), pl.ds(pl.multiple_of(ch * KC, KC), KC), :], bias[sel]], axis=1)
        return dot(keys, jnp.concatenate([qaug[slot, p], eye[...]], axis=0))

    for p in range(npair):
        s_first = score(p, 0, lc * nk, 1)
        s_s[p] = s_first
        mx_s[p] = fold_max(s_first)

    def wcopy(k, ii, n):
        w, wr = ((wg, wg_r), (wu, wu_r), (wd, wd_r))[k]
        sl = pl.ds(pl.multiple_of(ii * n, n), n)
        return remote(w.at[1 - s, sl], wr.at[sl], ew_s.at[k], ew_r.at[k], tp=part)

    def ocopy(slot, b, r):
        return remote(osend.at[slot], orecv.at[pl.ds(pl.multiple_of(r * QT, QT), QT), pl.ds(pl.multiple_of(t * tok, QT), tok)], o_s.at[slot], o_r.at[t, r], tp=b)

    def where_of(slot):
        u = lax.rem(slot, nt)
        chip = lax.rem(xx + slot // nt, 2)
        return 2 * chip + u // nr, lax.rem(u, nr)

    def attend(cur, nxt):
        slot, ch = cur[:2]
        k0 = pl.multiple_of(ch * KC, KC)
        for p in range(npair):
            g = p // (npair // 2)
            s_next = score(p, *nxt[:3])
            sc = s_s[p]
            m_old = m_s[slot, p]
            m_new = jnp.maximum(m_old, jnp.max(mx_s[p], axis=0, keepdims=True))
            alpha = jnp.exp2(m_old - m_new)
            pr = jnp.exp2(sc - m_new)
            l_s[slot, p] = l_s[slot, p] * alpha + jnp.sum(pr.reshape(KC // 8, 8, QW), axis=0)
            pv = dot(vt[g * 32:(g + 1) * 32, pl.ds(k0, KC)], pr.astype(BF16))
            acc_s[slot, p] = acc_s[slot, p] * alpha + pv
            m_s[slot, p] = m_new
            s_s[p] = s_next
            mx_s[p] = fold_max(s_next)

    def finish(slot):
        pieces = []
        for p in range(npair):
            o = acc_s[slot, p] / jnp.sum(l_s[slot, p], axis=0, keepdims=True)
            pieces += [o[:, :QT], o[:, QT:]]
        osend[slot] = jnp.concatenate(pieces, axis=0).T.astype(BF16)
        b, r = where_of(slot)

        @pl.when(b != t)
        def _():
            ocopy(slot, b, r).start()

        @pl.when(b == t)
        def _():
            orecv[pl.ds(pl.multiple_of(r * QT, QT), QT), pl.ds(pl.multiple_of(t * tok, QT), tok)] = osend[slot]

    g_step = [g // 2 for g in g_ev]
    r_step = [(e + 5) // 2 for e in (e0, e1, e2)]

    def any_of(m, steps):
        out = m == steps[0]
        for v in steps[1:]:
            out = jnp.logical_or(out, m == v)
        return out

    def step(m, carry):
        first, second = carry
        i = 2 * m

        @pl.when(any_of(m, g_step + r_step + [w1 // 2]))
        def _():
            @pl.when(m == nt - 1)
            def _():
                def take(k, cc):
                    kvcopy(0, k).wait_recv()
                    place(kvrecv[0, k], ln, k)
                    return cc
                lax.fori_loop(0, nk, take, 0)

            @pl.when(any_of(m, g_step))
            def _():
                k_ev = jnp.where(m <= g_step[0], 0, jnp.where(m <= g_step[1], 1, 2))
                xfar(k_ev).wait_recv()
                xfwd(k_ev).start()
                xfwd_in(k_ev).wait_recv()
                project(1, k_ev)

            @pl.when(m == w1 // 2)
            def _():
                locs[4].wait()
                for n in range(2):
                    wofar(n).wait_recv()
                    woy(n).start()
                    wofwd(n).start()

            @pl.when(any_of(m, r_step))
            def _():
                k_r = jnp.where(m <= r_step[0], 0, jnp.where(m <= r_step[1], 1, 2))
                kvcopy(1, k_r).wait_recv()
                place(kvrecv[1, k_r], rn, k_r)

        wi = m - w0 // 2

        @pl.when(jnp.logical_and(wi >= 0, wi < 32))
        def _():
            wcopy(0, wi, wg.shape[1] // 32).start()
            wcopy(1, wi, wu.shape[1] // 32).start()
            wcopy(2, wi, wd.shape[1] // 32).start()

        third = job(jnp.minimum(i + 2, njob - 1))
        fourth = job(jnp.minimum(i + 3, njob - 1))
        attend(first, second)
        attend(second, third)

        def done(n, cc):
            finish(first[0] + n * (second[0] - first[0]))
            return cc

        lax.fori_loop(1 - first[3], 1 + second[3], done, 0)
        return third, fourth

    lax.fori_loop(0, njob // 2, step, (job(jnp.int32(0)), job(jnp.int32(1))))

    for n in range(2):
        woy(n).wait_recv()
        wofwdy(n).start()

    def odone(slot, carry):
        b, r = where_of(slot)

        @pl.when(b != t)
        def _():
            ocopy(slot, b, r).wait_send()
            remote(osend.at[0], orecv.at[pl.ds(pl.multiple_of(r * QT, QT), QT), pl.ds(pl.multiple_of(b * tok, QT), tok)], o_s.at[0], o_r.at[b, r], tp=b).wait_recv()
        return carry

    lax.fori_loop(0, 2 * nt, odone, 0)
    wopart.wait()
    for n in range(2):
        wofar(n).wait_send()
        woy(n).wait_send()
        wofwd(n).wait()
        wofwdy(n).wait()

    nw = hid // 4

    def proj_out(n, carry):
        sl = pl.ds(pl.multiple_of(n * nw, QT), nw)
        ow = dot(orecv[...], wo[:, :, sl].reshape(hid, nw))
        h_out[:, sl] = (xh[0, own_rows, sl].astype(F32) + ow).astype(BF16)
        return carry

    lax.fori_loop(0, 4, proj_out, 0)

    def drain(k, carry):
        kvcopy(0, k).wait_send()
        kvcopy(1, k).wait_send()
        xfar(k).wait_send()
        xfwd(k).wait_send()
        return carry

    lax.fori_loop(0, nk, drain, 0)
    xpart.wait_send()
    for k, (w, wr) in enumerate(((wg, wg_r), (wu, wu_r), (wd, wd_r))):
        remote(w.at[1 - s], wr, ew_s.at[k], ew_r.at[k], tp=part).wait()


def moe_kernel(h, ids, gates, wg, wu, wd, wg_r, wu_r, wd_r,
               y_out,
               g_v, u_v, d_v, send, recv, zsend, zret, zacc, y_acc,
               w_sem, s_s, s_r, z_s, z_r):
    c = lax.axis_index("cp")
    t = lax.axis_index("tp")
    s = lax.rem(t, 2)
    xx = t // 2
    tok, hid = h.shape
    cap = recv.shape[1]
    nf = g_v.shape[0]
    fw = g_v.shape[2]
    half = nf // 2

    def peer(r):
        diag = r // 6
        mid = jnp.logical_and(r >= 2, r < 6)
        dy = jnp.where(mid, lax.rem(r, 2), diag)
        dx = jnp.where(mid, 1 - dy, diag)
        ds = jnp.where(mid, r // 2 - 1, lax.rem(r, 2))
        return {"cp": lax.rem(c + dy, 2), "tp": 2 * lax.rem(xx + dx, 2) + lax.rem(s + ds, 2)}

    bar = pltpu.get_barrier_semaphore()
    for r in range(1, 8):
        pl.semaphore_signal(bar, device_id=peer(jnp.int32(r)), device_id_type=MESH)

    def wload(f, own):
        if own:
            sl = pl.ds(pl.multiple_of(f * fw, fw), fw)
            srcs = (wg.at[s, :, sl], wu.at[s, :, sl], wd.at[s, sl])
        else:
            sl = pl.ds(pl.multiple_of((f - half) * fw, fw), fw)
            srcs = (wg_r.at[:, sl], wu_r.at[:, sl], wd_r.at[sl])
        return [pltpu.make_async_copy(src, dst.at[f], w_sem.at[k, f]) for k, (src, dst) in enumerate(zip(srcs, (g_v, u_v, d_v)))]

    for f in range(nf):
        for cp_ in wload(f, f < half):
            cp_.start()

    ids_v = ids[...]
    dx = lax.rem(ids_v // 2 + xx, 2)
    dy = lax.rem(ids_v // 4 + c, 2)
    ds = lax.rem(ids_v + s, 2)
    rel = jnp.where(dx == dy, 6 * dx + ds, 2 + 2 * ds + dy)
    ex_i = lax.broadcasted_iota(jnp.int32, (8, tok), 0)
    oh0 = (rel[0:1] == ex_i).astype(F32)
    oh1 = (rel[1:2] == ex_i).astype(F32)
    before = (lax.broadcasted_iota(jnp.int32, (tok, tok), 0) < lax.broadcasted_iota(jnp.int32, (tok, tok), 1)).astype(F32).astype(BF16)
    cum = dot(jnp.concatenate([oh0, oh1], axis=0).astype(BF16), before)
    base = ex_i.astype(F32) * cap
    tot0 = jnp.sum(oh0, axis=1, keepdims=True)
    slot0 = jnp.sum(oh0 * (base + cum[0:8]), axis=0, keepdims=True)
    slot1 = jnp.sum(oh1 * (base + tot0 + cum[8:16]), axis=0, keepdims=True)

    cap_i = lax.broadcasted_iota(jnp.int32, (cap, tok), 0).astype(F32)

    def block(r):
        want = cap_i + float(r * cap)
        sel = ((slot0 == want) | (slot1 == want)).astype(F32).astype(BF16)
        return dot(sel, h[...]).astype(BF16)

    def scopy(r):
        return remote(send.at[r], recv.at[r], s_s.at[r], s_r.at[r], **peer(r))

    def zcopy(r):
        return remote(zsend.at[r], zret.at[r], z_s.at[r], z_r.at[r], **peer(r))

    pl.semaphore_wait(bar, 7)
    for r in (2, 3, 1, 4, 5, 6, 7):
        send[r] = block(r)
        scopy(jnp.int32(r)).start()
    recv[0] = block(0)

    def group(g, carry):
        @pl.when(g > 0)
        def _():
            scopy(2 * g).wait_recv()
        scopy(2 * g + 1).wait_recv()
        xg = recv[pl.ds(2 * g, 2)].reshape(2 * cap, hid)
        zacc[...] = jnp.zeros(zacc.shape, F32)

        def fstep(f, cc):
            @pl.when(jnp.logical_and(g == 0, f < half))
            def _():
                for cp_ in wload(f, True):
                    cp_.wait()

            @pl.when(jnp.logical_and(g == 0, f >= half))
            def _():
                for cp_ in wload(f, False):
                    cp_.wait()

            gp = dot(xg, g_v[f])
            up = dot(xg, u_v[f])
            a = (jax.nn.silu(gp) * up).astype(BF16)
            zacc[...] += dot(a, d_v[f])
            return cc

        lax.fori_loop(0, nf, fstep, 0)
        z = zacc[...].astype(BF16)

        @pl.when(g > 0)
        def _():
            zsend[2 * g] = z[:cap]
            zcopy(2 * g).start()

        @pl.when(g == 0)
        def _():
            zret[0] = z[:cap]

        zsend[2 * g + 1] = z[cap:]
        zcopy(2 * g + 1).start()
        return carry

    lax.fori_loop(0, 4, group, 0)

    cols = jnp.concatenate([slot0, slot1, gates[...], jnp.zeros((4, tok), F32)], axis=0).T
    slot_i = lax.broadcasted_iota(jnp.int32, (tok, 2 * cap), 1).astype(F32)

    def combine(g, y):
        z = zret[pl.ds(2 * g, 2)].reshape(2 * cap, hid)
        want = slot_i + (2 * cap * g).astype(F32)
        for k in range(2):
            sel = (cols[:, k:k + 1] == want).astype(F32).astype(BF16)
            y = y + cols[:, 2 + k:3 + k] * dot(sel, z)
        return y

    def returned(g, cc):
        @pl.when(g > 0)
        def _():
            scopy(2 * g).wait_send()
            zcopy(2 * g).wait()
        scopy(2 * g + 1).wait_send()
        zcopy(2 * g + 1).wait()

        @pl.when(g < 3)
        def _():
            y_acc[...] = combine(g, y_acc[...])
        return cc

    y_acc[...] = h[...].astype(F32)
    lax.fori_loop(0, 4, returned, 0)
    y_out[...] = combine(jnp.int32(3), y_acc[...]).astype(BF16)


def solution(mesh):
    row_spec = P(("dp", "cp", "tp"), None)
    head_spec = P(None, "tp", None)
    expert_spec = P(("cp", "tp"), None, None)
    any_spec = pl.BlockSpec(memory_space=pl.ANY)
    vm = pl.BlockSpec(memory_space=pltpu.VMEM)
    DMA = pltpu.SemaphoreType.DMA

    def device_step(x, w_q, w_k, w_v, w_o, ids, gates, w_gate, w_up, w_down):
        tok, hid = x.shape
        nr = tok // QT
        hd = w_q.shape[1] * w_q.shape[2]
        kd = w_k.shape[1] * w_k.shape[2]
        wq_t = w_q.transpose(1, 2, 0).reshape(hd, hid)
        wk_t = w_k.transpose(1, 2, 0).reshape(kd, hid)
        wv_t = w_v.transpose(1, 2, 0).reshape(kd, hid)
        wo = w_o.reshape(hd, hid)
        seq = 8 * tok
        nk = 2 * tok // KC
        npair = w_q.shape[1] // 2
        f = w_gate.shape[2]

        h, wg_r, wu_r, wd_r = pl.pallas_call(
            attn_kernel,
            out_shape=[
                jax.ShapeDtypeStruct((tok, hid), BF16),
                jax.ShapeDtypeStruct((hid, f), BF16),
                jax.ShapeDtypeStruct((hid, f), BF16),
                jax.ShapeDtypeStruct((f, hid), BF16),
            ],
            in_specs=[any_spec] * 8,
            out_specs=[vm, any_spec, any_spec, any_spec],
            scratch_shapes=[
                pltpu.VMEM((2, 2 * tok, hid), BF16),
                pltpu.VMEM((hd, hid), BF16),
                pltpu.VMEM((2 * kd, hid), BF16),
                pltpu.VMEM((4, hd, hid), BF16),
                *[pltpu.VMEM((2, nk, 2 * kd, KC), BF16)] * 2,
                pltpu.VMEM((2, seq, 128), BF16),
                pltpu.VMEM((kd, seq), BF16),
                pltpu.VMEM((4 * nr, npair, 128, QW), BF16),
                pltpu.VMEM((4 * nr, QT, hd), BF16),
                pltpu.VMEM((tok, 4 * hd), BF16),
                pltpu.VMEM((4 * nr, npair, 1, QW), F32),
                pltpu.VMEM((4 * nr, npair, 8, QW), F32),
                pltpu.VMEM((4 * nr, npair, 32, QW), F32),
                pltpu.VMEM((npair, KC, QW), F32),
                pltpu.VMEM((npair, 8, QW), F32),
                pltpu.VMEM((3, KC, QT), BF16),
                pltpu.VMEM((QT, QW), BF16),
                DMA((5,)), *[DMA((nk,))] * 2, DMA, DMA, *[DMA((nk,))] * 2,
                *[DMA((2, nk))] * 2, *[DMA((9,))] * 2, *[DMA((3,))] * 2,
                DMA((4 * nr,)), DMA((4, nr)),
            ],
            compiler_params=pltpu.CompilerParams(collective_id=0, has_side_effects=True, vmem_limit_bytes=60 * 1024 * 1024),
            name="attn",
        )(x, wq_t, wk_t, wv_t, wo, w_gate, w_up, w_down)

        cap = tok * 2 // 8
        fw = f // 2
        nf = 2 * f // fw
        n_dev = 8
        return pl.pallas_call(
            moe_kernel,
            out_shape=jax.ShapeDtypeStruct((tok, hid), BF16),
            in_specs=[vm, vm, vm] + [any_spec] * 6,
            out_specs=vm,
            scratch_shapes=[
                pltpu.VMEM((nf, hid, fw), BF16),
                pltpu.VMEM((nf, hid, fw), BF16),
                pltpu.VMEM((nf, fw, hid), BF16),
                *[pltpu.VMEM((n_dev, cap, hid), BF16)] * 4,
                pltpu.VMEM((2 * cap, hid), F32),
                pltpu.VMEM((tok, hid), F32),
                DMA((3, nf)), *[DMA((n_dev,))] * 4,
            ],
            compiler_params=pltpu.CompilerParams(collective_id=1, has_side_effects=True, vmem_limit_bytes=63 * 1024 * 1024),
            name="moe",
        )(h, ids.T, gates.T, w_gate, w_up, w_down, wg_r, wu_r, wd_r)

    return jax.shard_map(device_step, mesh=mesh, in_specs=(row_spec, head_spec, head_spec, head_spec, P("tp", None, None), row_spec, row_spec, expert_spec, expert_spec, expert_spec), out_specs=row_spec, check_vma=False)
```

```python
import functools
import math

import jax
import jax.numpy as jnp
from jax import lax
from jax.experimental import pallas as pl
from jax.experimental.pallas import tpu as pltpu
from jax.sharding import PartitionSpec as P

MESH = pl.DeviceIdType.MESH
F32 = jnp.float32
BF16 = jnp.bfloat16

NT = (((1,), (1,)), ((), ()))
QT = 128
KC = 256
QW = QT + QT


def dot(a, b):
    return jnp.dot(a, b, preferred_element_type=F32)


def dot_nt(a, b):
    return lax.dot_general(a, b, NT, preferred_element_type=F32)


def remote(src, dst, send, recv, **dev):
    return pltpu.make_async_remote_copy(src_ref=src, dst_ref=dst, send_sem=send, recv_sem=recv, device_id=dev, device_id_type=MESH)


def attn_kernel(x, wq_h, wk_h, wv_h, wo_h, wg, wu, wd,
                h_out, wg_r, wu_r, wd_r,
                xh, wq, wkv, wo, kvown, kvrecv, kaug, vt, qaug, osend, orecv, m_s, l_s, acc_s, s_s, mx_s, bias, eye, h_s,
                loc_sem, xf_s, xf_r, xp_s, xp_r, xw_s, xw_r, kv_s, kv_r, wo_s, wo_r, ew_s, ew_r, o_s, o_r):
    c = lax.axis_index("cp")
    t = lax.axis_index("tp")
    s = lax.rem(t, 2)
    xx = t // 2
    part = t + 1 - 2 * s
    far = lax.rem(t + 2, 4)
    farp = lax.rem(part + 2, 4)
    cn = 1 - c
    tok, hid = x.shape
    nr = tok // QT
    nt = 2 * nr
    nk = 2 * tok // KC
    heads = wq_h.shape[0] // 32
    npair = heads // 2
    scale = 32 ** -0.5 * math.log2(math.e)

    lc = c + xx * (3 - 2 * c)
    rc = 3 - lc
    ln = cn + xx * (3 - 2 * cn)
    rn = 3 - ln
    pp = lax.rem(xx + c, 2)
    qq = 1 - pp

    bar = pltpu.get_barrier_semaphore()
    for dev in ({"tp": part}, {"tp": far}, {"tp": farp}, {"cp": cn}):
        pl.semaphore_signal(bar, device_id=dev, device_id_type=MESH)

    own_rows = pl.ds(pl.multiple_of(s * tok, QT), tok)
    locs = [
        pltpu.make_async_copy(x, xh.at[0, own_rows], loc_sem.at[0]),
        pltpu.make_async_copy(wq_h, wq, loc_sem.at[1]),
        pltpu.make_async_copy(wk_h, wkv.at[pl.ds(0, 64)], loc_sem.at[2]),
        pltpu.make_async_copy(wv_h, wkv.at[pl.ds(64, 64)], loc_sem.at[3]),
        pltpu.make_async_copy(wo_h, wo.at[t], loc_sem.at[4]),
    ]
    for cp_ in locs:
        cp_.start()
    pl.semaphore_wait(bar, 4)

    def piece(k, who):
        return pl.ds(pl.multiple_of((2 * k + who) * QT, QT), QT)

    def xfar(k):
        return remote(xh.at[0, piece(k, s)], xh.at[1, piece(k, s)], xf_s.at[k], xf_r.at[k], tp=far)

    def xfwd(k):
        return remote(xh.at[1, piece(k, s)], xh.at[1, piece(k, s)], xw_s.at[k], xw_r.at[k], tp=part)

    def xfwd_in(k):
        return remote(xh.at[1, piece(k, s)], xh.at[1, piece(k, 1 - s)], xw_s.at[k], xw_r.at[k], tp=part)

    hw = wo.shape[1] // 4

    def wo_rows(cc, n):
        return pl.ds(pl.multiple_of((2 * cc + n) * hw, hw), hw)

    def wofar(n):
        return remote(wo_h.at[wo_rows(c, n)], wo.at[t, wo_rows(c, n)], wo_s.at[n], wo_r.at[n], tp=far)

    def woy(n):
        return remote(wo.at[far, wo_rows(c, n)], wo.at[far, wo_rows(c, n)], wo_s.at[2 + n], wo_r.at[2 + n], cp=cn)

    def wofwd(n):
        return remote(wo.at[far, wo_rows(c, n)], wo.at[far, wo_rows(c, n)], wo_s.at[4 + n], wo_r.at[4 + n], tp=part)

    def wofwdy(n):
        return remote(wo.at[far, wo_rows(cn, n)], wo.at[far, wo_rows(cn, n)], wo_s.at[6 + n], wo_r.at[6 + n], tp=part)

    xpart = remote(x, xh.at[0, own_rows], xp_s, xp_r, tp=part)
    xpart.start()
    locs[0].wait()

    @pl.when(s == 0)
    def _():
        xfar(0).start()
        xfar(1).start()

    qaug[:, :, 96:128, :] = jnp.zeros((qaug.shape[0], npair, 32, QW), BF16)
    kaug[:, :, 96:128] = jnp.zeros((2, kaug.shape[1], 32), BF16)
    m_s[...] = jnp.full(m_s.shape, -jnp.inf, F32)
    l_s[...] = jnp.zeros(l_s.shape, F32)
    acc_s[...] = jnp.zeros(acc_s.shape, F32)

    zero_pad = jnp.zeros((32, KC), BF16)

    key_i = lax.broadcasted_iota(jnp.int32, (KC, QT), 0)
    q_i = lax.broadcasted_iota(jnp.int32, (KC, QT), 1)
    bias[0] = jnp.zeros((KC, QT), BF16)
    for n in range(2):
        bias[1 + n] = jnp.where(key_i > q_i + n * QT, -3.38e38, 0.0).astype(BF16)
    eye[...] = (lax.broadcasted_iota(jnp.int32, (QT, QW), 0) == lax.rem(lax.broadcasted_iota(jnp.int32, (QT, QW), 1), QT)).astype(F32).astype(BF16)

    def place(kv, ck, k):
        pos = pl.multiple_of((ck * nk + k) * KC, KC)
        for g in range(2):
            kt = kv[g * 32:(g + 1) * 32]
            kaug[g, pl.ds(pos, KC), :] = jnp.concatenate([kt, kt, kt, zero_pad], axis=0).T
        vt[:, pl.ds(pos, KC)] = kv[64:128]

    def kvcopy(side, k):
        return remote(kvown.at[side, k], kvrecv.at[side, k], kv_s.at[side, k], kv_r.at[side, k], cp=cn)

    def project(side, k):
        xb = xh[side, pl.ds(pl.multiple_of(k * KC, KC), KC), :]
        kv = dot_nt(wkv[...], xb).astype(BF16)
        kvown[side, k] = kv
        kvcopy(side, k).start()
        place(kv, lc + side * (rc - lc), k)
        qt = dot_nt(wq[...], xb).astype(BF16)
        qs = qt.astype(F32) * scale
        h1 = qs.astype(BF16)
        r1 = qs - h1.astype(F32)
        h2 = r1.astype(BF16)
        h3 = (r1 - h2.astype(F32)).astype(BF16)
        for r in range(2):
            for hd in range(heads):
                for n, part_v in enumerate((h1, h2, h3)):
                    qaug[side * nt + 2 * k + r, hd // 2, n * 32:(n + 1) * 32, (hd % 2) * QT:(hd % 2 + 1) * QT] = part_v[hd * 32:(hd + 1) * 32, r * QT:(r + 1) * QT]

    for cp_ in locs[1:4]:
        cp_.wait()
    xpart.wait_recv()

    @pl.when(s == 1)
    def _():
        xfar(0).start()
        xfar(1).start()

    xfar(2).start()
    for n in range(2):
        wofar(n).start()

    def project_own(k, carry):
        project(0, k)
        return carry

    lax.fori_loop(0, nk, project_own, 0)

    wopart = remote(wo_h, wo.at[t], wo_s.at[8], wo_r.at[8], tp=part)
    wopart.start()

    e0 = 2 * nt + 3 * nt * pp
    e1 = e0 + 14 + 2 * qq
    e2 = e1 + 16 + 6 * qq
    njob = 78
    w0 = 8
    w_step = [25, 31]
    g_ev = (11, 24, 38)

    def pick(*pairs):
        out = pairs[-1][1]
        for cond, val in reversed(pairs[:-1]):
            out = jnp.where(cond, val, out)
        return out

    def job(i):
        k1 = pick((i < 2, 0), (i < 6, 1), (None, 2))
        v1 = i - k1 * (k1 + 1)
        v2 = jnp.maximum(i - 2 * nt, 0)
        k = pick((i < e1, 0), (i < e2, 1), (None, 2))
        u = jnp.maximum(i - pick((i < e1, e0), (i < e2, e1), (None, e2)), 0)
        k_1 = k + 1
        pre = jnp.where(k == 2, 4 * qq, 0)
        ub = jnp.maximum(u - pre, 0)
        ua = u - pre - 2 * k_1
        w = ua - nt
        v = w - qq * 2 * k + pre
        len1 = qq * k_1 * (1 + xx)
        v3 = v - len1
        in1 = i < 2 * nt
        in2 = i < e0
        in_pre = u < pre
        in_b = ua < 0
        in_a2 = jnp.logical_and(v3 >= 0, v3 < nt)
        in_a = jnp.logical_or(w < 0, in_a2)
        in_c2 = v < 0
        na = jnp.maximum(jnp.where(w < 0, ua, v3), 0)
        half = jnp.where(in_a2, 1, 0)
        uc = jnp.maximum(jnp.where(v3 < 0, v, v - nt), 0)
        tc = pick((k == 0, uc), (k == 1, uc // 2), (None, uc // 3))
        far_tile = nt + 2 * k
        first = xx == 0
        slot_a = jnp.where(first, far_tile + half, na)
        ch_a = jnp.where(first, jnp.where(na < nk, lc, ln) * nk + lax.rem(na, nk), (rc + half * (rn - rc)) * nk + k)
        slot = pick((in1, 2 * k1 + lax.rem(v1, 2)), (in2, v2 // nk), (in_pre, nt + u), (in_b, far_tile + lax.rem(ub, 2)), (in_a, slot_a), (in_c2, nt + w), (None, far_tile + tc))
        ch = pick((in1, lc * nk + v1 // 2), (in2, ln * nk + lax.rem(v2, nk)), (in_pre, rn * nk + k), (in_b, rc * nk + ub // 2), (in_a, ch_a), (in_c2, rn * nk + k), (None, rn * nk + uc - tc * k_1))

        def flag(cond):
            return jnp.where(cond, 1, 0)

        masked = pick((in1, flag(v1 // 2 == k1)), (in2, 0), (in_pre, 0), (in_b, flag(ub // 2 == k)), (None, 0))
        last = flag(k == 2)
        fin = pick((in1, masked * (1 - xx) * qq), (in2, flag(lax.rem(v2, nk) == nk - 1) * (1 - xx)), (in_pre, last), (in_b, masked * pp * xx), (in_a, jnp.where(first, pp * flag(na == nt - 1), last * half)), (in_c2, last), (None, last * flag(uc - tc * k_1 == k)))
        return slot, ch, masked * (1 + lax.rem(slot, 2)), fin

    def fold_max(v):
        return jnp.max(v.reshape(KC // 8, 8, QW), axis=0)

    def score(p, slot, ch, sel):
        keys = jnp.concatenate([kaug[p // (npair // 2), pl.ds(pl.multiple_of(ch * KC, KC), KC), :], bias[sel]], axis=1)
        return dot(keys, jnp.concatenate([qaug[slot, p], eye[...]], axis=0))

    for p in range(npair):
        s_first = score(p, 0, lc * nk, 1)
        s_s[p] = s_first
        mx_s[p] = fold_max(s_first)

    def wcopy(k, ii, n):
        w, wr = ((wg, wg_r), (wu, wu_r), (wd, wd_r))[k]
        sl = pl.ds(pl.multiple_of(ii * n, n), n)
        return remote(w.at[1 - s, sl], wr.at[sl], ew_s.at[k], ew_r.at[k], tp=part)

    def ocopy(slot, b, r):
        return remote(osend.at[slot], orecv.at[pl.ds(pl.multiple_of(r * QT, QT), QT), pl.ds(pl.multiple_of(t * tok, QT), tok)], o_s.at[slot], o_r.at[t, r], tp=b)

    def where_of(slot):
        u = lax.rem(slot, nt)
        chip = lax.rem(xx + slot // nt, 2)
        return 2 * chip + u // nr, lax.rem(u, nr)

    def attend(cur, nxt):
        slot, ch = cur[:2]
        k0 = pl.multiple_of(ch * KC, KC)
        for p in range(npair):
            g = p // (npair // 2)
            s_next = score(p, *nxt[:3])
            sc = s_s[p]
            m_old = m_s[slot, p]
            m_new = jnp.maximum(m_old, jnp.max(mx_s[p], axis=0, keepdims=True))
            alpha = jnp.exp2(m_old - m_new)
            pr = jnp.exp2(sc - m_new)
            l_s[slot, p] = l_s[slot, p] * alpha + jnp.sum(pr.reshape(KC // 8, 8, QW), axis=0)
            pv = dot(vt[g * 32:(g + 1) * 32, pl.ds(k0, KC)], pr.astype(BF16))
            acc_s[slot, p] = acc_s[slot, p] * alpha + pv
            m_s[slot, p] = m_new
            s_s[p] = s_next
            mx_s[p] = fold_max(s_next)

    def finish(slot):
        pieces = []
        for p in range(npair):
            o = acc_s[slot, p] / jnp.sum(l_s[slot, p], axis=0, keepdims=True)
            pieces += [o[:, :QT], o[:, QT:]]
        osend[slot] = jnp.concatenate(pieces, axis=0).T.astype(BF16)
        b, r = where_of(slot)

        @pl.when(b != t)
        def _():
            ocopy(slot, b, r).start()

        @pl.when(b == t)
        def _():
            orecv[pl.ds(pl.multiple_of(r * QT, QT), QT), pl.ds(pl.multiple_of(t * tok, QT), tok)] = osend[slot]

    g_step = [g // 2 for g in g_ev]
    r_step = [(e0 + 7) // 2, (e1 + 9) // 2, (e2 - 1) // 2]

    def any_of(m, steps):
        out = m == steps[0]
        for v in steps[1:]:
            out = jnp.logical_or(out, m == v)
        return out

    def step(m, carry):
        first, second = carry
        i = 2 * m

        @pl.when(any_of(m, g_step + r_step + w_step))
        def _():
            @pl.when(m == nt - 1)
            def _():
                def take(k, cc):
                    kvcopy(0, k).wait_recv()
                    place(kvrecv[0, k], ln, k)
                    return cc
                lax.fori_loop(0, nk, take, 0)

            @pl.when(any_of(m, g_step))
            def _():
                k_ev = jnp.where(m <= g_step[0], 0, jnp.where(m <= g_step[1], 1, 2))
                xfar(k_ev).wait_recv()
                xfwd(k_ev).start()
                xfwd_in(k_ev).wait_recv()
                project(1, k_ev)

            for n in range(2):
                @pl.when(m == w_step[n])
                def _(n=n):
                    wofar(n).wait_recv()
                    woy(n).start()
                    wofwd(n).start()

            @pl.when(any_of(m, r_step))
            def _():
                k_r = jnp.where(m <= r_step[0], 0, jnp.where(m <= r_step[1], 1, 2))
                kvcopy(1, k_r).wait_recv()
                place(kvrecv[1, k_r], rn, k_r)

        wi = m - w0 // 2

        @pl.when(jnp.logical_and(wi >= 0, wi < 32))
        def _():
            wcopy(0, wi, wg.shape[1] // 32).start()
            wcopy(1, wi, wu.shape[1] // 32).start()
            wcopy(2, wi, wd.shape[1] // 32).start()

        third = job(jnp.minimum(i + 2, njob - 1))
        fourth = job(jnp.minimum(i + 3, njob - 1))
        attend(first, second)
        attend(second, third)

        def done(n, cc):
            finish(first[0] + n * (second[0] - first[0]))
            return cc

        lax.fori_loop(1 - first[3], 1 + second[3], done, 0)
        return third, fourth

    lax.fori_loop(0, njob // 2, step, (job(jnp.int32(0)), job(jnp.int32(1))))

    for n in range(2):
        woy(n).wait_recv()
        wofwdy(n).start()

    def o_from(b):
        def take(r, cc):
            remote(osend.at[0], orecv.at[pl.ds(pl.multiple_of(r * QT, QT), QT), pl.ds(pl.multiple_of(b * tok, QT), tok)], o_s.at[0], o_r.at[b, r], tp=b).wait_recv()
            return cc
        lax.fori_loop(0, nr, take, 0)

    nw = hid // 4
    near, away = 2 * xx, 2 - 2 * xx

    def part_out(chip, n):
        sl = pl.ds(pl.multiple_of(n * nw, QT), nw)
        o = orecv[:, pl.ds(pl.multiple_of(chip * tok, QT), 2 * tok)]
        return sl, dot(o, wo[pl.ds(chip, 2), :, sl].reshape(2 * tok, nw))

    def near_out(n, carry):
        sl, ow = part_out(near, n)
        h_s[:, sl] = xh[0, own_rows, sl].astype(F32) + ow
        return carry

    def far_out(n, carry):
        sl, ow = part_out(away, n)
        h_out[:, sl] = (h_s[:, sl] + ow).astype(BF16)
        return carry

    o_from(part)
    locs[4].wait()
    wopart.wait()
    lax.fori_loop(0, 4, near_out, 0)
    o_from(far)
    o_from(farp)
    for n in range(2):
        wofwd(n).wait()
        wofwdy(n).wait()
    lax.fori_loop(0, 4, far_out, 0)

    for n in range(2):
        wofar(n).wait_send()
        woy(n).wait_send()

    def odone(slot, carry):
        b, r = where_of(slot)

        @pl.when(b != t)
        def _():
            ocopy(slot, b, r).wait_send()
        return carry

    lax.fori_loop(0, 2 * nt, odone, 0)

    def drain(k, carry):
        kvcopy(0, k).wait_send()
        kvcopy(1, k).wait_send()
        xfar(k).wait_send()
        xfwd(k).wait_send()
        return carry

    lax.fori_loop(0, nk, drain, 0)
    xpart.wait_send()
    for k, (w, wr) in enumerate(((wg, wg_r), (wu, wu_r), (wd, wd_r))):
        remote(w.at[1 - s], wr, ew_s.at[k], ew_r.at[k], tp=part).wait()


def moe_kernel(h, ids, gates, wg, wu, wd, wg_r, wu_r, wd_r,
               y_out,
               g_v, u_v, d_v, send, recv, zsend, zret, zacc, y_acc,
               w_sem, s_s, s_r, z_s, z_r):
    c = lax.axis_index("cp")
    t = lax.axis_index("tp")
    s = lax.rem(t, 2)
    xx = t // 2
    tok, hid = h.shape
    cap = recv.shape[1]
    nf = g_v.shape[0]
    fw = g_v.shape[2]
    half = nf // 2

    def peer(r):
        diag = r // 6
        mid = jnp.logical_and(r >= 2, r < 6)
        dy = jnp.where(mid, lax.rem(r, 2), diag)
        dx = jnp.where(mid, 1 - dy, diag)
        ds = jnp.where(mid, r // 2 - 1, lax.rem(r, 2))
        return {"cp": lax.rem(c + dy, 2), "tp": 2 * lax.rem(xx + dx, 2) + lax.rem(s + ds, 2)}

    bar = pltpu.get_barrier_semaphore()
    for r in range(1, 8):
        pl.semaphore_signal(bar, device_id=peer(jnp.int32(r)), device_id_type=MESH)

    def wload(f, own):
        if own:
            sl = pl.ds(pl.multiple_of(f * fw, fw), fw)
            srcs = (wg.at[s, :, sl], wu.at[s, :, sl], wd.at[s, sl])
        else:
            sl = pl.ds(pl.multiple_of((f - half) * fw, fw), fw)
            srcs = (wg_r.at[:, sl], wu_r.at[:, sl], wd_r.at[sl])
        return [pltpu.make_async_copy(src, dst.at[f], w_sem.at[k, f]) for k, (src, dst) in enumerate(zip(srcs, (g_v, u_v, d_v)))]

    for f in range(nf):
        for cp_ in wload(f, f < half):
            cp_.start()

    ids_v = ids[...]
    dx = lax.rem(ids_v // 2 + xx, 2)
    dy = lax.rem(ids_v // 4 + c, 2)
    ds = lax.rem(ids_v + s, 2)
    rel = jnp.where(dx == dy, 6 * dx + ds, 2 + 2 * ds + dy)
    ex_i = lax.broadcasted_iota(jnp.int32, (8, tok), 0)
    oh0 = (rel[0:1] == ex_i).astype(F32)
    oh1 = (rel[1:2] == ex_i).astype(F32)
    before = (lax.broadcasted_iota(jnp.int32, (tok, tok), 0) < lax.broadcasted_iota(jnp.int32, (tok, tok), 1)).astype(F32).astype(BF16)
    cum = dot(jnp.concatenate([oh0, oh1], axis=0).astype(BF16), before)
    base = ex_i.astype(F32) * cap
    tot0 = jnp.sum(oh0, axis=1, keepdims=True)
    slot0 = jnp.sum(oh0 * (base + cum[0:8]), axis=0, keepdims=True)
    slot1 = jnp.sum(oh1 * (base + tot0 + cum[8:16]), axis=0, keepdims=True)

    cap_i = lax.broadcasted_iota(jnp.int32, (cap, tok), 0).astype(F32)

    def block(r):
        want = cap_i + float(r * cap)
        sel = ((slot0 == want) | (slot1 == want)).astype(F32).astype(BF16)
        return dot(sel, h[...]).astype(BF16)

    def scopy(r):
        return remote(send.at[r], recv.at[r], s_s.at[r], s_r.at[r], **peer(r))

    def zcopy(r):
        return remote(zsend.at[r], zret.at[r], z_s.at[r], z_r.at[r], **peer(r))

    pl.semaphore_wait(bar, 7)
    for r in (2, 3, 1, 4, 5, 6, 7):
        send[r] = block(r)
        scopy(jnp.int32(r)).start()
    recv[0] = block(0)

    def group(g, carry):
        @pl.when(g > 0)
        def _():
            scopy(2 * g).wait_recv()
        scopy(2 * g + 1).wait_recv()
        xg = recv[pl.ds(2 * g, 2)].reshape(2 * cap, hid)
        zacc[...] = jnp.zeros(zacc.shape, F32)

        def fstep(f, cc):
            @pl.when(jnp.logical_and(g == 0, f < half))
            def _():
                for cp_ in wload(f, True):
                    cp_.wait()

            @pl.when(jnp.logical_and(g == 0, f >= half))
            def _():
                for cp_ in wload(f, False):
                    cp_.wait()

            gp = dot(xg, g_v[f])
            up = dot(xg, u_v[f])
            a = (jax.nn.silu(gp) * up).astype(BF16)
            zacc[...] += dot(a, d_v[f])
            return cc

        lax.fori_loop(0, nf, fstep, 0)
        z = zacc[...].astype(BF16)

        @pl.when(g > 0)
        def _():
            zsend[2 * g] = z[:cap]
            zcopy(2 * g).start()

        @pl.when(g == 0)
        def _():
            zret[0] = z[:cap]

        zsend[2 * g + 1] = z[cap:]
        zcopy(2 * g + 1).start()
        return carry

    lax.fori_loop(0, 4, group, 0)

    cols = jnp.concatenate([slot0, slot1, gates[...], jnp.zeros((4, tok), F32)], axis=0).T
    slot_i = lax.broadcasted_iota(jnp.int32, (tok, 2 * cap), 1).astype(F32)

    def combine(g, y):
        z = zret[pl.ds(2 * g, 2)].reshape(2 * cap, hid)
        want = slot_i + (2 * cap * g).astype(F32)
        for k in range(2):
            sel = (cols[:, k:k + 1] == want).astype(F32).astype(BF16)
            y = y + cols[:, 2 + k:3 + k] * dot(sel, z)
        return y

    def returned(g, cc):
        @pl.when(g > 0)
        def _():
            scopy(2 * g).wait_send()
            zcopy(2 * g).wait()
        scopy(2 * g + 1).wait_send()
        zcopy(2 * g + 1).wait()

        @pl.when(g < 3)
        def _():
            y_acc[...] = combine(g, y_acc[...])
        return cc

    y_acc[...] = h[...].astype(F32)
    lax.fori_loop(0, 4, returned, 0)
    y_out[...] = combine(jnp.int32(3), y_acc[...]).astype(BF16)


def solution(mesh):
    row_spec = P(("dp", "cp", "tp"), None)
    head_spec = P(None, "tp", None)
    expert_spec = P(("cp", "tp"), None, None)
    any_spec = pl.BlockSpec(memory_space=pl.ANY)
    vm = pl.BlockSpec(memory_space=pltpu.VMEM)
    DMA = pltpu.SemaphoreType.DMA

    def device_step(x, w_q, w_k, w_v, w_o, ids, gates, w_gate, w_up, w_down):
        tok, hid = x.shape
        nr = tok // QT
        hd = w_q.shape[1] * w_q.shape[2]
        kd = w_k.shape[1] * w_k.shape[2]
        wq_t = w_q.transpose(1, 2, 0).reshape(hd, hid)
        wk_t = w_k.transpose(1, 2, 0).reshape(kd, hid)
        wv_t = w_v.transpose(1, 2, 0).reshape(kd, hid)
        wo = w_o.reshape(hd, hid)
        seq = 8 * tok
        nk = 2 * tok // KC
        npair = w_q.shape[1] // 2
        f = w_gate.shape[2]

        h, wg_r, wu_r, wd_r = pl.pallas_call(
            attn_kernel,
            out_shape=[
                jax.ShapeDtypeStruct((tok, hid), BF16),
                jax.ShapeDtypeStruct((hid, f), BF16),
                jax.ShapeDtypeStruct((hid, f), BF16),
                jax.ShapeDtypeStruct((f, hid), BF16),
            ],
            in_specs=[any_spec] * 8,
            out_specs=[vm, any_spec, any_spec, any_spec],
            scratch_shapes=[
                pltpu.VMEM((2, 2 * tok, hid), BF16),
                pltpu.VMEM((hd, hid), BF16),
                pltpu.VMEM((2 * kd, hid), BF16),
                pltpu.VMEM((4, hd, hid), BF16),
                *[pltpu.VMEM((2, nk, 2 * kd, KC), BF16)] * 2,
                pltpu.VMEM((2, seq, 128), BF16),
                pltpu.VMEM((kd, seq), BF16),
                pltpu.VMEM((4 * nr, npair, 128, QW), BF16),
                pltpu.VMEM((4 * nr, QT, hd), BF16),
                pltpu.VMEM((tok, 4 * hd), BF16),
                pltpu.VMEM((4 * nr, npair, 1, QW), F32),
                pltpu.VMEM((4 * nr, npair, 8, QW), F32),
                pltpu.VMEM((4 * nr, npair, 32, QW), F32),
                pltpu.VMEM((npair, KC, QW), F32),
                pltpu.VMEM((npair, 8, QW), F32),
                pltpu.VMEM((3, KC, QT), BF16),
                pltpu.VMEM((QT, QW), BF16),
                pltpu.VMEM((tok, hid), F32),
                DMA((5,)), *[DMA((nk,))] * 2, DMA, DMA, *[DMA((nk,))] * 2,
                *[DMA((2, nk))] * 2, *[DMA((9,))] * 2, *[DMA((3,))] * 2,
                DMA((4 * nr,)), DMA((4, nr)),
            ],
            compiler_params=pltpu.CompilerParams(collective_id=0, has_side_effects=True, vmem_limit_bytes=60 * 1024 * 1024),
            name="attn",
        )(x, wq_t, wk_t, wv_t, wo, w_gate, w_up, w_down)

        cap = tok * 2 // 8
        fw = f // 2
        nf = 2 * f // fw
        n_dev = 8
        return pl.pallas_call(
            moe_kernel,
            out_shape=jax.ShapeDtypeStruct((tok, hid), BF16),
            in_specs=[vm, vm, vm] + [any_spec] * 6,
            out_specs=vm,
            scratch_shapes=[
                pltpu.VMEM((nf, hid, fw), BF16),
                pltpu.VMEM((nf, hid, fw), BF16),
                pltpu.VMEM((nf, fw, hid), BF16),
                *[pltpu.VMEM((n_dev, cap, hid), BF16)] * 4,
                pltpu.VMEM((2 * cap, hid), F32),
                pltpu.VMEM((tok, hid), F32),
                DMA((3, nf)), *[DMA((n_dev,))] * 4,
            ],
            compiler_params=pltpu.CompilerParams(collective_id=1, has_side_effects=True, vmem_limit_bytes=63 * 1024 * 1024),
            name="moe",
        )(h, ids.T, gates.T, w_gate, w_up, w_down, wg_r, wu_r, wd_r)

    return jax.shard_map(device_step, mesh=mesh, in_specs=(row_spec, head_spec, head_spec, head_spec, P("tp", None, None), row_spec, row_spec, expert_spec, expert_spec, expert_spec), out_specs=row_spec, check_vma=False)
```

```python
import functools
import math

import jax
import jax.numpy as jnp
from jax import lax
from jax.experimental import pallas as pl
from jax.experimental.pallas import tpu as pltpu
from jax.sharding import PartitionSpec as P

MESH = pl.DeviceIdType.MESH
F32 = jnp.float32
BF16 = jnp.bfloat16

NT = (((1,), (1,)), ((), ()))
QT = 128
KC = 256
QW = QT + QT


def dot(a, b):
    return jnp.dot(a, b, preferred_element_type=F32)


def dot_nt(a, b):
    return lax.dot_general(a, b, NT, preferred_element_type=F32)


def remote(src, dst, send, recv, **dev):
    return pltpu.make_async_remote_copy(src_ref=src, dst_ref=dst, send_sem=send, recv_sem=recv, device_id=dev, device_id_type=MESH)


def attn_kernel(x, wq_h, wk_h, wv_h, wo_h, wg, wu, wd,
                h_out, wg_r, wu_r, wd_r,
                xh, wq, wkv, wo, kvown, kvrecv, kaug, vt, qaug, osend, orecv, m_s, l_s, acc_s, s_s, mx_s, h_s,
                loc_sem, xf_s, xf_r, xp_s, xp_r, xw_s, xw_r, kv_s, kv_r, wo_s, wo_r, ew_s, ew_r, o_s, o_r):
    c = lax.axis_index("cp")
    t = lax.axis_index("tp")
    s = lax.rem(t, 2)
    xx = t // 2
    part = t + 1 - 2 * s
    far = lax.rem(t + 2, 4)
    farp = lax.rem(part + 2, 4)
    cn = 1 - c
    tok, hid = x.shape
    nr = tok // QT
    nt = 2 * nr
    nk = 2 * tok // KC
    heads = wq_h.shape[0] // 32
    npair = heads // 2
    scale = 32 ** -0.5 * math.log2(math.e)

    lc = c + xx * (3 - 2 * c)
    rc = 3 - lc
    ln = cn + xx * (3 - 2 * cn)
    rn = 3 - ln
    pp = lax.rem(xx + c, 2)
    qq = 1 - pp

    bar = pltpu.get_barrier_semaphore()
    for dev in ({"tp": part}, {"tp": far}, {"tp": farp}, {"cp": cn}):
        pl.semaphore_signal(bar, device_id=dev, device_id_type=MESH)

    own_rows = pl.ds(pl.multiple_of(s * tok, QT), tok)
    locs = [
        pltpu.make_async_copy(x, xh.at[0, own_rows], loc_sem.at[0]),
        pltpu.make_async_copy(wq_h, wq, loc_sem.at[1]),
        pltpu.make_async_copy(wk_h, wkv.at[pl.ds(0, 64)], loc_sem.at[2]),
        pltpu.make_async_copy(wv_h, wkv.at[pl.ds(64, 64)], loc_sem.at[3]),
        pltpu.make_async_copy(wo_h, wo.at[t], loc_sem.at[4]),
    ]
    for cp_ in locs:
        cp_.start()
    pl.semaphore_wait(bar, 4)

    def piece(k, who):
        return pl.ds(pl.multiple_of((2 * k + who) * QT, QT), QT)

    def xfar(k):
        return remote(xh.at[0, piece(k, s)], xh.at[1, piece(k, s)], xf_s.at[k], xf_r.at[k], tp=far)

    def xfwd(k):
        return remote(xh.at[1, piece(k, s)], xh.at[1, piece(k, s)], xw_s.at[k], xw_r.at[k], tp=part)

    def xfwd_in(k):
        return remote(xh.at[1, piece(k, s)], xh.at[1, piece(k, 1 - s)], xw_s.at[k], xw_r.at[k], tp=part)

    hw = wo.shape[1] // 4

    def wo_rows(cc, n):
        return pl.ds(pl.multiple_of((2 * cc + n) * hw, hw), hw)

    def wofar(n):
        return remote(wo_h.at[wo_rows(c, n)], wo.at[t, wo_rows(c, n)], wo_s.at[n], wo_r.at[n], tp=far)

    def woy(n):
        return remote(wo.at[far, wo_rows(c, n)], wo.at[far, wo_rows(c, n)], wo_s.at[2 + n], wo_r.at[2 + n], cp=cn)

    def wofwd(n):
        return remote(wo.at[far, wo_rows(c, n)], wo.at[far, wo_rows(c, n)], wo_s.at[4 + n], wo_r.at[4 + n], tp=part)

    def wofwdy(n):
        return remote(wo.at[far, wo_rows(cn, n)], wo.at[far, wo_rows(cn, n)], wo_s.at[6 + n], wo_r.at[6 + n], tp=part)

    xpart = remote(x, xh.at[0, own_rows], xp_s, xp_r, tp=part)
    xpart.start()
    locs[0].wait()

    @pl.when(s == 0)
    def _():
        xfar(0).start()
        xfar(1).start()

    qaug[:, :, 96:128, :] = jnp.zeros((qaug.shape[0], npair, 32, QW), BF16)
    kaug[:, :, 96:128] = jnp.zeros((2, kaug.shape[1], 32), BF16)
    m_s[...] = jnp.full(m_s.shape, -jnp.inf, F32)
    l_s[...] = jnp.zeros(l_s.shape, F32)
    acc_s[...] = jnp.zeros(acc_s.shape, F32)

    zero_pad = jnp.zeros((32, KC), BF16)

    def place(kv, ck, k):
        pos = pl.multiple_of((ck * nk + k) * KC, KC)
        for g in range(2):
            kt = kv[g * 32:(g + 1) * 32]
            kaug[g, pl.ds(pos, KC), :] = jnp.concatenate([kt, kt, kt, zero_pad], axis=0).T
        vt[:, pl.ds(pos, KC)] = kv[64:128]

    def kvcopy(side, k):
        return remote(kvown.at[side, k], kvrecv.at[side, k], kv_s.at[side, k], kv_r.at[side, k], cp=cn)

    def project(side, k):
        xb = xh[side, pl.ds(pl.multiple_of(k * KC, KC), KC), :]
        kv = dot_nt(wkv[...], xb).astype(BF16)
        kvown[side, k] = kv
        kvcopy(side, k).start()
        place(kv, lc + side * (rc - lc), k)
        qt = dot_nt(wq[...], xb).astype(BF16)
        qs = qt.astype(F32) * scale
        h1 = qs.astype(BF16)
        r1 = qs - h1.astype(F32)
        h2 = r1.astype(BF16)
        h3 = (r1 - h2.astype(F32)).astype(BF16)
        for r in range(2):
            for hd in range(heads):
                for n, part_v in enumerate((h1, h2, h3)):
                    qaug[side * nt + 2 * k + r, hd // 2, n * 32:(n + 1) * 32, (hd % 2) * QT:(hd % 2 + 1) * QT] = part_v[hd * 32:(hd + 1) * 32, r * QT:(r + 1) * QT]

    for cp_ in locs[1:4]:
        cp_.wait()
    xpart.wait_recv()

    @pl.when(s == 1)
    def _():
        xfar(0).start()
        xfar(1).start()

    xfar(2).start()
    for n in range(2):
        wofar(n).start()

    def project_own(k, carry):
        project(0, k)
        return carry

    lax.fori_loop(0, nk, project_own, 0)

    wopart = remote(wo_h, wo.at[t], wo_s.at[8], wo_r.at[8], tp=part)
    wopart.start()

    e0 = 2 * nt + 3 * nt * pp
    e1 = e0 + 14 + 2 * qq
    e2 = e1 + 16 + 6 * qq
    njob = 78
    w0 = 8
    w_step = [25, 31]
    g_ev = (11, 24, 38)

    def pick(*pairs):
        out = pairs[-1][1]
        for cond, val in reversed(pairs[:-1]):
            out = jnp.where(cond, val, out)
        return out

    def job(i):
        n1 = i // 2
        odd = lax.rem(i, 2) == 1
        late = n1 >= 4
        v2 = jnp.maximum(i - 2 * nt, 0)
        k = pick((i < e1, 0), (i < e2, 1), (None, 2))
        u = jnp.maximum(i - pick((i < e1, e0), (i < e2, e1), (None, e2)), 0)
        k_1 = k + 1
        pre = jnp.where(k == 2, 4 * qq, 0)
        um = u - pre
        ub = jnp.maximum(jnp.where(um < 4, um // 2, um - 2), 0)
        ua = ub - 2 * k
        w = ua - nt
        v = w - qq * 2 * k + pre
        len1 = qq * k_1 * (1 + xx)
        v3 = v - len1
        in1 = i < 2 * nt
        in2 = i < e0
        in_pre = um < 0
        in_m = jnp.logical_or(um == 0, um == 2)
        in_b = ua < 0
        in_a2 = jnp.logical_and(v3 >= 0, v3 < nt)
        in_a = jnp.logical_or(w < 0, in_a2)
        in_c2 = v < 0
        na = jnp.maximum(jnp.where(w < 0, ua, v3), 0)
        half = jnp.where(in_a2, 1, 0)
        uc = jnp.maximum(jnp.where(v3 < 0, v, v - nt), 0)
        tc = pick((k == 0, uc), (k == 1, uc // 2), (None, uc // 3))
        far_tile = nt + 2 * k
        first = xx == 0

        def flag(cond):
            return jnp.where(cond, 1, 0)

        slot_a = jnp.where(first, far_tile + half, na)
        ch_a = jnp.where(first, jnp.where(na < nk, lc, ln) * nk + lax.rem(na, nk), (rc + half * (rn - rc)) * nk + k)
        slot_1 = jnp.where(odd, n1 + jnp.where(late, 0, 2), n1)
        slot = pick((in1, slot_1), (in2, v2 // nk), (in_pre, nt + u), (in_m, far_tile + um // 2), (in_b, far_tile + lax.rem(ub, 2)), (in_a, slot_a), (in_c2, nt + w), (None, far_tile + tc))
        ch = pick((in1, lc * nk + jnp.where(odd, flag(late), n1 // 2)), (in2, ln * nk + lax.rem(v2, nk)), (in_pre, rn * nk + k), (in_m, rc * nk + k), (in_b, rc * nk + ub // 2), (in_a, ch_a), (in_c2, rn * nk + k), (None, rn * nk + uc - tc * k_1))
        masked = pick((in1, 1 - flag(odd)), (in2, 0), (in_pre, 0), (in_m, 1), (None, 0))
        last = flag(k == 2)
        fin = pick((in1, flag(odd == late) * (1 - xx) * qq), (in2, flag(lax.rem(v2, nk) == nk - 1) * (1 - xx)), (in_pre, last), (in_m, flag(k == 0) * pp * xx), (in_b, flag(ub // 2 == k - 1) * pp * xx), (in_a, jnp.where(first, pp * flag(na == nt - 1), last * half)), (in_c2, last), (None, last * flag(uc - tc * k_1 == k)))
        return slot, ch, masked, fin

    def fold_max(v):
        return jnp.max(v.reshape(KC // 8, 8, QW), axis=0)

    def score(p, slot, ch):
        return dot(kaug[p // (npair // 2), pl.ds(pl.multiple_of(ch * KC, KC), KC), :], qaug[slot, p])

    for p in range(npair):
        s_first = score(p, 0, lc * nk)
        s_s[p] = s_first
        mx_s[p] = fold_max(s_first)

    def wcopy(k, ii, n):
        w, wr = ((wg, wg_r), (wu, wu_r), (wd, wd_r))[k]
        sl = pl.ds(pl.multiple_of(ii * n, n), n)
        return remote(w.at[1 - s, sl], wr.at[sl], ew_s.at[k], ew_r.at[k], tp=part)

    def ocopy(slot, b, r):
        return remote(osend.at[slot], orecv.at[pl.ds(pl.multiple_of(r * QT, QT), QT), pl.ds(pl.multiple_of(t * tok, QT), tok)], o_s.at[slot], o_r.at[t, r], tp=b)

    def where_of(slot):
        u = lax.rem(slot, nt)
        chip = lax.rem(xx + slot // nt, 2)
        return 2 * chip + u // nr, lax.rem(u, nr)

    def attend(cur, nxt):
        slot, ch = cur[:2]
        k0 = pl.multiple_of(ch * KC, KC)
        for p in range(npair):
            g = p // (npair // 2)
            s_next = score(p, *nxt[:2])
            sc = s_s[p]
            m_old = m_s[slot, p]
            m_new = jnp.maximum(m_old, jnp.max(mx_s[p], axis=0, keepdims=True))
            alpha = jnp.exp2(m_old - m_new)
            pr = jnp.exp2(sc - m_new)
            l_s[slot, p] = l_s[slot, p] * alpha + jnp.sum(pr.reshape(KC // 8, 8, QW), axis=0)
            pv = dot(vt[g * 32:(g + 1) * 32, pl.ds(k0, KC)], pr.astype(BF16))
            acc_s[slot, p] = acc_s[slot, p] * alpha + pv
            m_s[slot, p] = m_new
            s_s[p] = s_next
            mx_s[p] = fold_max(s_next)

    def finish(slot):
        pieces = []
        for p in range(npair):
            o = acc_s[slot, p] / jnp.sum(l_s[slot, p], axis=0, keepdims=True)
            pieces += [o[:, :QT], o[:, QT:]]
        osend[slot] = jnp.concatenate(pieces, axis=0).T.astype(BF16)
        b, r = where_of(slot)

        @pl.when(b != t)
        def _():
            ocopy(slot, b, r).start()

        @pl.when(b == t)
        def _():
            orecv[pl.ds(pl.multiple_of(r * QT, QT), QT), pl.ds(pl.multiple_of(t * tok, QT), tok)] = osend[slot]

    g_step = [g // 2 for g in g_ev]
    r_step = [(e0 + 7) // 2, (e1 + 9) // 2, (e2 - 1) // 2]

    def any_of(m, steps):
        out = m == steps[0]
        for v in steps[1:]:
            out = jnp.logical_or(out, m == v)
        return out

    def step(m, carry):
        first, second = carry
        i = 2 * m

        @pl.when(any_of(m, g_step + r_step + w_step))
        def _():
            @pl.when(m == nt - 1)
            def _():
                def take(k, cc):
                    kvcopy(0, k).wait_recv()
                    place(kvrecv[0, k], ln, k)
                    return cc
                lax.fori_loop(0, nk, take, 0)

            @pl.when(any_of(m, g_step))
            def _():
                k_ev = jnp.where(m <= g_step[0], 0, jnp.where(m <= g_step[1], 1, 2))
                xfar(k_ev).wait_recv()
                xfwd(k_ev).start()
                xfwd_in(k_ev).wait_recv()
                project(1, k_ev)

            for n in range(2):
                @pl.when(m == w_step[n])
                def _(n=n):
                    wofar(n).wait_recv()
                    woy(n).start()
                    wofwd(n).start()

            @pl.when(any_of(m, r_step))
            def _():
                k_r = jnp.where(m <= r_step[0], 0, jnp.where(m <= r_step[1], 1, 2))
                kvcopy(1, k_r).wait_recv()
                place(kvrecv[1, k_r], rn, k_r)

        wi = m - w0 // 2

        @pl.when(jnp.logical_and(wi >= 0, wi < 32))
        def _():
            wcopy(0, wi, wg.shape[1] // 32).start()
            wcopy(1, wi, wu.shape[1] // 32).start()
            wcopy(2, wi, wd.shape[1] // 32).start()

        @pl.when(first[2] == 1)
        def _():
            key_i = lax.broadcasted_iota(jnp.int32, (KC, QW), 0)
            q_i = lax.rem(lax.broadcasted_iota(jnp.int32, (KC, QW), 1), QT) + lax.rem(first[0], 2) * QT
            for p in range(npair):
                sc = jnp.where(key_i <= q_i, s_s[p], -jnp.inf)
                s_s[p] = sc
                mx_s[p] = fold_max(sc)

        third = job(jnp.minimum(i + 2, njob - 1))
        fourth = job(jnp.minimum(i + 3, njob - 1))
        attend(first, second)
        attend(second, third)

        def done(n, cc):
            finish(first[0] + n * (second[0] - first[0]))
            return cc

        lax.fori_loop(1 - first[3], 1 + second[3], done, 0)
        return third, fourth

    lax.fori_loop(0, njob // 2, step, (job(jnp.int32(0)), job(jnp.int32(1))))

    for n in range(2):
        woy(n).wait_recv()
        wofwdy(n).start()

    def o_from(b):
        def take(r, cc):
            remote(osend.at[0], orecv.at[pl.ds(pl.multiple_of(r * QT, QT), QT), pl.ds(pl.multiple_of(b * tok, QT), tok)], o_s.at[0], o_r.at[b, r], tp=b).wait_recv()
            return cc
        lax.fori_loop(0, nr, take, 0)

    nw = hid // 4
    near, away = 2 * xx, 2 - 2 * xx

    def part_out(chip, n):
        sl = pl.ds(pl.multiple_of(n * nw, QT), nw)
        o = orecv[:, pl.ds(pl.multiple_of(chip * tok, QT), 2 * tok)]
        return sl, dot(o, wo[pl.ds(chip, 2), :, sl].reshape(2 * tok, nw))

    def near_out(n, carry):
        sl, ow = part_out(near, n)
        h_s[:, sl] = xh[0, own_rows, sl].astype(F32) + ow
        return carry

    def far_out(n, carry):
        sl, ow = part_out(away, n)
        h_out[:, sl] = (h_s[:, sl] + ow).astype(BF16)
        return carry

    o_from(part)
    locs[4].wait()
    wopart.wait()
    lax.fori_loop(0, 4, near_out, 0)
    o_from(far)
    o_from(farp)
    for n in range(2):
        wofwd(n).wait()
        wofwdy(n).wait()
    lax.fori_loop(0, 4, far_out, 0)

    for n in range(2):
        wofar(n).wait_send()
        woy(n).wait_send()

    def odone(slot, carry):
        b, r = where_of(slot)

        @pl.when(b != t)
        def _():
            ocopy(slot, b, r).wait_send()
        return carry

    lax.fori_loop(0, 2 * nt, odone, 0)

    def drain(k, carry):
        kvcopy(0, k).wait_send()
        kvcopy(1, k).wait_send()
        xfar(k).wait_send()
        xfwd(k).wait_send()
        return carry

    lax.fori_loop(0, nk, drain, 0)
    xpart.wait_send()
    for k, (w, wr) in enumerate(((wg, wg_r), (wu, wu_r), (wd, wd_r))):
        remote(w.at[1 - s], wr, ew_s.at[k], ew_r.at[k], tp=part).wait()


def moe_kernel(h, ids, gates, wg, wu, wd, wg_r, wu_r, wd_r,
               y_out,
               g_v, u_v, d_v, send, recv, zsend, zret, zacc, y_acc,
               w_sem, s_s, s_r, z_s, z_r):
    c = lax.axis_index("cp")
    t = lax.axis_index("tp")
    s = lax.rem(t, 2)
    xx = t // 2
    tok, hid = h.shape
    cap = recv.shape[1]
    nf = g_v.shape[0]
    fw = g_v.shape[2]
    half = nf // 2

    def peer(r):
        diag = r // 6
        mid = jnp.logical_and(r >= 2, r < 6)
        dy = jnp.where(mid, lax.rem(r, 2), diag)
        dx = jnp.where(mid, 1 - dy, diag)
        ds = jnp.where(mid, r // 2 - 1, lax.rem(r, 2))
        return {"cp": lax.rem(c + dy, 2), "tp": 2 * lax.rem(xx + dx, 2) + lax.rem(s + ds, 2)}

    bar = pltpu.get_barrier_semaphore()
    for r in range(1, 8):
        pl.semaphore_signal(bar, device_id=peer(jnp.int32(r)), device_id_type=MESH)

    def wload(f, own):
        if own:
            sl = pl.ds(pl.multiple_of(f * fw, fw), fw)
            srcs = (wg.at[s, :, sl], wu.at[s, :, sl], wd.at[s, sl])
        else:
            sl = pl.ds(pl.multiple_of((f - half) * fw, fw), fw)
            srcs = (wg_r.at[:, sl], wu_r.at[:, sl], wd_r.at[sl])
        return [pltpu.make_async_copy(src, dst.at[f], w_sem.at[k, f]) for k, (src, dst) in enumerate(zip(srcs, (g_v, u_v, d_v)))]

    for f in range(nf):
        for cp_ in wload(f, f < half):
            cp_.start()

    ids_v = ids[...]
    dx = lax.rem(ids_v // 2 + xx, 2)
    dy = lax.rem(ids_v // 4 + c, 2)
    ds = lax.rem(ids_v + s, 2)
    rel = jnp.where(dx == dy, 6 * dx + ds, 2 + 2 * ds + dy)
    ex_i = lax.broadcasted_iota(jnp.int32, (8, tok), 0)
    oh0 = (rel[0:1] == ex_i).astype(F32)
    oh1 = (rel[1:2] == ex_i).astype(F32)
    before = (lax.broadcasted_iota(jnp.int32, (tok, tok), 0) < lax.broadcasted_iota(jnp.int32, (tok, tok), 1)).astype(F32).astype(BF16)
    cum = dot(jnp.concatenate([oh0, oh1], axis=0).astype(BF16), before)
    base = ex_i.astype(F32) * cap
    tot0 = jnp.sum(oh0, axis=1, keepdims=True)
    slot0 = jnp.sum(oh0 * (base + cum[0:8]), axis=0, keepdims=True)
    slot1 = jnp.sum(oh1 * (base + tot0 + cum[8:16]), axis=0, keepdims=True)

    cap_i = lax.broadcasted_iota(jnp.int32, (cap, tok), 0).astype(F32)

    def block(r):
        want = cap_i + float(r * cap)
        sel = ((slot0 == want) | (slot1 == want)).astype(F32).astype(BF16)
        return dot(sel, h[...]).astype(BF16)

    def scopy(r):
        return remote(send.at[r], recv.at[r], s_s.at[r], s_r.at[r], **peer(r))

    def zcopy(r):
        return remote(zsend.at[r], zret.at[r], z_s.at[r], z_r.at[r], **peer(r))

    pl.semaphore_wait(bar, 7)
    for r in (3, 2, 1, 5, 4, 6, 7):
        send[r] = block(r)
        scopy(jnp.int32(r)).start()
    recv[0] = block(0)

    def group(g, carry):
        @pl.when(g > 0)
        def _():
            scopy(2 * g).wait_recv()
        scopy(2 * g + 1).wait_recv()
        xg = recv[pl.ds(2 * g, 2)].reshape(2 * cap, hid)
        zacc[...] = jnp.zeros(zacc.shape, F32)

        def fstep(f, cc):
            @pl.when(jnp.logical_and(g == 0, f < half))
            def _():
                for cp_ in wload(f, True):
                    cp_.wait()

            @pl.when(jnp.logical_and(g == 0, f >= half))
            def _():
                for cp_ in wload(f, False):
                    cp_.wait()

            gp = dot(xg, g_v[f])
            up = dot(xg, u_v[f])
            a = (jax.nn.silu(gp) * up).astype(BF16)
            zacc[...] += dot(a, d_v[f])
            return cc

        lax.fori_loop(0, nf, fstep, 0)
        z = zacc[...].astype(BF16)

        @pl.when(g > 0)
        def _():
            zsend[2 * g] = z[:cap]
            zcopy(2 * g).start()

        @pl.when(g == 0)
        def _():
            zret[0] = z[:cap]

        zsend[2 * g + 1] = z[cap:]
        zcopy(2 * g + 1).start()
        return carry

    lax.fori_loop(0, 4, group, 0)

    cols = jnp.concatenate([slot0, slot1, gates[...], jnp.zeros((4, tok), F32)], axis=0).T
    slot_i = lax.broadcasted_iota(jnp.int32, (tok, 2 * cap), 1).astype(F32)

    def combine(g, y):
        z = zret[pl.ds(2 * g, 2)].reshape(2 * cap, hid)
        want = slot_i + (2 * cap * g).astype(F32)
        for k in range(2):
            sel = (cols[:, k:k + 1] == want).astype(F32).astype(BF16)
            y = y + cols[:, 2 + k:3 + k] * dot(sel, z)
        return y

    def returned(g, cc):
        @pl.when(g > 0)
        def _():
            scopy(2 * g).wait_send()
            zcopy(2 * g).wait()
        scopy(2 * g + 1).wait_send()
        zcopy(2 * g + 1).wait()

        @pl.when(g < 3)
        def _():
            y_acc[...] = combine(g, y_acc[...])
        return cc

    y_acc[...] = h[...].astype(F32)
    lax.fori_loop(0, 4, returned, 0)
    y_out[...] = combine(jnp.int32(3), y_acc[...]).astype(BF16)


def solution(mesh):
    row_spec = P(("dp", "cp", "tp"), None)
    head_spec = P(None, "tp", None)
    expert_spec = P(("cp", "tp"), None, None)
    any_spec = pl.BlockSpec(memory_space=pl.ANY)
    vm = pl.BlockSpec(memory_space=pltpu.VMEM)
    DMA = pltpu.SemaphoreType.DMA

    def device_step(x, w_q, w_k, w_v, w_o, ids, gates, w_gate, w_up, w_down):
        tok, hid = x.shape
        nr = tok // QT
        hd = w_q.shape[1] * w_q.shape[2]
        kd = w_k.shape[1] * w_k.shape[2]
        wq_t = w_q.transpose(1, 2, 0).reshape(hd, hid)
        wk_t = w_k.transpose(1, 2, 0).reshape(kd, hid)
        wv_t = w_v.transpose(1, 2, 0).reshape(kd, hid)
        wo = w_o.reshape(hd, hid)
        seq = 8 * tok
        nk = 2 * tok // KC
        npair = w_q.shape[1] // 2
        f = w_gate.shape[2]

        h, wg_r, wu_r, wd_r = pl.pallas_call(
            attn_kernel,
            out_shape=[
                jax.ShapeDtypeStruct((tok, hid), BF16),
                jax.ShapeDtypeStruct((hid, f), BF16),
                jax.ShapeDtypeStruct((hid, f), BF16),
                jax.ShapeDtypeStruct((f, hid), BF16),
            ],
            in_specs=[any_spec] * 8,
            out_specs=[vm, any_spec, any_spec, any_spec],
            scratch_shapes=[
                pltpu.VMEM((2, 2 * tok, hid), BF16),
                pltpu.VMEM((hd, hid), BF16),
                pltpu.VMEM((2 * kd, hid), BF16),
                pltpu.VMEM((4, hd, hid), BF16),
                *[pltpu.VMEM((2, nk, 2 * kd, KC), BF16)] * 2,
                pltpu.VMEM((2, seq, 128), BF16),
                pltpu.VMEM((kd, seq), BF16),
                pltpu.VMEM((4 * nr, npair, 128, QW), BF16),
                pltpu.VMEM((4 * nr, QT, hd), BF16),
                pltpu.VMEM((tok, 4 * hd), BF16),
                pltpu.VMEM((4 * nr, npair, 1, QW), F32),
                pltpu.VMEM((4 * nr, npair, 8, QW), F32),
                pltpu.VMEM((4 * nr, npair, 32, QW), F32),
                pltpu.VMEM((npair, KC, QW), F32),
                pltpu.VMEM((npair, 8, QW), F32),
                pltpu.VMEM((tok, hid), F32),
                DMA((5,)), *[DMA((nk,))] * 2, DMA, DMA, *[DMA((nk,))] * 2,
                *[DMA((2, nk))] * 2, *[DMA((9,))] * 2, *[DMA((3,))] * 2,
                DMA((4 * nr,)), DMA((4, nr)),
            ],
            compiler_params=pltpu.CompilerParams(collective_id=0, has_side_effects=True, vmem_limit_bytes=60 * 1024 * 1024),
            name="attn",
        )(x, wq_t, wk_t, wv_t, wo, w_gate, w_up, w_down)

        cap = tok * 2 // 8
        fw = f // 2
        nf = 2 * f // fw
        n_dev = 8
        return pl.pallas_call(
            moe_kernel,
            out_shape=jax.ShapeDtypeStruct((tok, hid), BF16),
            in_specs=[vm, vm, vm] + [any_spec] * 6,
            out_specs=vm,
            scratch_shapes=[
                pltpu.VMEM((nf, hid, fw), BF16),
                pltpu.VMEM((nf, hid, fw), BF16),
                pltpu.VMEM((nf, fw, hid), BF16),
                *[pltpu.VMEM((n_dev, cap, hid), BF16)] * 4,
                pltpu.VMEM((2 * cap, hid), F32),
                pltpu.VMEM((tok, hid), F32),
                DMA((3, nf)), *[DMA((n_dev,))] * 4,
            ],
            compiler_params=pltpu.CompilerParams(collective_id=1, has_side_effects=True, vmem_limit_bytes=63 * 1024 * 1024),
            name="moe",
        )(h, ids.T, gates.T, w_gate, w_up, w_down, wg_r, wu_r, wd_r)

    return jax.shard_map(device_step, mesh=mesh, in_specs=(row_spec, head_spec, head_spec, head_spec, P("tp", None, None), row_spec, row_spec, expert_spec, expert_spec, expert_spec), out_specs=row_spec, check_vma=False)
```

```python
import functools
import math

import jax
import jax.numpy as jnp
from jax import lax
from jax.experimental import pallas as pl
from jax.experimental.pallas import tpu as pltpu
from jax.sharding import PartitionSpec as P

MESH = pl.DeviceIdType.MESH
F32 = jnp.float32
BF16 = jnp.bfloat16

NT = (((1,), (1,)), ((), ()))
QT = 128
KC = 256
QW = QT + QT


def dot(a, b):
    return jnp.dot(a, b, preferred_element_type=F32)


def dot_nt(a, b):
    return lax.dot_general(a, b, NT, preferred_element_type=F32)


def remote(src, dst, send, recv, **dev):
    return pltpu.make_async_remote_copy(src_ref=src, dst_ref=dst, send_sem=send, recv_sem=recv, device_id=dev, device_id_type=MESH)


def attn_kernel(x, wq_h, wk_h, wv_h, wo_h, wg, wu, wd,
                h_out, wg_r, wu_r, wd_r,
                xh, wq, wkv, wo, kvown, kvrecv, kaug, vt, qaug, osend, orecv, m_s, l_s, acc_s, s_s, mx_s, h_s,
                loc_sem, xf_s, xf_r, xp_s, xp_r, xw_s, xw_r, kv_s, kv_r, wo_s, wo_r, ew_s, ew_r, o_s, o_r):
    c = lax.axis_index("cp")
    t = lax.axis_index("tp")
    s = lax.rem(t, 2)
    xx = t // 2
    part = t + 1 - 2 * s
    far = lax.rem(t + 2, 4)
    farp = lax.rem(part + 2, 4)
    cn = 1 - c
    tok, hid = x.shape
    nr = tok // QT
    nt = 2 * nr
    nk = 2 * tok // KC
    heads = wq_h.shape[0] // 32
    npair = heads // 2
    scale = 32 ** -0.5 * math.log2(math.e)

    lc = c + xx * (3 - 2 * c)
    rc = 3 - lc
    ln = cn + xx * (3 - 2 * cn)
    rn = 3 - ln
    pp = lax.rem(xx + c, 2)
    qq = 1 - pp

    bar = pltpu.get_barrier_semaphore()
    for dev in ({"tp": part}, {"tp": far}, {"tp": farp}, {"cp": cn}):
        pl.semaphore_signal(bar, device_id=dev, device_id_type=MESH)

    own_rows = pl.ds(pl.multiple_of(s * tok, QT), tok)
    locs = [
        pltpu.make_async_copy(x, xh.at[0, own_rows], loc_sem.at[0]),
        pltpu.make_async_copy(wq_h, wq, loc_sem.at[1]),
        pltpu.make_async_copy(wk_h, wkv.at[pl.ds(0, 64)], loc_sem.at[2]),
        pltpu.make_async_copy(wv_h, wkv.at[pl.ds(64, 64)], loc_sem.at[3]),
        pltpu.make_async_copy(wo_h, wo.at[t], loc_sem.at[4]),
    ]
    for cp_ in locs:
        cp_.start()
    pl.semaphore_wait(bar, 4)

    def piece(k, who):
        return pl.ds(pl.multiple_of((2 * k + who) * QT, QT), QT)

    def xfar(k):
        return remote(xh.at[0, piece(k, s)], xh.at[1, piece(k, s)], xf_s.at[k], xf_r.at[k], tp=far)

    def xfwd(k):
        return remote(xh.at[1, piece(k, s)], xh.at[1, piece(k, s)], xw_s.at[k], xw_r.at[k], tp=part)

    def xfwd_in(k):
        return remote(xh.at[1, piece(k, s)], xh.at[1, piece(k, 1 - s)], xw_s.at[k], xw_r.at[k], tp=part)

    hw = wo.shape[1] // 4

    def wo_rows(cc, n):
        return pl.ds(pl.multiple_of((2 * cc + n) * hw, hw), hw)

    def wofar(n):
        return remote(wo_h.at[wo_rows(c, n)], wo.at[t, wo_rows(c, n)], wo_s.at[n], wo_r.at[n], tp=far)

    def woy(n):
        return remote(wo.at[far, wo_rows(c, n)], wo.at[far, wo_rows(c, n)], wo_s.at[2 + n], wo_r.at[2 + n], cp=cn)

    def wofwd(n):
        return remote(wo.at[far, wo_rows(c, n)], wo.at[far, wo_rows(c, n)], wo_s.at[4 + n], wo_r.at[4 + n], tp=part)

    def wofwdy(n):
        return remote(wo.at[far, wo_rows(cn, n)], wo.at[far, wo_rows(cn, n)], wo_s.at[6 + n], wo_r.at[6 + n], tp=part)

    xpart = remote(x, xh.at[0, own_rows], xp_s, xp_r, tp=part)
    xpart.start()
    locs[0].wait()

    @pl.when(s == 0)
    def _():
        xfar(0).start()
        xfar(1).start()

    qaug[:, :, 96:128, :] = jnp.zeros((qaug.shape[0], npair, 32, QW), BF16)
    kaug[:, :, 96:128] = jnp.zeros((2, kaug.shape[1], 32), BF16)
    m_s[...] = jnp.full(m_s.shape, -jnp.inf, F32)
    l_s[...] = jnp.zeros(l_s.shape, F32)
    acc_s[...] = jnp.zeros(acc_s.shape, F32)

    zero_pad = jnp.zeros((32, KC), BF16)

    def place(kv, ck, k):
        pos = pl.multiple_of((ck * nk + k) * KC, KC)
        for g in range(2):
            kt = kv[g * 32:(g + 1) * 32]
            kaug[g, pl.ds(pos, KC), :] = jnp.concatenate([kt, kt, kt, zero_pad], axis=0).T
        vt[:, pl.ds(pos, KC)] = kv[64:128]

    def kvcopy(side, k):
        return remote(kvown.at[side, k], kvrecv.at[side, k], kv_s.at[side, k], kv_r.at[side, k], cp=cn)

    def project(side, k):
        xb = xh[side, pl.ds(pl.multiple_of(k * KC, KC), KC), :]
        kv = dot_nt(wkv[...], xb).astype(BF16)
        kvown[side, k] = kv
        kvcopy(side, k).start()
        place(kv, lc + side * (rc - lc), k)
        qt = dot_nt(wq[...], xb).astype(BF16)
        qs = qt.astype(F32) * scale
        h1 = qs.astype(BF16)
        r1 = qs - h1.astype(F32)
        h2 = r1.astype(BF16)
        h3 = (r1 - h2.astype(F32)).astype(BF16)
        for r in range(2):
            for hd in range(heads):
                for n, part_v in enumerate((h1, h2, h3)):
                    qaug[side * nt + 2 * k + r, hd // 2, n * 32:(n + 1) * 32, (hd % 2) * QT:(hd % 2 + 1) * QT] = part_v[hd * 32:(hd + 1) * 32, r * QT:(r + 1) * QT]

    for cp_ in locs[1:4]:
        cp_.wait()
    xpart.wait_recv()

    @pl.when(s == 1)
    def _():
        xfar(0).start()
        xfar(1).start()

    xfar(2).start()
    for n in range(2):
        wofar(n).start()

    def project_own(k, carry):
        project(0, k)
        return carry

    lax.fori_loop(0, nk, project_own, 0)

    wopart = remote(wo_h, wo.at[t], wo_s.at[8], wo_r.at[8], tp=part)
    wopart.start()

    e0 = 2 * nt + 3 * nt * pp
    e1 = e0 + 14 + 2 * qq
    e2 = e1 + 16 + 6 * qq
    njob = 78
    w0 = 8
    w_step = [24, 29]
    g_ev = (11, 24, 38)

    def pick(*pairs):
        out = pairs[-1][1]
        for cond, val in reversed(pairs[:-1]):
            out = jnp.where(cond, val, out)
        return out

    def job(i):
        n1 = i // 2
        odd = lax.rem(i, 2) == 1
        late = n1 >= 4
        v2 = jnp.maximum(i - 2 * nt, 0)
        k = pick((i < e1, 0), (i < e2, 1), (None, 2))
        u = jnp.maximum(i - pick((i < e1, e0), (i < e2, e1), (None, e2)), 0)
        k_1 = k + 1
        pre = jnp.where(k == 2, 4 * qq, 0)
        um = u - pre
        ub = jnp.maximum(jnp.where(um < 4, um // 2, um - 2), 0)
        ua = ub - 2 * k
        w = ua - nt
        v = w - qq * 2 * k + pre
        len1 = qq * k_1 * (1 + xx)
        v3 = v - len1
        in1 = i < 2 * nt
        in2 = i < e0
        in_pre = um < 0
        in_m = jnp.logical_or(um == 0, um == 2)
        in_b = ua < 0
        in_a2 = jnp.logical_and(v3 >= 0, v3 < nt)
        in_a = jnp.logical_or(w < 0, in_a2)
        in_c2 = v < 0
        na = jnp.maximum(jnp.where(w < 0, ua, v3), 0)
        half = jnp.where(in_a2, 1, 0)
        uc = jnp.maximum(jnp.where(v3 < 0, v, v - nt), 0)
        tc = pick((k == 0, uc), (k == 1, uc // 2), (None, uc // 3))
        far_tile = nt + 2 * k
        first = xx == 0

        def flag(cond):
            return jnp.where(cond, 1, 0)

        slot_a = jnp.where(first, far_tile + half, na)
        ch_a = jnp.where(first, jnp.where(na < nk, lc, ln) * nk + lax.rem(na, nk), (rc + half * (rn - rc)) * nk + k)
        slot_1 = jnp.where(odd, n1 + jnp.where(late, 0, 2), n1)
        slot = pick((in1, slot_1), (in2, v2 // nk), (in_pre, nt + u), (in_m, far_tile + um // 2), (in_b, far_tile + lax.rem(ub, 2)), (in_a, slot_a), (in_c2, nt + w), (None, far_tile + tc))
        ch = pick((in1, lc * nk + jnp.where(odd, flag(late), n1 // 2)), (in2, ln * nk + lax.rem(v2, nk)), (in_pre, rn * nk + k), (in_m, rc * nk + k), (in_b, rc * nk + ub // 2), (in_a, ch_a), (in_c2, rn * nk + k), (None, rn * nk + uc - tc * k_1))
        masked = pick((in1, 1 - flag(odd)), (in2, 0), (in_pre, 0), (in_m, 1), (None, 0))
        last = flag(k == 2)
        fin = pick((in1, flag(odd == late) * (1 - xx) * qq), (in2, flag(lax.rem(v2, nk) == nk - 1) * (1 - xx)), (in_pre, last), (in_m, flag(k == 0) * pp * xx), (in_b, flag(ub // 2 == k - 1) * pp * xx), (in_a, jnp.where(first, pp * flag(na == nt - 1), last * half)), (in_c2, last), (None, last * flag(uc - tc * k_1 == k)))
        return slot, ch, masked, fin

    def fold_max(v):
        return jnp.max(v.reshape(KC // 8, 8, QW), axis=0)

    def score(p, slot, ch):
        return dot(kaug[p // (npair // 2), pl.ds(pl.multiple_of(ch * KC, KC), KC), :], qaug[slot, p])

    for p in range(npair):
        s_first = score(p, 0, lc * nk)
        s_s[p] = s_first
        mx_s[p] = fold_max(s_first)

    def wcopy(k, ii, n):
        w, wr = ((wg, wg_r), (wu, wu_r), (wd, wd_r))[k]
        sl = pl.ds(pl.multiple_of(ii * n, n), n)
        return remote(w.at[1 - s, sl], wr.at[sl], ew_s.at[k], ew_r.at[k], tp=part)

    def ocopy(slot, b, r):
        return remote(osend.at[slot], orecv.at[pl.ds(pl.multiple_of(r * QT, QT), QT), pl.ds(pl.multiple_of(t * tok, QT), tok)], o_s.at[slot], o_r.at[t, r], tp=b)

    def where_of(slot):
        u = lax.rem(slot, nt)
        chip = lax.rem(xx + slot // nt, 2)
        return 2 * chip + u // nr, lax.rem(u, nr)

    def attend(cur, nxt):
        slot, ch = cur[:2]
        k0 = pl.multiple_of(ch * KC, KC)
        for p in range(npair):
            g = p // (npair // 2)
            s_next = score(p, *nxt[:2])
            sc = s_s[p]
            m_old = m_s[slot, p]
            m_new = jnp.maximum(m_old, jnp.max(mx_s[p], axis=0, keepdims=True))
            alpha = jnp.exp2(m_old - m_new)
            pr = jnp.exp2(sc - m_new)
            l_s[slot, p] = l_s[slot, p] * alpha + jnp.sum(pr.reshape(KC // 8, 8, QW), axis=0)
            pv = dot(vt[g * 32:(g + 1) * 32, pl.ds(k0, KC)], pr.astype(BF16))
            acc_s[slot, p] = acc_s[slot, p] * alpha + pv
            m_s[slot, p] = m_new
            s_s[p] = s_next
            mx_s[p] = fold_max(s_next)

    def finish(slot):
        pieces = []
        for p in range(npair):
            o = acc_s[slot, p] / jnp.sum(l_s[slot, p], axis=0, keepdims=True)
            pieces += [o[:, :QT], o[:, QT:]]
        osend[slot] = jnp.concatenate(pieces, axis=0).T.astype(BF16)
        b, r = where_of(slot)

        @pl.when(b != t)
        def _():
            ocopy(slot, b, r).start()

        @pl.when(b == t)
        def _():
            orecv[pl.ds(pl.multiple_of(r * QT, QT), QT), pl.ds(pl.multiple_of(t * tok, QT), tok)] = osend[slot]

    g_step = [g // 2 for g in g_ev]
    r_step = [(e0 + 7) // 2, (e1 + 9) // 2, (e2 - 1) // 2]

    def any_of(m, steps):
        out = m == steps[0]
        for v in steps[1:]:
            out = jnp.logical_or(out, m == v)
        return out

    def step(m, carry):
        first, second = carry
        i = 2 * m

        @pl.when(any_of(m, g_step + r_step + w_step))
        def _():
            @pl.when(m == nt - 1)
            def _():
                def take(k, cc):
                    kvcopy(0, k).wait_recv()
                    place(kvrecv[0, k], ln, k)
                    return cc
                lax.fori_loop(0, nk, take, 0)

            @pl.when(any_of(m, g_step))
            def _():
                k_ev = jnp.where(m <= g_step[0], 0, jnp.where(m <= g_step[1], 1, 2))
                xfar(k_ev).wait_recv()
                xfwd(k_ev).start()
                xfwd_in(k_ev).wait_recv()
                project(1, k_ev)

            for n in range(2):
                @pl.when(m == w_step[n])
                def _(n=n):
                    wofar(n).wait_recv()
                    woy(n).start()
                    wofwd(n).start()

            @pl.when(any_of(m, r_step))
            def _():
                k_r = jnp.where(m <= r_step[0], 0, jnp.where(m <= r_step[1], 1, 2))
                kvcopy(1, k_r).wait_recv()
                place(kvrecv[1, k_r], rn, k_r)

        wi = m - w0 // 2

        @pl.when(jnp.logical_and(wi >= 0, wi < 32))
        def _():
            wcopy(0, wi, wg.shape[1] // 32).start()
            wcopy(1, wi, wu.shape[1] // 32).start()
            wcopy(2, wi, wd.shape[1] // 32).start()

        @pl.when(first[2] == 1)
        def _():
            key_i = lax.broadcasted_iota(jnp.int32, (KC, QW), 0)
            q_i = lax.rem(lax.broadcasted_iota(jnp.int32, (KC, QW), 1), QT) + lax.rem(first[0], 2) * QT
            for p in range(npair):
                sc = jnp.where(key_i <= q_i, s_s[p], -jnp.inf)
                s_s[p] = sc
                mx_s[p] = fold_max(sc)

        third = job(jnp.minimum(i + 2, njob - 1))
        fourth = job(jnp.minimum(i + 3, njob - 1))
        attend(first, second)
        attend(second, third)

        def done(n, cc):
            finish(first[0] + n * (second[0] - first[0]))
            return cc

        lax.fori_loop(1 - first[3], 1 + second[3], done, 0)
        return third, fourth

    lax.fori_loop(0, njob // 2, step, (job(jnp.int32(0)), job(jnp.int32(1))))

    for n in range(2):
        woy(n).wait_recv()
        wofwdy(n).start()

    def o_from(b):
        def take(r, cc):
            remote(osend.at[0], orecv.at[pl.ds(pl.multiple_of(r * QT, QT), QT), pl.ds(pl.multiple_of(b * tok, QT), tok)], o_s.at[0], o_r.at[b, r], tp=b).wait_recv()
            return cc
        lax.fori_loop(0, nr, take, 0)

    nw = hid // 3
    near, away = 2 * xx, 2 - 2 * xx

    def part_out(chip, n):
        sl = pl.ds(pl.multiple_of(n * nw, QT), nw)
        o = orecv[:, pl.ds(pl.multiple_of(chip * tok, QT), 2 * tok)]
        return sl, dot(o, wo[pl.ds(chip, 2), :, sl].reshape(2 * tok, nw))

    def near_out(n, carry):
        sl, ow = part_out(near, n)
        h_s[:, sl] = xh[0, own_rows, sl].astype(F32) + ow
        return carry

    def far_out(n, carry):
        sl, ow = part_out(away, n)
        h_out[:, sl] = (h_s[:, sl] + ow).astype(BF16)
        return carry

    o_from(part)
    locs[4].wait()
    wopart.wait()
    lax.fori_loop(0, hid // nw, near_out, 0)
    o_from(far)
    o_from(farp)
    for n in range(2):
        wofwd(n).wait()
        wofwdy(n).wait()
    lax.fori_loop(0, hid // nw, far_out, 0)

    for n in range(2):
        wofar(n).wait_send()
        woy(n).wait_send()

    def odone(slot, carry):
        b, r = where_of(slot)

        @pl.when(b != t)
        def _():
            ocopy(slot, b, r).wait_send()
        return carry

    lax.fori_loop(0, 2 * nt, odone, 0)

    def drain(k, carry):
        kvcopy(0, k).wait_send()
        kvcopy(1, k).wait_send()
        xfar(k).wait_send()
        xfwd(k).wait_send()
        return carry

    lax.fori_loop(0, nk, drain, 0)
    xpart.wait_send()
    for k, (w, wr) in enumerate(((wg, wg_r), (wu, wu_r), (wd, wd_r))):
        remote(w.at[1 - s], wr, ew_s.at[k], ew_r.at[k], tp=part).wait()


def moe_kernel(h, ids, gates, wg, wu, wd, wg_r, wu_r, wd_r,
               y_out,
               g_v, u_v, d_v, send, recv, zsend, zret, zacc, y_acc,
               w_sem, s_s, s_r, z_s, z_r):
    c = lax.axis_index("cp")
    t = lax.axis_index("tp")
    s = lax.rem(t, 2)
    xx = t // 2
    tok, hid = h.shape
    cap = recv.shape[1]
    nf = g_v.shape[0]
    fw = g_v.shape[2]
    half = nf // 2

    def peer(r):
        diag = r // 6
        mid = jnp.logical_and(r >= 2, r < 6)
        dy = jnp.where(mid, lax.rem(r, 2), diag)
        dx = jnp.where(mid, 1 - dy, diag)
        ds = jnp.where(mid, r // 2 - 1, lax.rem(r, 2))
        return {"cp": lax.rem(c + dy, 2), "tp": 2 * lax.rem(xx + dx, 2) + lax.rem(s + ds, 2)}

    bar = pltpu.get_barrier_semaphore()
    for r in range(1, 8):
        pl.semaphore_signal(bar, device_id=peer(jnp.int32(r)), device_id_type=MESH)

    def wload(f, own):
        if own:
            sl = pl.ds(pl.multiple_of(f * fw, fw), fw)
            srcs = (wg.at[s, :, sl], wu.at[s, :, sl], wd.at[s, sl])
        else:
            sl = pl.ds(pl.multiple_of((f - half) * fw, fw), fw)
            srcs = (wg_r.at[:, sl], wu_r.at[:, sl], wd_r.at[sl])
        return [pltpu.make_async_copy(src, dst.at[f], w_sem.at[k, f]) for k, (src, dst) in enumerate(zip(srcs, (g_v, u_v, d_v)))]

    for f in range(nf):
        for cp_ in wload(f, f < half):
            cp_.start()

    ids_v = ids[...]
    dx = lax.rem(ids_v // 2 + xx, 2)
    dy = lax.rem(ids_v // 4 + c, 2)
    ds = lax.rem(ids_v + s, 2)
    rel = jnp.where(dx == dy, 6 * dx + ds, 2 + 2 * ds + dy)
    ex_i = lax.broadcasted_iota(jnp.int32, (8, tok), 0)
    oh0 = (rel[0:1] == ex_i).astype(F32)
    oh1 = (rel[1:2] == ex_i).astype(F32)
    before = (lax.broadcasted_iota(jnp.int32, (tok, tok), 0) < lax.broadcasted_iota(jnp.int32, (tok, tok), 1)).astype(F32).astype(BF16)
    cum = dot(jnp.concatenate([oh0, oh1], axis=0).astype(BF16), before)
    base = ex_i.astype(F32) * cap
    tot0 = jnp.sum(oh0, axis=1, keepdims=True)
    slot0 = jnp.sum(oh0 * (base + cum[0:8]), axis=0, keepdims=True)
    slot1 = jnp.sum(oh1 * (base + tot0 + cum[8:16]), axis=0, keepdims=True)

    cap_i = lax.broadcasted_iota(jnp.int32, (cap, tok), 0).astype(F32)

    def block(r):
        want = cap_i + float(r * cap)
        sel = ((slot0 == want) | (slot1 == want)).astype(F32).astype(BF16)
        return dot(sel, h[...]).astype(BF16)

    def scopy(r):
        return remote(send.at[r], recv.at[r], s_s.at[r], s_r.at[r], **peer(r))

    def zcopy(r):
        return remote(zsend.at[r], zret.at[r], z_s.at[r], z_r.at[r], **peer(r))

    pl.semaphore_wait(bar, 7)
    for r in (3, 2, 1, 5, 4, 6, 7):
        send[r] = block(r)
        scopy(jnp.int32(r)).start()
    recv[0] = block(0)

    def group(g, carry):
        @pl.when(g > 0)
        def _():
            scopy(2 * g).wait_recv()
        scopy(2 * g + 1).wait_recv()
        xg = recv[pl.ds(2 * g, 2)].reshape(2 * cap, hid)
        zacc[...] = jnp.zeros(zacc.shape, F32)

        def fstep(f, cc):
            @pl.when(jnp.logical_and(g == 0, f < half))
            def _():
                for cp_ in wload(f, True):
                    cp_.wait()

            @pl.when(jnp.logical_and(g == 0, f >= half))
            def _():
                for cp_ in wload(f, False):
                    cp_.wait()

            gp = dot(xg, g_v[f])
            up = dot(xg, u_v[f])
            a = (jax.nn.silu(gp) * up).astype(BF16)
            zacc[...] += dot(a, d_v[f])
            return cc

        lax.fori_loop(0, nf, fstep, 0)
        z = zacc[...].astype(BF16)

        @pl.when(g > 0)
        def _():
            zsend[2 * g] = z[:cap]
            zcopy(2 * g).start()

        @pl.when(g == 0)
        def _():
            zret[0] = z[:cap]

        zsend[2 * g + 1] = z[cap:]
        zcopy(2 * g + 1).start()
        return carry

    lax.fori_loop(0, 4, group, 0)

    cols = jnp.concatenate([slot0, slot1, gates[...], jnp.zeros((4, tok), F32)], axis=0).T
    slot_i = lax.broadcasted_iota(jnp.int32, (tok, 2 * cap), 1).astype(F32)

    def combine(g, y):
        z = zret[pl.ds(2 * g, 2)].reshape(2 * cap, hid)
        want = slot_i + (2 * cap * g).astype(F32)
        for k in range(2):
            sel = (cols[:, k:k + 1] == want).astype(F32).astype(BF16)
            y = y + cols[:, 2 + k:3 + k] * dot(sel, z)
        return y

    def returned(g, cc):
        @pl.when(g > 0)
        def _():
            scopy(2 * g).wait_send()
            zcopy(2 * g).wait()
        scopy(2 * g + 1).wait_send()
        zcopy(2 * g + 1).wait()

        @pl.when(g < 3)
        def _():
            y_acc[...] = combine(g, y_acc[...])
        return cc

    y_acc[...] = h[...].astype(F32)
    lax.fori_loop(0, 4, returned, 0)
    y_out[...] = combine(jnp.int32(3), y_acc[...]).astype(BF16)


def solution(mesh):
    row_spec = P(("dp", "cp", "tp"), None)
    head_spec = P(None, "tp", None)
    expert_spec = P(("cp", "tp"), None, None)
    any_spec = pl.BlockSpec(memory_space=pl.ANY)
    vm = pl.BlockSpec(memory_space=pltpu.VMEM)
    DMA = pltpu.SemaphoreType.DMA

    def device_step(x, w_q, w_k, w_v, w_o, ids, gates, w_gate, w_up, w_down):
        tok, hid = x.shape
        nr = tok // QT
        hd = w_q.shape[1] * w_q.shape[2]
        kd = w_k.shape[1] * w_k.shape[2]
        wq_t = w_q.transpose(1, 2, 0).reshape(hd, hid)
        wk_t = w_k.transpose(1, 2, 0).reshape(kd, hid)
        wv_t = w_v.transpose(1, 2, 0).reshape(kd, hid)
        wo = w_o.reshape(hd, hid)
        seq = 8 * tok
        nk = 2 * tok // KC
        npair = w_q.shape[1] // 2
        f = w_gate.shape[2]

        h, wg_r, wu_r, wd_r = pl.pallas_call(
            attn_kernel,
            out_shape=[
                jax.ShapeDtypeStruct((tok, hid), BF16),
                jax.ShapeDtypeStruct((hid, f), BF16),
                jax.ShapeDtypeStruct((hid, f), BF16),
                jax.ShapeDtypeStruct((f, hid), BF16),
            ],
            in_specs=[any_spec] * 8,
            out_specs=[vm, any_spec, any_spec, any_spec],
            scratch_shapes=[
                pltpu.VMEM((2, 2 * tok, hid), BF16),
                pltpu.VMEM((hd, hid), BF16),
                pltpu.VMEM((2 * kd, hid), BF16),
                pltpu.VMEM((4, hd, hid), BF16),
                *[pltpu.VMEM((2, nk, 2 * kd, KC), BF16)] * 2,
                pltpu.VMEM((2, seq, 128), BF16),
                pltpu.VMEM((kd, seq), BF16),
                pltpu.VMEM((4 * nr, npair, 128, QW), BF16),
                pltpu.VMEM((4 * nr, QT, hd), BF16),
                pltpu.VMEM((tok, 4 * hd), BF16),
                pltpu.VMEM((4 * nr, npair, 1, QW), F32),
                pltpu.VMEM((4 * nr, npair, 8, QW), F32),
                pltpu.VMEM((4 * nr, npair, 32, QW), F32),
                pltpu.VMEM((npair, KC, QW), F32),
                pltpu.VMEM((npair, 8, QW), F32),
                pltpu.VMEM((tok, hid), F32),
                DMA((5,)), *[DMA((nk,))] * 2, DMA, DMA, *[DMA((nk,))] * 2,
                *[DMA((2, nk))] * 2, *[DMA((9,))] * 2, *[DMA((3,))] * 2,
                DMA((4 * nr,)), DMA((4, nr)),
            ],
            compiler_params=pltpu.CompilerParams(collective_id=0, has_side_effects=True, vmem_limit_bytes=60 * 1024 * 1024),
            name="attn",
        )(x, wq_t, wk_t, wv_t, wo, w_gate, w_up, w_down)

        cap = tok * 2 // 8
        fw = f // 2
        nf = 2 * f // fw
        n_dev = 8
        return pl.pallas_call(
            moe_kernel,
            out_shape=jax.ShapeDtypeStruct((tok, hid), BF16),
            in_specs=[vm, vm, vm] + [any_spec] * 6,
            out_specs=vm,
            scratch_shapes=[
                pltpu.VMEM((nf, hid, fw), BF16),
                pltpu.VMEM((nf, hid, fw), BF16),
                pltpu.VMEM((nf, fw, hid), BF16),
                *[pltpu.VMEM((n_dev, cap, hid), BF16)] * 4,
                pltpu.VMEM((2 * cap, hid), F32),
                pltpu.VMEM((tok, hid), F32),
                DMA((3, nf)), *[DMA((n_dev,))] * 4,
            ],
            compiler_params=pltpu.CompilerParams(collective_id=1, has_side_effects=True, vmem_limit_bytes=63 * 1024 * 1024),
            name="moe",
        )(h, ids.T, gates.T, w_gate, w_up, w_down, wg_r, wu_r, wd_r)

    return jax.shard_map(device_step, mesh=mesh, in_specs=(row_spec, head_spec, head_spec, head_spec, P("tp", None, None), row_spec, row_spec, expert_spec, expert_spec, expert_spec), out_specs=row_spec, check_vma=False)
```
